32 devices in a mesh: dp: 8 (over z, y), tensor: 4 (over x, core).
Axes of the slice: x: 2, y: 2, z: 4, core: 2. Of those that a mesh axis runs over, the one named last changes fastest.
Arguments:
- layer_input: bfloat16 [3072, 2304], P('dp'), may hold values from -6 to 6
- cotangent: bfloat16 [3072, 2304], P('dp'), may hold values from -6 to 6
- seq_lengths: int32 [8, 8], P('dp'), may hold values from 0 to 256, as said below
- norm_attn_in: float32 [2304], replicated, may hold values from 0.1 to 1.9
- w_query: bfloat16 [2304, 2048], P('dp', 'tensor'), may hold values from -1 to 1
- w_key: bfloat16 [2304, 1024], P('dp', 'tensor'), may hold values from -1 to 1
- w_value: bfloat16 [2304, 1024], P('dp', 'tensor'), may hold values from -0.125 to 0.125
- w_out: bfloat16 [2048, 2304], P('tensor', 'dp'), may hold values from -0.125 to 0.125
- norm_attn_out: float32 [2304], replicated, may hold values from 0.1 to 1.9
- norm_ffn_in: float32 [2304], replicated, may hold values from 0.1 to 1.9
- w_gate: bfloat16 [2304, 9216], P('dp', 'tensor'), may hold values from -0.125 to 0.125
- w_up: bfloat16 [2304, 9216], P('dp', 'tensor'), may hold values from -0.125 to 0.125
- w_down: bfloat16 [9216, 2304], P('tensor', 'dp'), may hold values from -0.0625 to 0.0625
- norm_ffn_out: float32 [2304], replicated, may hold values from 0.1 to 1.9
Outputs:
- layer_output: bfloat16 [3072, 2304], P('dp')
- input_grad: float32 [3072, 2304], P('dp')
- grad_norm_attn_in: float32 [2304], P('dp')
- grad_w_query: float32 [2304, 2048], P('dp', 'tensor')
- grad_w_key: float32 [2304, 1024], P('dp', 'tensor')
- grad_w_value: float32 [2304, 1024], P('dp', 'tensor')
- grad_w_out: float32 [2048, 2304], P('tensor', 'dp')
- grad_norm_attn_out: float32 [2304], P('dp')
- grad_norm_ffn_in: float32 [2304], P('dp')
- grad_w_gate: float32 [2304, 9216], P('dp', 'tensor')
- grad_w_up: float32 [2304, 9216], P('dp', 'tensor')
- grad_w_down: float32 [9216, 2304], P('tensor', 'dp')
- grad_norm_ffn_out: float32 [2304], P('dp')
The draws below stay inside these ranges and needn't reach their ends.
Inputs may be any that keep to these rules, and one draw needn't show every extreme that they name: `seq_lengths`: row r lists the lengths of the sequences on data index r in packing order; slots after the last sequence hold 0. Each row sums to at most 384 and some row sums to exactly 384; some sequence has exactly 256 tokens.
All inputs are finite; a program needn't handle non-finite values.
Results may differ from the reference program's by a relative error of at most 0.02.
The reference program's roundings to bfloat16 on the way count: a program that leaves them out, or rounds other values in their place, can miss the bound.
Values may be sent and summed in bfloat16 or wider, within the bound.
A program may use at most 256 MiB of HBM per device.

```python
import math
import jax
import jax.numpy as jnp
from jax import lax

D = 2304
H = 8
KV = 4
HD = 256
FF = 9216
CAP = 384
SLOTS = 8
MAXLEN = 256
TOKENS = 3072
N_DP = 8


def draw_seq_lengths(key, part):
    first_key, second_key, third_key = jax.random.split(key, 3)
    raw_lengths = jax.random.randint(first_key, (N_DP, SLOTS), MAXLEN // 2, MAXLEN + 1).astype(jnp.int32)
    budgets = jax.random.randint(second_key, (N_DP,), CAP // 4, CAP + 1).astype(jnp.int32)
    full_row = jax.random.randint(third_key, (), 0, N_DP).astype(jnp.int32)
    row_index = jnp.arange(N_DP, dtype=jnp.int32)
    budgets = jnp.where(row_index == full_row, CAP, budgets)
    leading = jnp.where(row_index == full_row, MAXLEN, raw_lengths[:, 0])
    raw_lengths = jnp.concatenate([leading[:, None], raw_lengths[:, 1:]], axis=1)
    before = jnp.cumsum(raw_lengths, axis=1).astype(jnp.int32) - raw_lengths
    lengths = jnp.minimum(jnp.maximum(budgets[:, None] - before, 0), raw_lengths)
    return lengths.astype(jnp.int32)


def head_scaled(key, head_count):
    entry_key, factor_key = jax.random.split(key)
    columns = head_count * HD
    entries = jnp.clip(jax.random.normal(entry_key, (D, columns), jnp.float32), -6.0, 6.0)
    factors = jnp.exp(jax.random.uniform(factor_key, (head_count,), jnp.float32, 0.0, math.log(6.0)))
    column_factors = jnp.repeat(factors, HD)
    scaled = entries * column_factors[None, :] * float(D) ** (-0.5)
    return jnp.clip(scaled, -1.0, 1.0)


def draw_w_query(key, part):
    return head_scaled(jax.random.fold_in(key, 71), H).astype(jnp.bfloat16)


def draw_w_key(key, part):
    return head_scaled(jax.random.fold_in(key, 83), KV).astype(jnp.bfloat16)


def spiked(array, own_key, source, target, parts, factor):
    owner, partner = [(jnp.arange(array.shape[position]) // (array.shape[position] // parts)).reshape([-1 if axis == position else 1 for axis in range(array.ndim)]) for position in (source, target)]
    chosen = jax.random.permutation(own_key, parts)[partner]
    strong = (owner == chosen) | (owner == (partner + parts // 2) % parts)
    return jnp.where(strong, factor * array, array)


def steps_of(stream_key, shape, cuts, smallest, top_value):
    factor_of = 1.0
    for dim, blocks in cuts:
        steps = jax.random.uniform(jax.random.fold_in(jax.random.fold_in(stream_key, 6), dim), (blocks,), jnp.float32, smallest / len(cuts), top_value / len(cuts))
        factor_of = factor_of * jnp.repeat(jnp.exp(steps), shape[dim] // blocks).reshape((-1,) + (1,) * (len(shape) - 1 - dim))
    return factor_of


def scatter_about(key, extent, scale, reach, cuts=(), kind=jnp.bfloat16):
    level = steps_of(key, extent, cuts, -0.22, 0.18) if cuts else 1.0
    values = jax.random.normal(key, extent, jnp.float32) * scale * level
    return jnp.minimum(jnp.maximum(values, -reach), reach).astype(kind)


def gaussian_with(rng, extent, width, most, cuts, heavy, held_as=jnp.bfloat16):
    drawn = width * jax.random.normal(rng, extent, jnp.float32)
    if cuts:
        drawn = drawn * steps_of(rng, extent, cuts, -0.22, 0.18)
    return jnp.clip(spiked(drawn, jax.random.fold_in(rng, 3), *heavy), -most, most).astype(held_as)


def setup_inputs(seed: int = 0) -> dict:
    key_list = jax.random.split(jax.random.key(seed), 15)
    layer_input = gaussian_with(key_list[0], (TOKENS, D), 1.0, 6.0, ((0, 8),), (0, 1, 8, 2.0))
    cotangent = scatter_about(key_list[1], (TOKENS, D), 1.0, 6.0, ((0, 8),))
    seq_lengths = draw_seq_lengths(jax.random.fold_in(key_list[14], 71), 0)
    norm_attn_in = jnp.clip(1.0 + 0.18 * jax.random.normal(key_list[3], (D,), jnp.float32), 0.1, 1.9)
    w_query = draw_w_query(jax.random.fold_in(key_list[14], 71), 0)
    w_key = draw_w_key(jax.random.fold_in(key_list[14], 71), 0)
    w_value = scatter_about(key_list[6], (D, KV * HD), D ** -0.5, 0.125, ((0, 8), (1, 4)))
    w_out = scatter_about(key_list[7], (H * HD, D), (H * HD) ** -0.5, 0.125, ((0, 4), (1, 8)))
    norm_attn_out = jnp.clip(1.0 + 0.18 * jax.random.normal(key_list[8], (D,), jnp.float32), 0.1, 1.9)
    norm_ffn_in = jnp.clip(1.0 + 0.18 * jax.random.normal(key_list[9], (D,), jnp.float32), 0.1, 1.9)
    w_gate = scatter_about(key_list[10], (D, FF), D ** -0.5, 0.125, ((0, 8), (1, 4)))
    w_up = scatter_about(key_list[11], (D, FF), D ** -0.5, 0.125, ((0, 8), (1, 4)))
    w_down = scatter_about(key_list[12], (FF, D), FF ** -0.5, 0.0625, ((0, 4), (1, 8)))
    norm_ffn_out = jnp.clip(1.0 + 0.18 * jax.random.normal(key_list[13], (D,), jnp.float32), 0.1, 1.9)
    return {"layer_input": layer_input, "cotangent": cotangent, "seq_lengths": seq_lengths, "norm_attn_in": norm_attn_in, "w_query": w_query, "w_key": w_key, "w_value": w_value, "w_out": w_out, "norm_attn_out": norm_attn_out, "norm_ffn_in": norm_ffn_in, "w_gate": w_gate, "w_up": w_up, "w_down": w_down, "norm_ffn_out": norm_ffn_out}


EPSILON = 1e-06
SOFT_CAP = 50.0
QUERY_SCALE = 0.0625
GELU_COEFF = 0.7978845608028654

def rms_scale(values, scales):
    return values * lax.rsqrt(lax.optimization_barrier(jnp.mean(values * values, axis=-1, keepdims=True)) + EPSILON) * scales

def gelu_tanh(inputs):
    return 0.5 * inputs * (1.0 + jnp.tanh(GELU_COEFF * (inputs + 0.044715 * inputs * inputs * inputs)))

def rotate_half(heads):
    middle = heads.shape[-1] // 2
    return jnp.concatenate([-heads[..., middle:], heads[..., :middle]], axis=-1)

def layout(lengths, row_count):
    lengths = lengths.astype(jnp.int32)
    seq_ends = jnp.cumsum(lengths).astype(jnp.int32)
    row_index = jnp.arange(row_count, dtype=jnp.int32)
    passed = (row_index[:, None] >= seq_ends[None, :]).astype(jnp.int32)
    segment = lax.optimization_barrier(jnp.sum(passed, axis=1)).astype(jnp.int32)
    is_live = row_index < seq_ends[-1]
    seq_ident = jnp.where(is_live, segment, lengths.shape[0] + row_index)
    offset = row_index - lax.optimization_barrier(jnp.sum(passed * lengths[None, :], axis=1)).astype(jnp.int32)
    allowed = (seq_ident[:, None] == seq_ident[None, :]) & (row_index[None, :] <= row_index[:, None])
    middle = HD // 2
    inverse = jnp.exp(jnp.arange(middle, dtype=jnp.float32) * (-2.0 * math.log(10000.0) / HD))
    angles = offset.astype(jnp.float32)[:, None] * inverse[None, :]
    cosine = jnp.concatenate([jnp.cos(angles), jnp.cos(angles)], axis=1)
    sine_wave = jnp.concatenate([jnp.sin(angles), jnp.sin(angles)], axis=1)
    return (is_live, allowed, cosine, sine_wave)

def product(left, right, form):
    return jnp.einsum(form, left.astype(jnp.float32), right.astype(jnp.float32))

def matmul(left, right):
    return jnp.dot(left, right, preferred_element_type=jnp.float32)

def block(layer_rows, cot_rows, lengths, params):
    norm_attn_in, w_query, w_key, w_value, w_out, norm_attn_out, norm_ffn_in, w_gate, w_up, w_down, norm_ffn_out = params
    row_count = layer_rows.shape[0]
    is_live, allowed, cosine, sine_wave = layout(lengths, row_count)
    kv_heads = w_key.shape[1] // HD
    groups = H // KV
    layer_float = layer_rows.astype(jnp.float32)
    h_attn = rms_scale(layer_float, norm_attn_in).astype(jnp.bfloat16)
    query_pre = matmul(h_attn, w_query).reshape(row_count, kv_heads, groups, HD).transpose(1, 2, 0, 3)
    query = ((query_pre * cosine + rotate_half(query_pre) * sine_wave) * QUERY_SCALE).astype(jnp.bfloat16)
    key_pre = matmul(h_attn, w_key).reshape(row_count, kv_heads, HD).transpose(1, 0, 2)
    keys = (key_pre * cosine + rotate_half(key_pre) * sine_wave).astype(jnp.bfloat16)
    values = matmul(h_attn, w_value).astype(jnp.bfloat16).reshape(row_count, kv_heads, HD).transpose(1, 0, 2)
    capped = SOFT_CAP * jnp.tanh(product(query, keys, 'kgqd,ksd->kgqs') / SOFT_CAP)
    expo = jnp.where(allowed, jnp.exp(capped), 0.0)
    log_total = jnp.log(lax.optimization_barrier(jnp.sum(expo, axis=-1, keepdims=True)))
    probs = jnp.where(allowed, jnp.exp(capped - log_total), 0.0)
    probs_low = probs.astype(jnp.bfloat16)
    mixed = product(probs_low, values, 'kgqs,ksd->kgqd').astype(jnp.bfloat16)
    mixed_flat = mixed.transpose(2, 0, 1, 3).reshape(row_count, -1)
    attn_branch = matmul(mixed_flat, w_out)
    resid = layer_float + rms_scale(attn_branch, norm_attn_out)
    h_ffn = rms_scale(resid, norm_ffn_in).astype(jnp.bfloat16)
    gate_pre = matmul(h_ffn, w_gate)
    up_pre = matmul(h_ffn, w_up)
    gelu_gate = gelu_tanh(gate_pre)
    hidden = (gelu_gate * up_pre).astype(jnp.bfloat16)
    ffn_branch = matmul(hidden, w_down)
    layer_output = (resid + rms_scale(ffn_branch, norm_ffn_out)).astype(jnp.bfloat16)
    grad_out = cot_rows.astype(jnp.float32) * is_live[:, None].astype(jnp.float32)
    _, pull_four = jax.vjp(rms_scale, ffn_branch, norm_ffn_out)
    grad_ffn_float, grad_norm_ffn_out = pull_four(grad_out)
    grad_ffn_branch = grad_ffn_float.astype(jnp.bfloat16)
    grad_w_down = matmul(hidden.T, grad_ffn_branch)
    grad_hidden = matmul(grad_ffn_branch, w_down.T)
    grad_up = (grad_hidden * gelu_gate).astype(jnp.bfloat16)
    _, pull_gelu = jax.vjp(gelu_tanh, gate_pre)
    grad_gate = pull_gelu(grad_hidden * up_pre)[0].astype(jnp.bfloat16)
    grad_w_gate = matmul(h_ffn.T, grad_gate)
    grad_w_up = matmul(h_ffn.T, grad_up)
    grad_h_ffn = matmul(grad_gate, w_gate.T) + matmul(grad_up, w_up.T)
    _, pull_three = jax.vjp(rms_scale, resid, norm_ffn_in)
    grad_resid_part, grad_norm_ffn_in = pull_three(grad_h_ffn)
    grad_resid = grad_out + grad_resid_part
    _, pull_two = jax.vjp(rms_scale, attn_branch, norm_attn_out)
    grad_attn_float, grad_norm_attn_out = pull_two(grad_resid)
    grad_attn_branch = grad_attn_float.astype(jnp.bfloat16)
    grad_w_out = matmul(mixed_flat.T, grad_attn_branch)
    grad_mixed = matmul(grad_attn_branch, w_out.T).astype(jnp.bfloat16)
    grad_mixed = grad_mixed.reshape(row_count, kv_heads, groups, HD).transpose(1, 2, 0, 3)
    capped_back = SOFT_CAP * jnp.tanh(product(query, keys, 'kgqd,ksd->kgqs') / SOFT_CAP)
    weights_back = jnp.where(allowed, jnp.exp(capped_back - log_total), 0.0)
    grad_values = product(weights_back.astype(jnp.bfloat16), grad_mixed, 'kgqs,kgqd->ksd').astype(jnp.bfloat16)
    grad_probs = product(grad_mixed, values, 'kgqd,ksd->kgqs')
    row_delta = lax.optimization_barrier(jnp.sum(weights_back * grad_probs, axis=-1, keepdims=True))
    tanh_part = capped_back / SOFT_CAP
    grad_scores = (weights_back * (grad_probs - row_delta) * (1.0 - tanh_part * tanh_part)).astype(jnp.bfloat16)
    grad_query_raw = product(grad_scores, keys, 'kgqs,ksd->kgqd')
    grad_query = ((grad_query_raw * cosine - rotate_half(grad_query_raw) * sine_wave) * QUERY_SCALE).astype(jnp.bfloat16)
    grad_keys_raw = product(grad_scores, query, 'kgqs,kgqd->ksd')
    grad_keys = (grad_keys_raw * cosine - rotate_half(grad_keys_raw) * sine_wave).astype(jnp.bfloat16)
    grad_query_flat = grad_query.transpose(2, 0, 1, 3).reshape(row_count, -1)
    grad_keys_flat = grad_keys.transpose(1, 0, 2).reshape(row_count, -1)
    grad_values_flat = grad_values.transpose(1, 0, 2).reshape(row_count, -1)
    grad_w_query = matmul(h_attn.T, grad_query_flat)
    grad_w_key = matmul(h_attn.T, grad_keys_flat)
    grad_w_value = matmul(h_attn.T, grad_values_flat)
    grad_h_attn = matmul(grad_query_flat, w_query.T) + matmul(grad_keys_flat, w_key.T) + matmul(grad_values_flat, w_value.T)
    _, pull_one = jax.vjp(rms_scale, layer_float, norm_attn_in)
    grad_input_part, grad_norm_attn_in = pull_one(grad_h_attn)
    input_grad = grad_resid + grad_input_part
    grads = (grad_norm_attn_in, grad_w_query, grad_w_key, grad_w_value, grad_w_out, grad_norm_attn_out, grad_norm_ffn_in, grad_w_gate, grad_w_up, grad_w_down, grad_norm_ffn_out)
    return (layer_output, input_grad, grads)

def reference(layer_input, cotangent, seq_lengths, norm_attn_in, w_query, w_key, w_value, w_out, norm_attn_out, norm_ffn_in, w_gate, w_up, w_down, norm_ffn_out):
    params = (norm_attn_in, w_query, w_key, w_value, w_out, norm_attn_out, norm_ffn_in, w_gate, w_up, w_down, norm_ffn_out)
    starting = tuple((jnp.zeros(item.shape, jnp.float32) for item in params))

    def advance(running, items):
        layer_rows, cot_rows, lengths = items
        output_rows, input_rows, grads = block(layer_rows, cot_rows, lengths, params)
        running = tuple((earlier + addend for earlier, addend in zip(running, grads)))
        return (running, (output_rows, input_rows))
    running, (outputs, input_grads) = lax.scan(advance, starting, (layer_input.reshape(N_DP, CAP, D), cotangent.reshape(N_DP, CAP, D), seq_lengths))
    return (outputs.reshape(TOKENS, D), input_grads.reshape(TOKENS, D), running[0], running[1], running[2], running[3], running[4], running[5], running[6], running[7], running[8], running[9], running[10])
```

```python
import functools
import math

import jax
import jax.numpy as jnp
from jax import lax
from jax.experimental import pallas as pl
from jax.experimental.pallas import tpu as pltpu
from jax.sharding import Mesh, PartitionSpec as P

H = 8
KV = 4
HD = 256


EPSILON = 1e-06
SOFT_CAP = 50.0
QUERY_SCALE = 0.0625
GELU_COEFF = 0.7978845608028654

MESH = pl.DeviceIdType.MESH


def rms_scale(values, scales):
    return values * lax.rsqrt(jnp.mean(values * values, axis=-1, keepdims=True) + EPSILON) * scales


def gelu_tanh(inputs):
    return (
        0.5 * inputs * (1.0 + jnp.tanh(GELU_COEFF * (inputs + 0.044715 * inputs * inputs * inputs)))
    )


def rotate_half(heads):
    middle = heads.shape[-1] // 2
    return jnp.concatenate([-heads[..., middle:], heads[..., :middle]], axis=-1)


def layout(lengths, row_count):
    seq_ends = jnp.cumsum(lengths)
    row_index = jnp.arange(row_count, dtype=jnp.int32)
    passed = (row_index[:, None] >= seq_ends[None, :]).astype(jnp.int32)
    segment = jnp.sum(passed, axis=1)
    is_live = row_index < seq_ends[-1]
    seq_ident = jnp.where(is_live, segment, lengths.shape[0] + row_index)
    offset = row_index - jnp.sum(passed * lengths[None, :], axis=1)
    allowed = (seq_ident[:, None] == seq_ident[None, :]) & (
        row_index[None, :] <= row_index[:, None]
    )
    middle = HD // 2
    inverse = jnp.exp(jnp.arange(middle, dtype=jnp.float32) * (-2.0 * math.log(10000.0) / HD))
    angles = offset.astype(jnp.float32)[:, None] * inverse[None, :]
    cosine = jnp.concatenate([jnp.cos(angles), jnp.cos(angles)], axis=1)
    sine_wave = jnp.concatenate([jnp.sin(angles), jnp.sin(angles)], axis=1)
    return (is_live, allowed, cosine, sine_wave)


def matmul(left, right):
    return jnp.dot(left, right, preferred_element_type=jnp.float32)


def left_product(left, right):
    return jnp.einsum("td,tc->dc", left, right, preferred_element_type=jnp.float32)


def right_product(left, right):
    return jnp.einsum("tc,dc->td", left, right, preferred_element_type=jnp.float32)


def capped_scores(query, keys):
    raw_scores = jnp.einsum("kgqd,ksd->kgqs", query, keys, preferred_element_type=jnp.float32)
    return SOFT_CAP * jnp.tanh(raw_scores / SOFT_CAP)


def pick(blocks, index):
    return lax.dynamic_index_in_dim(blocks, index, 0, keepdims=False)


def swap_blocks(blocks, axis):
    size = blocks.shape[0]
    here = lax.axis_index(axis)
    result = lax.dynamic_update_index_in_dim(
        jnp.zeros_like(blocks), pick(blocks, here), here, 0
    )
    for step in range(1, size):
        came = lax.ppermute(
            pick(blocks, lax.rem(here + step, size)),
            axis,
            [(i, (i + step) % size) for i in range(size)],
        )
        result = lax.dynamic_update_index_in_dim(
            result, came, lax.rem(here - step + size, size), 0
        )
    return result


def collect(block, axis, size):
    here = lax.axis_index(axis)
    result = jnp.zeros((size,) + block.shape, block.dtype)
    result = lax.dynamic_update_index_in_dim(result, block, here, 0)
    for step in range(1, size):
        came = lax.ppermute(block, axis, [(i, (i + step) % size) for i in range(size)])
        result = lax.dynamic_update_index_in_dim(
            result, came, lax.rem(here - step + size, size), 0
        )
    return result


def sum_blocks(blocks, axis):
    size = blocks.shape[0]
    here = lax.axis_index(axis)
    total = pick(blocks, here).astype(jnp.float32)
    for step in range(1, size):
        came = lax.ppermute(
            pick(blocks, lax.rem(here + step, size)),
            axis,
            [(i, (i + step) % size) for i in range(size)],
        )
        total = total + came.astype(jnp.float32)
    return total


def device_layout(lanes):
    _, inner, tensor = lanes
    cores = 2 if tensor % 2 == 0 else 1
    return {"inner": inner, "x": tensor // cores, "core": cores}


class Spot:
    def __init__(self, lanes, chain, levels):
        self.sizes = device_layout(lanes)
        self.chain, self.levels = chain, levels
        self.length = lanes[0] if chain else 1
        self.at_chain = lax.axis_index("outer")
        tensor = lax.axis_index("tensor")
        cores = self.sizes["core"]
        self.here = {
            "inner": lax.axis_index("inner"),
            "x": lax.div(tensor, cores),
            "core": lax.rem(tensor, cores),
        }
        self.step = self.at_chain if chain else 0
        self.slots = {}
        for level in levels:
            for shift in range(1, self.sizes[level]):
                self.slots[level, shift] = 2 + len(self.slots)

    def moved(self, **shifts):
        at = dict(self.here)
        for level, shift in shifts.items():
            at[level] = lax.rem(at[level] + shift, self.sizes[level])
        return at

    def device(self, at, chain_shift=0):
        return (
            self.at_chain + chain_shift,
            at["inner"],
            at["x"] * self.sizes["core"] + at["core"],
        )

    def flat(self, step, at):
        index = step
        for level in self.levels:
            index = index * self.sizes[level] + at[level]
        return index

    def greet(self):
        barrier = pltpu.get_barrier_semaphore()
        count = 0
        for level in self.levels:
            for shift in range(1, self.sizes[level]):
                pl.semaphore_signal(
                    barrier, device_id=self.device(self.moved(**{level: shift})), device_id_type=MESH
                )
                count += 1
        if self.length > 1:
            for shift, there in ((-1, self.step > 0), (1, self.step < self.length - 1)):
                count = count + there.astype(jnp.int32)

                @pl.when(there)
                def _(shift=shift):
                    pl.semaphore_signal(
                        barrier, device_id=self.device(self.here, shift), device_id_type=MESH
                    )

        pl.semaphore_wait(barrier, count)


def guarded(condition, action):
    if condition is None:
        action()
    else:
        pl.when(condition)(action)


def both(first, second):
    if first is None:
        return second
    return first if second is None else jnp.logical_and(first, second)


def gather_kernel(lanes, chain, levels, x_ref, o_ref, send_sem, recv_sem, local_sem):
    spot = Spot(lanes, chain, levels)
    length, step, here = spot.length, spot.step, spot.here
    started = []

    def send(condition, source, index, slot, device):
        def copy():
            return pltpu.make_async_remote_copy(
                src_ref=source,
                dst_ref=o_ref.at[index],
                send_sem=send_sem.at[slot, index],
                recv_sem=recv_sem.at[index],
                device_id=device,
                device_id_type=MESH,
            )

        guarded(condition, lambda: copy().start())
        started.append((condition, copy))

    def arrive(condition, index):
        def wait():
            pltpu.make_async_remote_copy(
                src_ref=o_ref.at[index],
                dst_ref=o_ref.at[index],
                send_sem=send_sem.at[0, index],
                recv_sem=recv_sem.at[index],
                device_id=spot.device(here),
                device_id_type=MESH,
            ).wait_recv()

        guarded(condition, wait)

    def spread(condition, source, index, first):
        for level in levels[first:]:
            for shift in range(1, spot.sizes[level]):
                send(
                    condition,
                    source,
                    index,
                    spot.slots[level, shift],
                    spot.device(spot.moved(**{level: shift})),
                )

    def around(distance):
        if distance == 0:
            return [(None, step)]
        return [(step - distance >= 0, step - distance), (step + distance < length, step + distance)]

    def clipped(position):
        return lax.rem(position + length, length) if length > 1 else position

    spot.greet()
    mine = spot.flat(step, here)
    local = pltpu.make_async_copy(x_ref, o_ref.at[mine], local_sem)
    local.start()
    if length > 1:
        send(step < length - 1, x_ref, mine, 1, spot.device(here, 1))
        send(step > 0, x_ref, mine, 0, spot.device(here, -1))
    spread(None, x_ref, mine, 0)

    def relay(distance):
        if len(levels) < 2:
            return
        level = levels[0]
        for there, position in around(distance):
            for shift in range(1, spot.sizes[level]):
                index = spot.flat(clipped(position), spot.moved(**{level: shift}))
                arrive(there, index)
                spread(there, o_ref.at[index], index, 1)

    for distance in range(1, length):
        for way, (there, position) in enumerate(around(distance)):
            index = spot.flat(clipped(position), here)
            arrive(there, index)
            onward = step < length - 1 if way == 0 else step > 0
            send(
                both(there, onward),
                o_ref.at[index],
                index,
                1 - way,
                spot.device(here, 1 if way == 0 else -1),
            )
            spread(there, o_ref.at[index], index, 0)
        relay(distance - 1)
    relay(length - 1)
    last = levels[-1]
    others = [{}]
    for level in levels[:-1]:
        others = [{**rest, level: shift} for rest in others for shift in range(spot.sizes[level])]
    for position in range(length):
        for rest in others:
            for shift in range(1, spot.sizes[last]):
                arrive(None, spot.flat(position, spot.moved(**{**rest, last: shift})))
    for condition, copy in started:
        guarded(condition, lambda copy=copy: copy().wait_send())
    local.wait()


def gather_blocks(block, lanes, chain, levels, collective_id):
    sizes = device_layout(lanes)
    count = (lanes[0] if chain else 1) * math.prod(sizes[level] for level in levels)
    slots = 2 + sum(sizes[level] - 1 for level in levels)
    return pl.pallas_call(
        functools.partial(gather_kernel, lanes, chain, levels),
        out_shape=jax.ShapeDtypeStruct((count,) + block.shape, block.dtype),
        in_specs=[pl.BlockSpec(memory_space=pltpu.VMEM)],
        out_specs=pl.BlockSpec(memory_space=pl.ANY),
        scratch_shapes=[
            pltpu.SemaphoreType.DMA((slots, count)),
            pltpu.SemaphoreType.DMA((count,)),
            pltpu.SemaphoreType.DMA,
        ],
        compiler_params=pltpu.CompilerParams(collective_id=collective_id, has_side_effects=True),
        cost_estimate=pl.CostEstimate(
            flops=0, bytes_accessed=20 * count * block.size, transcendentals=0
        ),
    )(block)


def add_into(target, parts, condition=None):
    rows = target.shape[0]
    tile = math.gcd(rows, 16)

    def action():
        def body(r, carry):
            window = pl.ds(pl.multiple_of(r * tile, tile), tile)
            total = parts[0][window, :].astype(jnp.float32)
            for part in parts[1:]:
                total = total + part[window, :].astype(jnp.float32)
            target[window, :] = total.astype(target.dtype)
            return carry

        lax.fori_loop(0, rows // tile, body, 0)

    guarded(condition, action)


def scatter_kernel(
    lanes, chain, levels, order, x_ref, o_ref, came0, came1, held0, held1, chained, sems, got0, got1, gotc
):
    spot = Spot(lanes, chain, levels)
    length, step, here = spot.length, spot.step, spot.here
    started = []

    def send(condition, source, target, send_at, recv_at, device):
        def copy():
            return pltpu.make_async_remote_copy(
                src_ref=source,
                dst_ref=target,
                send_sem=send_at,
                recv_sem=recv_at,
                device_id=device,
                device_id_type=MESH,
            )

        guarded(condition, lambda: copy().start())
        started.append((condition, copy))

    def arrive(condition, target, recv_at):
        def wait():
            pltpu.make_async_remote_copy(
                src_ref=target,
                dst_ref=target,
                send_sem=recv_at,
                recv_sem=recv_at,
                device_id=spot.device(here),
                device_id_type=MESH,
            ).wait_recv()

        guarded(condition, wait)

    visits = []
    for distance in range(length - 1, -1, -1):
        if distance == 0:
            visits.append((None, step, 0))
        else:
            visits.append(
                (step - distance >= 0, lax.rem(step - distance + length, length), -1)
            )
            visits.append((step + distance < length, lax.rem(step + distance, length), 1))

    spot.greet()
    first = order[0]
    second = order[1] if len(order) > 1 else None
    n_first = spot.sizes[first]
    n_second = spot.sizes[second] if second else 1

    def second_shifts(own):
        return [0] if own else list(range(1, n_second))

    for own in (False, True):
        for there, position, _ in visits:
            for other in second_shifts(own):
                for shift in range(1, n_first):
                    where = {first: shift}
                    if second:
                        where[second] = other
                    at = spot.moved(**where)
                    lane = position * n_second + (at[second] if second else 0)
                    send(
                        there,
                        x_ref.at[spot.flat(position, at)],
                        came0.at[shift - 1, lane],
                        sems.at[shift - 1, lane],
                        got0.at[shift - 1, lane],
                        spot.device(spot.moved(**{first: shift})),
                    )

    def first_sum(there, position, other):
        at = spot.moved(**({second: other} if second else {}))
        lane = position * n_second + (at[second] if second else 0)
        parts = [x_ref.at[spot.flat(position, at)]]
        for shift in range(1, n_first):
            arrive(there, came0.at[shift - 1, lane], got0.at[shift - 1, lane])
            parts.append(came0.at[shift - 1, lane])
        return parts

    for there, position, _ in visits:
        for other in second_shifts(False):
            parts = first_sum(there, position, other)
            add_into(held0.at[other - 1, position], parts, there)
            send(
                there,
                held0.at[other - 1, position],
                came1.at[other - 1, position],
                sems.at[n_first - 1 + other - 1, position],
                got1.at[other - 1, position],
                spot.device(spot.moved(**{second: other})),
            )
    base = n_first - 1 + n_second - 1
    for there, position, way in visits:
        parts = first_sum(there, position, 0)
        for other in second_shifts(False):
            arrive(there, came1.at[other - 1, position], got1.at[other - 1, position])
            parts.append(came1.at[other - 1, position])
        if way == 0:
            if length > 1:
                for side, exists in ((0, step > 0), (1, step < length - 1)):
                    arrive(exists, chained.at[side, position], gotc.at[side, position])

                def extra(sides):
                    return parts + [chained.at[side, position] for side in sides]

                inside = jnp.logical_and(step > 0, step < length - 1)
                add_into(o_ref, extra((0, 1)), inside)
                add_into(o_ref, extra((1,)), step == 0)
                add_into(o_ref, extra((0,)), step == length - 1)
            else:
                add_into(o_ref, parts)
        else:
            side = 1 if way == -1 else 0
            inner_link = step < length - 1 if way == -1 else step > 0
            with_more = both(there, inner_link)
            alone = both(there, jnp.logical_not(inner_link))
            arrive(with_more, chained.at[side, position], gotc.at[side, position])
            add_into(held1.at[position], parts + [chained.at[side, position]], with_more)
            add_into(held1.at[position], parts, alone)
            send(
                there,
                held1.at[position],
                chained.at[side, position],
                sems.at[base, position],
                gotc.at[side, position],
                spot.device(here, way),
            )
    for condition, copy in started:
        guarded(condition, lambda copy=copy: copy().wait_send())


def scatter_sum(blocks, lanes, chain, levels, order, collective_id, kind=jnp.float32):
    sizes = device_layout(lanes)
    length = lanes[0] if chain else 1
    rows, columns = blocks.shape[1:]
    low = blocks.dtype
    n_first = sizes[order[0]]
    n_second = sizes[order[1]] if len(order) > 1 else 1
    extra = max(n_first - 1, 1)
    further = max(n_second - 1, 1)
    return pl.pallas_call(
        functools.partial(scatter_kernel, lanes, chain, levels, order),
        out_shape=jax.ShapeDtypeStruct((rows, columns), kind),
        in_specs=[pl.BlockSpec(memory_space=pltpu.VMEM)],
        out_specs=pl.BlockSpec(memory_space=pltpu.VMEM),
        scratch_shapes=[
            pltpu.VMEM((extra, length * n_second, rows, columns), low),
            pltpu.VMEM((further, length, rows, columns), low),
            pltpu.VMEM((further, length, rows, columns), low),
            pltpu.VMEM((length, rows, columns), low),
            pltpu.VMEM((2, length, rows, columns), low),
            pltpu.SemaphoreType.DMA((n_first + n_second, length * n_second)),
            pltpu.SemaphoreType.DMA((extra, length * n_second)),
            pltpu.SemaphoreType.DMA((further, length)),
            pltpu.SemaphoreType.DMA((2, length)),
        ],
        compiler_params=pltpu.CompilerParams(collective_id=collective_id, has_side_effects=True),
        cost_estimate=pl.CostEstimate(
            flops=0, bytes_accessed=20 * blocks.size, transcendentals=0
        ),
    )(blocks)


def shards(
    lanes,
    layer_input,
    cotangent,
    seq_lengths,
    norm_attn_in,
    w_query,
    w_key,
    w_value,
    w_out,
    norm_attn_out,
    norm_ffn_in,
    w_gate,
    w_up,
    w_down,
    norm_ffn_out,
):
    outer, inner, tensor = lanes
    low = jnp.bfloat16
    dp = ("outer", "inner")
    shard_rows, width = w_gate.shape
    part = width // outer
    query_cols, key_cols = w_query.shape[1], w_key.shape[1]
    qkv_cols = query_cols + 2 * key_cols

    attn_shard = jnp.concatenate([w_query, w_key, w_value, w_out.T], axis=1)
    attn_full = gather_blocks(attn_shard, lanes, True, ("inner",), 0)
    attn_full = attn_full.reshape(-1, attn_shard.shape[1])
    down_turned = w_down.T
    ffn_shard = jnp.stack(
        [
            jnp.concatenate(
                [item[:, i * part : (i + 1) * part] for item in (w_gate, w_up, down_turned)],
                axis=1,
            )
            for i in range(outer)
        ]
    )
    ffn_mine = swap_blocks(ffn_shard, "outer")
    attn_full, ffn_mine = lax.optimization_barrier((attn_full, ffn_mine))
    ffn_full = collect(ffn_mine, "inner", inner).transpose(1, 0, 2, 3).reshape(-1, 3 * part)

    row_count = layer_input.shape[0]
    split_rows = row_count // tensor
    first_row = lax.axis_index("tensor") * split_rows

    def own_rows(array):
        return lax.dynamic_slice_in_dim(array, first_row, split_rows, 0)

    is_live, allowed, cosine, sine_wave = layout(seq_lengths[0], row_count)
    kv_heads = key_cols // HD
    groups = H // KV
    layer_float = layer_input.astype(jnp.float32)
    h_attn = rms_scale(layer_float, norm_attn_in).astype(low)
    projected = matmul(h_attn, attn_full[:, :qkv_cols])
    query_pre = (
        projected[:, :query_cols].reshape(row_count, kv_heads, groups, HD).transpose(1, 2, 0, 3)
    )
    query = ((query_pre * cosine + rotate_half(query_pre) * sine_wave) * QUERY_SCALE).astype(low)
    key_pre = (
        projected[:, query_cols : query_cols + key_cols]
        .reshape(row_count, kv_heads, HD)
        .transpose(1, 0, 2)
    )
    keys = (key_pre * cosine + rotate_half(key_pre) * sine_wave).astype(low)
    values = (
        projected[:, query_cols + key_cols :]
        .astype(low)
        .reshape(row_count, kv_heads, HD)
        .transpose(1, 0, 2)
    )
    capped = capped_scores(query, keys)
    expo = jnp.where(allowed, jnp.exp(capped), 0.0)
    log_total = jnp.log(jnp.sum(expo, axis=-1, keepdims=True))
    weights = jnp.where(allowed, jnp.exp(capped - log_total), 0.0)
    probs = weights.astype(low)
    mixed = jnp.einsum("kgqs,ksd->kgqd", probs, values, preferred_element_type=jnp.float32).astype(
        low
    )
    mixed_flat = mixed.transpose(2, 0, 1, 3).reshape(row_count, -1)
    out_turned = attn_full[:, qkv_cols:]
    attn_branch = scatter_sum(
        right_product(mixed_flat, out_turned).astype(low).reshape(tensor, split_rows, -1),
        lanes,
        False,
        ("x", "core"),
        ("core", "x"),
        1,
    )
    layer_own = own_rows(layer_float)
    resid = layer_own + rms_scale(attn_branch, norm_attn_out)
    h_ffn = rms_scale(resid, norm_ffn_in).astype(low)

    h_all = gather_blocks(h_ffn, lanes, True, ("x", "core"), 2).reshape(-1, h_ffn.shape[1])
    gate_up = matmul(h_all, ffn_full[:, : 2 * part])
    gate_pre, up_pre = gate_up[:, :part], gate_up[:, part:]
    gelu_gate = gelu_tanh(gate_pre)
    hidden = (gelu_gate * up_pre).astype(low)
    down_full = ffn_full[:, 2 * part :]
    ffn_branch = scatter_sum(
        right_product(hidden, down_full).astype(low).reshape(outer * tensor, split_rows, -1),
        lanes,
        True,
        ("x", "core"),
        ("core", "x"),
        3,
    )
    output_own = (resid + rms_scale(ffn_branch, norm_ffn_out)).astype(low)

    grad_out = own_rows(cotangent).astype(jnp.float32) * own_rows(
        is_live.astype(jnp.float32)[:, None]
    )
    _, pull_four = jax.vjp(rms_scale, ffn_branch, norm_ffn_out)
    grad_ffn_float, grad_norm_ffn_out = pull_four(grad_out)
    grad_ffn_all = gather_blocks(grad_ffn_float.astype(low), lanes, True, ("x", "core"), 4)
    grad_ffn_all = grad_ffn_all.reshape(-1, h_ffn.shape[1])
    grad_hidden = matmul(grad_ffn_all, down_full)
    grad_up = (grad_hidden * gelu_gate).astype(low)
    _, pull_gelu = jax.vjp(gelu_tanh, gate_pre)
    grad_gate = pull_gelu(grad_hidden * up_pre)[0].astype(low)
    grad_both = jnp.concatenate([grad_gate, grad_up], axis=1)
    grad_h_part = right_product(grad_both, ffn_full[:, : 2 * part]).astype(low)
    grad_h_ffn = scatter_sum(
        grad_h_part.reshape(outer * tensor, split_rows, -1),
        lanes,
        True,
        ("x", "core"),
        ("core", "x"),
        5,
    )
    grad_w_ffn = jnp.concatenate(
        [
            left_product(h_all, grad_both).astype(low),
            left_product(grad_ffn_all, hidden).astype(low),
        ],
        axis=1,
    )
    grad_w_ffn = grad_w_ffn.reshape(outer, inner, shard_rows, 3 * part).transpose(1, 0, 2, 3)
    grad_w_ffn = sum_blocks(grad_w_ffn, "inner").astype(low)
    grad_w_ffn = swap_blocks(grad_w_ffn, "outer").astype(jnp.float32)
    sum_gate, sum_up, sum_down = (
        jnp.concatenate([grad_w_ffn[i, :, j * part : (j + 1) * part] for i in range(outer)], axis=1)
        for j in range(3)
    )
    sum_down = sum_down.T

    _, pull_three = jax.vjp(rms_scale, resid, norm_ffn_in)
    grad_resid_part, grad_norm_ffn_in = pull_three(grad_h_ffn)
    grad_resid = grad_out + grad_resid_part
    _, pull_two = jax.vjp(rms_scale, attn_branch, norm_attn_out)
    grad_attn_float, grad_norm_attn_out = pull_two(grad_resid)
    grad_attn_branch = gather_blocks(
        grad_attn_float.astype(low), lanes, False, ("x", "core"), 6
    ).reshape(row_count, -1)
    grad_mixed = matmul(grad_attn_branch, out_turned).astype(low)
    grad_mixed = grad_mixed.reshape(row_count, kv_heads, groups, HD).transpose(1, 2, 0, 3)
    grad_values = jnp.einsum(
        "kgqs,kgqd->ksd", probs, grad_mixed, preferred_element_type=jnp.float32
    ).astype(low)
    grad_probs = jnp.einsum(
        "kgqd,ksd->kgqs", grad_mixed, values, preferred_element_type=jnp.float32
    )
    row_delta = jnp.sum(weights * grad_probs, axis=-1, keepdims=True)
    tanh_part = capped / SOFT_CAP
    grad_scores = (weights * (grad_probs - row_delta) * (1.0 - tanh_part * tanh_part)).astype(low)
    grad_query_raw = jnp.einsum(
        "kgqs,ksd->kgqd", grad_scores, keys, preferred_element_type=jnp.float32
    )
    grad_query = (
        (grad_query_raw * cosine - rotate_half(grad_query_raw) * sine_wave) * QUERY_SCALE
    ).astype(low)
    grad_keys_raw = jnp.einsum(
        "kgqs,kgqd->ksd", grad_scores, query, preferred_element_type=jnp.float32
    )
    grad_keys = (grad_keys_raw * cosine - rotate_half(grad_keys_raw) * sine_wave).astype(low)
    grad_qkv = jnp.concatenate(
        [
            grad_query.transpose(2, 0, 1, 3).reshape(row_count, -1),
            grad_keys.transpose(1, 0, 2).reshape(row_count, -1),
            grad_values.transpose(1, 0, 2).reshape(row_count, -1),
        ],
        axis=1,
    )
    grad_a_part = right_product(grad_qkv, attn_full[:, :qkv_cols]).astype(low)
    grad_h_attn = scatter_sum(
        grad_a_part.reshape(tensor, split_rows, -1),
        lanes,
        False,
        ("x", "core"),
        ("core", "x"),
        7,
    )
    _, pull_one = jax.vjp(rms_scale, layer_own, norm_attn_in)
    grad_input_part, grad_norm_attn_in = pull_one(grad_h_attn)
    input_own = grad_resid + grad_input_part

    layer_output = lax.all_gather(output_own, "tensor", axis=0, tiled=True)
    input_grad = lax.all_gather(input_own.astype(low), "tensor", axis=0, tiled=True)
    norm_rows = jnp.stack(
        [grad_norm_attn_in, grad_norm_attn_out, grad_norm_ffn_in, grad_norm_ffn_out]
    )
    norm_all = lax.all_gather(norm_rows, (*dp, "tensor"), axis=0, tiled=False)
    input_grad = input_grad.astype(jnp.float32)
    position = lax.axis_index("outer") * inner + lax.axis_index("inner")
    norm_all = lax.dynamic_slice_in_dim(norm_all, position * shard_rows, shard_rows, 2)
    sum_attn_in, sum_attn_out, sum_ffn_in, sum_ffn_out = (
        item for item in jnp.sum(norm_all, axis=0)
    )

    grad_w_attn = jnp.concatenate(
        [
            left_product(h_attn, grad_qkv).astype(low),
            left_product(grad_attn_branch, mixed_flat).astype(low),
        ],
        axis=1,
    )
    sum_last = scatter_sum(
        grad_w_attn.reshape(outer * inner, shard_rows, -1),
        lanes,
        True,
        ("inner",),
        ("inner",),
        8,
    )
    sum_out = sum_last[:, qkv_cols:].T
    sum_query = sum_last[:, :query_cols]
    sum_key = sum_last[:, query_cols : query_cols + key_cols]
    sum_value = sum_last[:, query_cols + key_cols : qkv_cols]
    return (
        layer_output,
        input_grad,
        sum_attn_in,
        sum_query,
        sum_key,
        sum_value,
        sum_out,
        sum_attn_out,
        sum_ffn_in,
        sum_gate,
        sum_up,
        sum_down,
        sum_ffn_out,
    )


def solution(mesh):
    dp_size, tensor = mesh.shape["dp"], mesh.shape["tensor"]
    outer = math.gcd(4, dp_size)
    lanes = (outer, dp_size // outer, tensor)
    split = Mesh(mesh.devices.reshape(lanes), ("outer", "inner", "tensor"))
    dp = ("outer", "inner")

    def run(*args):
        return jax.shard_map(
            lambda *blocks: shards(lanes, *blocks),
            mesh=split,
            in_specs=(
                P(dp, None),
                P(dp, None),
                P(dp, None),
                P(),
                P(dp, "tensor"),
                P(dp, "tensor"),
                P(dp, "tensor"),
                P("tensor", dp),
                P(),
                P(),
                P(dp, "tensor"),
                P(dp, "tensor"),
                P("tensor", dp),
                P(),
            ),
            out_specs=(
                P(dp, None),
                P(dp, None),
                P(dp),
                P(dp, "tensor"),
                P(dp, "tensor"),
                P(dp, "tensor"),
                P("tensor", dp),
                P(dp),
                P(dp),
                P(dp, "tensor"),
                P(dp, "tensor"),
                P("tensor", dp),
                P(dp),
            ),
            check_vma=False,
        )(*args)

    return run
```

```python
import functools
import math

import jax
import jax.numpy as jnp
from jax import lax
from jax.experimental import pallas as pl
from jax.experimental.pallas import tpu as pltpu
from jax.sharding import Mesh, PartitionSpec as P

H = 8
KV = 4
HD = 256


EPSILON = 1e-06
SOFT_CAP = 50.0
QUERY_SCALE = 0.0625
GELU_COEFF = 0.7978845608028654

MESH = pl.DeviceIdType.MESH


def rms_scale(values, scales):
    return values * lax.rsqrt(jnp.mean(values * values, axis=-1, keepdims=True) + EPSILON) * scales


def gelu_tanh(inputs):
    return (
        0.5 * inputs * (1.0 + jnp.tanh(GELU_COEFF * (inputs + 0.044715 * inputs * inputs * inputs)))
    )


def rotate_half(heads):
    middle = heads.shape[-1] // 2
    return jnp.concatenate([-heads[..., middle:], heads[..., :middle]], axis=-1)


def layout(lengths, row_count):
    seq_ends = jnp.cumsum(lengths)
    row_index = jnp.arange(row_count, dtype=jnp.int32)
    passed = (row_index[:, None] >= seq_ends[None, :]).astype(jnp.int32)
    segment = jnp.sum(passed, axis=1)
    is_live = row_index < seq_ends[-1]
    seq_ident = jnp.where(is_live, segment, lengths.shape[0] + row_index)
    offset = row_index - jnp.sum(passed * lengths[None, :], axis=1)
    allowed = (seq_ident[:, None] == seq_ident[None, :]) & (
        row_index[None, :] <= row_index[:, None]
    )
    middle = HD // 2
    inverse = jnp.exp(jnp.arange(middle, dtype=jnp.float32) * (-2.0 * math.log(10000.0) / HD))
    angles = offset.astype(jnp.float32)[:, None] * inverse[None, :]
    cosine = jnp.concatenate([jnp.cos(angles), jnp.cos(angles)], axis=1)
    sine_wave = jnp.concatenate([jnp.sin(angles), jnp.sin(angles)], axis=1)
    return (is_live, allowed, cosine, sine_wave)


def matmul(left, right):
    return jnp.dot(left, right, preferred_element_type=jnp.float32)


def right_product(left, right):
    return jnp.einsum("tc,dc->td", left, right, preferred_element_type=jnp.float32)


def capped_scores(query, keys):
    raw_scores = jnp.einsum("kgqd,ksd->kgqs", query, keys, preferred_element_type=jnp.float32)
    return SOFT_CAP * jnp.tanh(raw_scores / SOFT_CAP)


def pick(blocks, index):
    return lax.dynamic_index_in_dim(blocks, index, 0, keepdims=False)


def swap_blocks(blocks, axis):
    size = blocks.shape[0]
    here = lax.axis_index(axis)
    result = lax.dynamic_update_index_in_dim(
        jnp.zeros_like(blocks), pick(blocks, here), here, 0
    )
    for step in range(1, size):
        came = lax.ppermute(
            pick(blocks, lax.rem(here + step, size)),
            axis,
            [(i, (i + step) % size) for i in range(size)],
        )
        result = lax.dynamic_update_index_in_dim(
            result, came, lax.rem(here - step + size, size), 0
        )
    return result


def collect(block, axis, size):
    here = lax.axis_index(axis)
    result = jnp.zeros((size,) + block.shape, block.dtype)
    result = lax.dynamic_update_index_in_dim(result, block, here, 0)
    for step in range(1, size):
        came = lax.ppermute(block, axis, [(i, (i + step) % size) for i in range(size)])
        result = lax.dynamic_update_index_in_dim(
            result, came, lax.rem(here - step + size, size), 0
        )
    return result


def sum_blocks(blocks, axis):
    size = blocks.shape[0]
    here = lax.axis_index(axis)
    total = pick(blocks, here).astype(jnp.float32)
    for step in range(1, size):
        came = lax.ppermute(
            pick(blocks, lax.rem(here + step, size)),
            axis,
            [(i, (i + step) % size) for i in range(size)],
        )
        total = total + came.astype(jnp.float32)
    return total


def device_layout(lanes):
    _, inner, tensor = lanes
    cores = 2 if tensor % 2 == 0 else 1
    return {"inner": inner, "x": tensor // cores, "core": cores}


class Spot:
    def __init__(self, lanes, chain, levels):
        self.sizes = device_layout(lanes)
        self.chain, self.levels = chain, levels
        self.length = lanes[0] if chain else 1
        self.at_chain = lax.axis_index("outer")
        tensor = lax.axis_index("tensor")
        cores = self.sizes["core"]
        self.here = {
            "inner": lax.axis_index("inner"),
            "x": lax.div(tensor, cores),
            "core": lax.rem(tensor, cores),
        }
        self.step = self.at_chain if chain else 0
        self.slots = {}
        for level in levels:
            for shift in range(1, self.sizes[level]):
                self.slots[level, shift] = 2 + len(self.slots)

    def moved(self, **shifts):
        at = dict(self.here)
        for level, shift in shifts.items():
            at[level] = lax.rem(at[level] + shift, self.sizes[level])
        return at

    def device(self, at, chain_shift=0):
        return (
            self.at_chain + chain_shift,
            at["inner"],
            at["x"] * self.sizes["core"] + at["core"],
        )

    def flat(self, step, at):
        index = step
        for level in self.levels:
            index = index * self.sizes[level] + at[level]
        return index

    def greet(self):
        barrier = pltpu.get_barrier_semaphore()
        count = 0
        for level in self.levels:
            for shift in range(1, self.sizes[level]):
                pl.semaphore_signal(
                    barrier, device_id=self.device(self.moved(**{level: shift})), device_id_type=MESH
                )
                count += 1
        if self.length > 1:
            for shift, there in ((-1, self.step > 0), (1, self.step < self.length - 1)):
                count = count + there.astype(jnp.int32)

                @pl.when(there)
                def _(shift=shift):
                    pl.semaphore_signal(
                        barrier, device_id=self.device(self.here, shift), device_id_type=MESH
                    )

        pl.semaphore_wait(barrier, count)


def guarded(condition, action):
    if condition is None:
        action()
    else:
        pl.when(condition)(action)


def both(first, second):
    if first is None:
        return second
    return first if second is None else jnp.logical_and(first, second)


def gather_kernel(lanes, chain, levels, x_ref, o_ref, send_sem, recv_sem, local_sem):
    spot = Spot(lanes, chain, levels)
    length, step, here = spot.length, spot.step, spot.here
    started = []

    def send(condition, source, index, slot, device):
        def copy():
            return pltpu.make_async_remote_copy(
                src_ref=source,
                dst_ref=o_ref.at[index],
                send_sem=send_sem.at[slot, index],
                recv_sem=recv_sem.at[index],
                device_id=device,
                device_id_type=MESH,
            )

        guarded(condition, lambda: copy().start())
        started.append((condition, copy))

    def arrive(condition, index):
        def wait():
            pltpu.make_async_remote_copy(
                src_ref=o_ref.at[index],
                dst_ref=o_ref.at[index],
                send_sem=send_sem.at[0, index],
                recv_sem=recv_sem.at[index],
                device_id=spot.device(here),
                device_id_type=MESH,
            ).wait_recv()

        guarded(condition, wait)

    def spread(condition, source, index, first):
        for level in levels[first:]:
            for shift in range(1, spot.sizes[level]):
                send(
                    condition,
                    source,
                    index,
                    spot.slots[level, shift],
                    spot.device(spot.moved(**{level: shift})),
                )

    def around(distance):
        if distance == 0:
            return [(None, step)]
        return [(step - distance >= 0, step - distance), (step + distance < length, step + distance)]

    def clipped(position):
        return lax.rem(position + length, length) if length > 1 else position

    spot.greet()
    mine = spot.flat(step, here)
    local = pltpu.make_async_copy(x_ref, o_ref.at[mine], local_sem)
    local.start()
    if length > 1:
        send(step < length - 1, x_ref, mine, 1, spot.device(here, 1))
        send(step > 0, x_ref, mine, 0, spot.device(here, -1))
    spread(None, x_ref, mine, 0)

    def relay(distance):
        if len(levels) < 2:
            return
        level = levels[0]
        for there, position in around(distance):
            for shift in range(1, spot.sizes[level]):
                index = spot.flat(clipped(position), spot.moved(**{level: shift}))
                arrive(there, index)
                spread(there, o_ref.at[index], index, 1)

    for distance in range(1, length):
        for way, (there, position) in enumerate(around(distance)):
            index = spot.flat(clipped(position), here)
            arrive(there, index)
            onward = step < length - 1 if way == 0 else step > 0
            send(
                both(there, onward),
                o_ref.at[index],
                index,
                1 - way,
                spot.device(here, 1 if way == 0 else -1),
            )
            spread(there, o_ref.at[index], index, 0)
        relay(distance - 1)
    relay(length - 1)
    last = levels[-1]
    others = [{}]
    for level in levels[:-1]:
        others = [{**rest, level: shift} for rest in others for shift in range(spot.sizes[level])]
    for position in range(length):
        for rest in others:
            for shift in range(1, spot.sizes[last]):
                arrive(None, spot.flat(position, spot.moved(**{**rest, last: shift})))
    for condition, copy in started:
        guarded(condition, lambda copy=copy: copy().wait_send())
    local.wait()


def gather_blocks(block, lanes, chain, levels, collective_id):
    sizes = device_layout(lanes)
    count = (lanes[0] if chain else 1) * math.prod(sizes[level] for level in levels)
    slots = 2 + sum(sizes[level] - 1 for level in levels)
    return pl.pallas_call(
        functools.partial(gather_kernel, lanes, chain, levels),
        out_shape=jax.ShapeDtypeStruct((count,) + block.shape, block.dtype),
        in_specs=[pl.BlockSpec(memory_space=pltpu.VMEM)],
        out_specs=pl.BlockSpec(memory_space=pl.ANY),
        scratch_shapes=[
            pltpu.SemaphoreType.DMA((slots, count)),
            pltpu.SemaphoreType.DMA((count,)),
            pltpu.SemaphoreType.DMA,
        ],
        compiler_params=pltpu.CompilerParams(collective_id=collective_id, has_side_effects=True),
        cost_estimate=pl.CostEstimate(
            flops=0, bytes_accessed=20 * count * block.size, transcendentals=0
        ),
    )(block)


def add_into(target, parts, condition=None):
    rows = target.shape[0]
    tile = math.gcd(rows, 16)

    def action():
        def body(r, carry):
            window = pl.ds(pl.multiple_of(r * tile, tile), tile)
            total = parts[0][window, :].astype(jnp.float32)
            for part in parts[1:]:
                total = total + part[window, :].astype(jnp.float32)
            target[window, :] = total.astype(target.dtype)
            return carry

        lax.fori_loop(0, rows // tile, body, 0)

    guarded(condition, action)


def scatter_kernel(
    lanes, chain, levels, order, x_ref, o_ref, came0, came1, held0, held1, chained, sems, got0, got1, gotc
):
    spot = Spot(lanes, chain, levels)
    length, step, here = spot.length, spot.step, spot.here
    started = []

    def send(condition, source, target, send_at, recv_at, device):
        def copy():
            return pltpu.make_async_remote_copy(
                src_ref=source,
                dst_ref=target,
                send_sem=send_at,
                recv_sem=recv_at,
                device_id=device,
                device_id_type=MESH,
            )

        guarded(condition, lambda: copy().start())
        started.append((condition, copy))

    def arrive(condition, target, recv_at):
        def wait():
            pltpu.make_async_remote_copy(
                src_ref=target,
                dst_ref=target,
                send_sem=recv_at,
                recv_sem=recv_at,
                device_id=spot.device(here),
                device_id_type=MESH,
            ).wait_recv()

        guarded(condition, wait)

    visits = []
    for distance in range(length - 1, -1, -1):
        if distance == 0:
            visits.append((None, step, 0))
        else:
            visits.append(
                (step - distance >= 0, lax.rem(step - distance + length, length), -1)
            )
            visits.append((step + distance < length, lax.rem(step + distance, length), 1))

    spot.greet()
    first = order[0]
    second = order[1] if len(order) > 1 else None
    n_first = spot.sizes[first]
    n_second = spot.sizes[second] if second else 1

    def second_shifts(own):
        return [0] if own else list(range(1, n_second))

    for own in (False, True):
        for there, position, _ in visits:
            for other in second_shifts(own):
                for shift in range(1, n_first):
                    where = {first: shift}
                    if second:
                        where[second] = other
                    at = spot.moved(**where)
                    lane = position * n_second + (at[second] if second else 0)
                    send(
                        there,
                        x_ref.at[spot.flat(position, at)],
                        came0.at[shift - 1, lane],
                        sems.at[shift - 1, lane],
                        got0.at[shift - 1, lane],
                        spot.device(spot.moved(**{first: shift})),
                    )

    def first_sum(there, position, other):
        at = spot.moved(**({second: other} if second else {}))
        lane = position * n_second + (at[second] if second else 0)
        parts = [x_ref.at[spot.flat(position, at)]]
        for shift in range(1, n_first):
            arrive(there, came0.at[shift - 1, lane], got0.at[shift - 1, lane])
            parts.append(came0.at[shift - 1, lane])
        return parts

    for there, position, _ in visits:
        for other in second_shifts(False):
            parts = first_sum(there, position, other)
            add_into(held0.at[other - 1, position], parts, there)
            send(
                there,
                held0.at[other - 1, position],
                came1.at[other - 1, position],
                sems.at[n_first - 1 + other - 1, position],
                got1.at[other - 1, position],
                spot.device(spot.moved(**{second: other})),
            )
    base = n_first - 1 + n_second - 1
    for there, position, way in visits:
        parts = first_sum(there, position, 0)
        for other in second_shifts(False):
            arrive(there, came1.at[other - 1, position], got1.at[other - 1, position])
            parts.append(came1.at[other - 1, position])
        if way == 0:
            if length > 1:
                for side, exists in ((0, step > 0), (1, step < length - 1)):
                    arrive(exists, chained.at[side, position], gotc.at[side, position])

                def extra(sides):
                    return parts + [chained.at[side, position] for side in sides]

                inside = jnp.logical_and(step > 0, step < length - 1)
                add_into(o_ref, extra((0, 1)), inside)
                add_into(o_ref, extra((1,)), step == 0)
                add_into(o_ref, extra((0,)), step == length - 1)
            else:
                add_into(o_ref, parts)
        else:
            side = 1 if way == -1 else 0
            inner_link = step < length - 1 if way == -1 else step > 0
            with_more = both(there, inner_link)
            alone = both(there, jnp.logical_not(inner_link))
            arrive(with_more, chained.at[side, position], gotc.at[side, position])
            add_into(held1.at[position], parts + [chained.at[side, position]], with_more)
            add_into(held1.at[position], parts, alone)
            send(
                there,
                held1.at[position],
                chained.at[side, position],
                sems.at[base, position],
                gotc.at[side, position],
                spot.device(here, way),
            )
    for condition, copy in started:
        guarded(condition, lambda copy=copy: copy().wait_send())


def scatter_sum(blocks, lanes, chain, levels, order, collective_id, kind=jnp.float32):
    sizes = device_layout(lanes)
    length = lanes[0] if chain else 1
    rows, columns = blocks.shape[1:]
    low = blocks.dtype
    n_first = sizes[order[0]]
    n_second = sizes[order[1]] if len(order) > 1 else 1
    extra = max(n_first - 1, 1)
    further = max(n_second - 1, 1)
    return pl.pallas_call(
        functools.partial(scatter_kernel, lanes, chain, levels, order),
        out_shape=jax.ShapeDtypeStruct((rows, columns), kind),
        in_specs=[pl.BlockSpec(memory_space=pltpu.VMEM)],
        out_specs=pl.BlockSpec(memory_space=pltpu.VMEM),
        scratch_shapes=[
            pltpu.VMEM((extra, length * n_second, rows, columns), low),
            pltpu.VMEM((further, length, rows, columns), low),
            pltpu.VMEM((further, length, rows, columns), low),
            pltpu.VMEM((length, rows, columns), low),
            pltpu.VMEM((2, length, rows, columns), low),
            pltpu.SemaphoreType.DMA((n_first + n_second, length * n_second)),
            pltpu.SemaphoreType.DMA((extra, length * n_second)),
            pltpu.SemaphoreType.DMA((further, length)),
            pltpu.SemaphoreType.DMA((2, length)),
        ],
        compiler_params=pltpu.CompilerParams(collective_id=collective_id, has_side_effects=True),
        cost_estimate=pl.CostEstimate(
            flops=0, bytes_accessed=20 * blocks.size, transcendentals=0
        ),
    )(blocks)


def weight_grads_kernel(h_ref, g_ref, both_ref, hidden_ref, o_ref):
    turned = (((0,), (0,)), ((), ()))
    wide = both_ref.shape[1]
    o_ref[:, :wide] = lax.dot_general(
        h_ref[...], both_ref[...], turned, preferred_element_type=jnp.float32
    ).astype(o_ref.dtype)
    o_ref[:, wide:] = lax.dot_general(
        g_ref[...], hidden_ref[...], turned, preferred_element_type=jnp.float32
    ).astype(o_ref.dtype)


def weight_grads(h_all, g_all, both, hidden):
    tokens, width = h_all.shape
    tile = math.gcd(width, 384)
    columns = both.shape[1] + hidden.shape[1]
    return pl.pallas_call(
        weight_grads_kernel,
        grid=(width // tile,),
        out_shape=jax.ShapeDtypeStruct((width, columns), h_all.dtype),
        in_specs=[
            pl.BlockSpec((tokens, tile), lambda i: (0, i)),
            pl.BlockSpec((tokens, tile), lambda i: (0, i)),
            pl.BlockSpec(both.shape, lambda i: (0, 0)),
            pl.BlockSpec(hidden.shape, lambda i: (0, 0)),
        ],
        out_specs=pl.BlockSpec((tile, columns), lambda i: (i, 0)),
        cost_estimate=pl.CostEstimate(
            flops=2 * tokens * width * columns,
            bytes_accessed=4 * tokens * width + 2 * width * columns,
            transcendentals=0,
        ),
    )(h_all, g_all, both, hidden)


def unpack_kernel(part, x_ref, gate_ref, up_ref, down_ref):
    for i in range(x_ref.shape[0]):
        columns = slice(i * part, (i + 1) * part)
        for j, target in enumerate((gate_ref, up_ref, down_ref)):
            target[:, columns] = x_ref[i, :, j * part : (j + 1) * part].astype(jnp.float32)


def unpack(blocks, part):
    count, rows, columns = blocks.shape
    tile = math.gcd(rows, 48)
    width = count * part
    return pl.pallas_call(
        functools.partial(unpack_kernel, part),
        grid=(rows // tile,),
        out_shape=[jax.ShapeDtypeStruct((rows, width), jnp.float32)] * 3,
        in_specs=[pl.BlockSpec((count, tile, columns), lambda i: (0, i, 0))],
        out_specs=[pl.BlockSpec((tile, width), lambda i: (i, 0))] * 3,
    )(blocks)


def finish_kernel(
    lanes, h_ref, a_ref, qkv_ref, mixed_ref, strip_ref, tail_ref,
    o_ref, tails_ref,
    made, came, held, chained, shared, total,
    send0, got0, sendc, gotc, sendt, gott, sends, gots, local_sem,
):
    outer, inner, tensor = lanes
    step = lax.axis_index("outer")
    row = lax.axis_index("inner")
    lane = lax.axis_index("tensor")
    rows = h_ref.shape[0] // (outer * inner)
    extra = strip_ref.shape[1]
    wide = qkv_ref.shape[1]
    left, right = step > 0, step < outer - 1

    def peer_row(shift):
        return lax.rem(row + shift, inner)

    def peer_lane(shift):
        return lax.rem(lane + shift, tensor)

    barrier = pltpu.get_barrier_semaphore()
    for shift in range(1, inner):
        pl.semaphore_signal(barrier, device_id=(step, peer_row(shift), lane), device_id_type=MESH)
    for shift in range(1, tensor):
        pl.semaphore_signal(barrier, device_id=(step, row, peer_lane(shift)), device_id_type=MESH)
    for there, move in ((left, -1), (right, 1)):

        @pl.when(there)
        def _(move=move):
            pl.semaphore_signal(barrier, device_id=(step + move, row, lane), device_id_type=MESH)

    pl.semaphore_wait(
        barrier, inner + tensor - 2 + left.astype(jnp.int32) + right.astype(jnp.int32)
    )

    def make(index):
        window = pl.ds(pl.multiple_of(index * rows, rows), rows)
        made[index, :rows, :wide] = jnp.dot(
            h_ref[window, :], qkv_ref[...], preferred_element_type=jnp.float32
        ).astype(made.dtype)
        made[index, :rows, wide:] = jnp.dot(
            a_ref[window, :], mixed_ref[...], preferred_element_type=jnp.float32
        ).astype(made.dtype)
        made[index, rows:, :] = strip_ref[index]

    def remote(source, target, send_at, recv_at, device):
        return pltpu.make_async_remote_copy(
            src_ref=source,
            dst_ref=target,
            send_sem=send_at,
            recv_sem=recv_at,
            device_id=device,
            device_id_type=MESH,
        )

    upper = (step * 2 >= outer).astype(jnp.int32)

    def place(j):
        return upper * j + (1 - upper) * (outer - 1 - j)

    def row_copy(k):
        shift = 1 + lax.div(k, outer)
        position = place(lax.rem(k, outer))
        there = peer_row(shift)
        return position * inner + there, remote(
            made.at[position * inner + there],
            came.at[shift - 1, position],
            send0.at[shift - 1, position],
            got0.at[shift - 1, position],
            (step, there, lane),
        )

    def first(k, carry):
        index, copy = row_copy(k)
        make(index)
        copy.start()
        return carry

    lax.fori_loop(0, outer * (inner - 1), first, 0)

    def tail_copy(shift):
        return remote(
            tail_ref,
            tails_ref.at[lane],
            sendt.at[shift - 1],
            gott.at[shift - 1],
            (step, row, peer_lane(shift)),
        )

    local = pltpu.make_async_copy(tail_ref, tails_ref.at[lane], local_sem)
    local.start()
    for shift in range(1, tensor):
        tail_copy(shift).start()

    def second(j, carry):
        make(place(j) * inner + row)
        return carry

    lax.fori_loop(0, outer, second, 0)

    visits = []
    for distance in range(outer - 1, -1, -1):
        if distance == 0:
            visits.append((None, step, 0))
        else:
            visits.append((step - distance >= 0, lax.rem(step - distance + outer, outer), -1))
            visits.append((step + distance < outer, lax.rem(step + distance, outer), 1))

    started = []
    for there, position, way in visits:
        parts = [made.at[position * inner + row]]
        for shift in range(1, inner):
            target = came.at[shift - 1, position]
            guarded(
                there,
                remote(
                    target,
                    target,
                    send0.at[shift - 1, position],
                    got0.at[shift - 1, position],
                    (step, row, lane),
                ).wait_recv,
            )
            parts.append(target)

        def linked(side, position=position):
            target = chained.at[side, position]
            return remote(
                target, target, sendc.at[position], gotc.at[side, position], (step, row, lane)
            )

        if way == 0:
            for side, exists in ((0, left), (1, right)):
                guarded(exists, linked(side).wait_recv)
            inside = jnp.logical_and(left, right)
            add_into(total, parts + [chained.at[0, position], chained.at[1, position]], inside)
            add_into(total, parts + [chained.at[1, position]], jnp.logical_not(left))
            add_into(total, parts + [chained.at[0, position]], jnp.logical_not(right))
        else:
            side = 1 if way == -1 else 0
            link = right if way == -1 else left
            more, alone = jnp.logical_and(there, link), jnp.logical_and(there, jnp.logical_not(link))
            guarded(more, linked(side).wait_recv)
            add_into(held.at[position], parts + [chained.at[side, position]], more)
            add_into(held.at[position], parts, alone)
            copy = remote(
                held.at[position],
                chained.at[side, position],
                sendc.at[position],
                gotc.at[side, position],
                (step + way, row, lane),
            )
            guarded(there, copy.start)
            started.append((there, copy))

    strip = total.at[pl.ds(rows, extra), :]
    small = [
        remote(
            strip,
            shared.at[shift - 1],
            sends.at[shift - 1],
            gots.at[shift - 1],
            (step, row, peer_lane(shift)),
        )
        for shift in range(1, tensor)
    ]
    for copy in small:
        copy.start()
    o_ref[pl.ds(0, rows), :] = total[pl.ds(0, rows), :]
    summed = total[pl.ds(rows, extra), :]
    for shift in range(1, tensor):
        small[shift - 1].wait_recv()
        summed = summed + shared[shift - 1]
    o_ref[pl.ds(rows, extra), :] = summed

    for shift in range(1, tensor):
        small[shift - 1].wait_send()
        tail_copy(shift).wait()
    for there, copy in started:
        guarded(there, copy.wait_send)

    def drain(k, carry):
        row_copy(k)[1].wait_send()
        return carry

    lax.fori_loop(0, outer * (inner - 1), drain, 0)
    local.wait()


def finish(lanes, h_turned, a_turned, grad_qkv, mixed, strips, tail, collective_id):
    outer, inner, tensor = lanes
    low = h_turned.dtype
    count, extra, columns = strips.shape
    rows = h_turned.shape[0] // count
    block = (rows + extra, columns)
    peers = max(inner - 1, 1)
    vmem = pl.BlockSpec(memory_space=pltpu.VMEM)
    dma = pltpu.SemaphoreType.DMA
    return pl.pallas_call(
        functools.partial(finish_kernel, lanes),
        out_shape=[
            jax.ShapeDtypeStruct(block, jnp.float32),
            jax.ShapeDtypeStruct((tensor,) + tail.shape, low),
        ],
        in_specs=[vmem] * 6,
        out_specs=[vmem, pl.BlockSpec(memory_space=pl.ANY)],
        scratch_shapes=[
            pltpu.VMEM((count,) + block, low),
            pltpu.VMEM((peers, outer) + block, low),
            pltpu.VMEM((outer,) + block, low),
            pltpu.VMEM((2, outer) + block, low),
            pltpu.VMEM((tensor - 1, extra, columns), jnp.float32),
            pltpu.VMEM(block, jnp.float32),
            dma((peers, outer)),
            dma((peers, outer)),
            dma((outer,)),
            dma((2, outer)),
            dma((tensor - 1,)),
            dma((tensor - 1,)),
            dma((tensor - 1,)),
            dma((tensor - 1,)),
            dma,
        ],
        compiler_params=pltpu.CompilerParams(collective_id=collective_id, has_side_effects=True),
        cost_estimate=pl.CostEstimate(
            flops=2 * h_turned.size * columns,
            bytes_accessed=20 * count * rows * columns,
            transcendentals=0,
        ),
    )(h_turned, a_turned, grad_qkv, mixed, strips, tail)


def shards(
    lanes,
    layer_input,
    cotangent,
    seq_lengths,
    norm_attn_in,
    w_query,
    w_key,
    w_value,
    w_out,
    norm_attn_out,
    norm_ffn_in,
    w_gate,
    w_up,
    w_down,
    norm_ffn_out,
):
    outer, inner, tensor = lanes
    low = jnp.bfloat16
    shard_rows, width = w_gate.shape
    part = width // outer
    query_cols, key_cols = w_query.shape[1], w_key.shape[1]
    qkv_cols = query_cols + 2 * key_cols

    attn_shard = jnp.concatenate([w_query, w_key, w_value, w_out.T], axis=1)
    attn_full = gather_blocks(attn_shard, lanes, True, ("inner",), 0)
    attn_full = attn_full.reshape(-1, attn_shard.shape[1])
    down_turned = w_down.T
    ffn_shard = jnp.stack(
        [
            jnp.concatenate(
                [item[:, i * part : (i + 1) * part] for item in (w_gate, w_up, down_turned)],
                axis=1,
            )
            for i in range(outer)
        ]
    )
    ffn_mine = swap_blocks(ffn_shard, "outer")
    attn_full, ffn_mine = lax.optimization_barrier((attn_full, ffn_mine))
    ffn_full = collect(ffn_mine, "inner", inner).transpose(1, 0, 2, 3).reshape(-1, 3 * part)

    row_count = layer_input.shape[0]
    split_rows = row_count // tensor
    first_row = lax.axis_index("tensor") * split_rows

    def own_rows(array):
        return lax.dynamic_slice_in_dim(array, first_row, split_rows, 0)

    is_live, allowed, cosine, sine_wave = layout(seq_lengths[0], row_count)
    kv_heads = key_cols // HD
    groups = H // KV
    layer_float = layer_input.astype(jnp.float32)
    h_attn = rms_scale(layer_float, norm_attn_in).astype(low)
    projected = matmul(h_attn, attn_full[:, :qkv_cols])
    query_pre = (
        projected[:, :query_cols].reshape(row_count, kv_heads, groups, HD).transpose(1, 2, 0, 3)
    )
    query = ((query_pre * cosine + rotate_half(query_pre) * sine_wave) * QUERY_SCALE).astype(low)
    key_pre = (
        projected[:, query_cols : query_cols + key_cols]
        .reshape(row_count, kv_heads, HD)
        .transpose(1, 0, 2)
    )
    keys = (key_pre * cosine + rotate_half(key_pre) * sine_wave).astype(low)
    values = (
        projected[:, query_cols + key_cols :]
        .astype(low)
        .reshape(row_count, kv_heads, HD)
        .transpose(1, 0, 2)
    )
    capped = capped_scores(query, keys)
    expo = jnp.where(allowed, jnp.exp(capped), 0.0)
    log_total = jnp.log(jnp.sum(expo, axis=-1, keepdims=True))
    weights = jnp.where(allowed, jnp.exp(capped - log_total), 0.0)
    probs = weights.astype(low)
    mixed = jnp.einsum("kgqs,ksd->kgqd", probs, values, preferred_element_type=jnp.float32).astype(
        low
    )
    mixed_flat = mixed.transpose(2, 0, 1, 3).reshape(row_count, -1)
    out_turned = attn_full[:, qkv_cols:]
    attn_branch = scatter_sum(
        right_product(mixed_flat, out_turned).astype(low).reshape(tensor, split_rows, -1),
        lanes,
        False,
        ("x", "core"),
        ("core", "x"),
        1,
    )
    layer_own = own_rows(layer_float)
    resid = layer_own + rms_scale(attn_branch, norm_attn_out)
    h_ffn = rms_scale(resid, norm_ffn_in).astype(low)

    h_all = gather_blocks(h_ffn, lanes, True, ("x", "core"), 2).reshape(-1, h_ffn.shape[1])
    gate_up = matmul(h_all, ffn_full[:, : 2 * part])
    gate_pre, up_pre = gate_up[:, :part], gate_up[:, part:]
    gelu_gate = gelu_tanh(gate_pre)
    hidden = (gelu_gate * up_pre).astype(low)
    down_full = ffn_full[:, 2 * part :]
    ffn_branch = scatter_sum(
        right_product(hidden, down_full).astype(low).reshape(outer * tensor, split_rows, -1),
        lanes,
        True,
        ("x", "core"),
        ("core", "x"),
        3,
    )
    output_own = (resid + rms_scale(ffn_branch, norm_ffn_out)).astype(low)

    grad_out = own_rows(cotangent).astype(jnp.float32) * own_rows(
        is_live.astype(jnp.float32)[:, None]
    )
    _, pull_four = jax.vjp(rms_scale, ffn_branch, norm_ffn_out)
    grad_ffn_float, grad_norm_ffn_out = pull_four(grad_out)
    grad_ffn_all = gather_blocks(grad_ffn_float.astype(low), lanes, True, ("x", "core"), 4)
    grad_ffn_all = grad_ffn_all.reshape(-1, h_ffn.shape[1])
    grad_hidden = matmul(grad_ffn_all, down_full)
    grad_up = (grad_hidden * gelu_gate).astype(low)
    _, pull_gelu = jax.vjp(gelu_tanh, gate_pre)
    grad_gate = pull_gelu(grad_hidden * up_pre)[0].astype(low)
    grad_both = jnp.concatenate([grad_gate, grad_up], axis=1)
    grad_h_part = right_product(grad_both, ffn_full[:, : 2 * part]).astype(low)
    grad_h_ffn = scatter_sum(
        grad_h_part.reshape(outer * tensor, split_rows, -1),
        lanes,
        True,
        ("x", "core"),
        ("core", "x"),
        5,
    )
    grad_w_ffn = weight_grads(h_all, grad_ffn_all, grad_both, hidden)
    grad_w_ffn = grad_w_ffn.reshape(outer, inner, shard_rows, 3 * part).transpose(1, 0, 2, 3)
    grad_w_ffn = sum_blocks(grad_w_ffn, "inner").astype(low)
    grad_w_ffn = swap_blocks(grad_w_ffn, "outer")
    sum_gate, sum_up, sum_down = unpack(grad_w_ffn, part)
    sum_down = sum_down.T

    _, pull_three = jax.vjp(rms_scale, resid, norm_ffn_in)
    grad_resid_part, grad_norm_ffn_in = pull_three(grad_h_ffn)
    grad_resid = grad_out + grad_resid_part
    _, pull_two = jax.vjp(rms_scale, attn_branch, norm_attn_out)
    grad_attn_float, grad_norm_attn_out = pull_two(grad_resid)
    grad_attn_branch = gather_blocks(
        grad_attn_float.astype(low), lanes, False, ("x", "core"), 6
    ).reshape(row_count, -1)
    grad_mixed = matmul(grad_attn_branch, out_turned).astype(low)
    grad_mixed = grad_mixed.reshape(row_count, kv_heads, groups, HD).transpose(1, 2, 0, 3)
    grad_values = jnp.einsum(
        "kgqs,kgqd->ksd", probs, grad_mixed, preferred_element_type=jnp.float32
    ).astype(low)
    grad_probs = jnp.einsum(
        "kgqd,ksd->kgqs", grad_mixed, values, preferred_element_type=jnp.float32
    )
    row_delta = jnp.sum(weights * grad_probs, axis=-1, keepdims=True)
    tanh_part = capped / SOFT_CAP
    grad_scores = (weights * (grad_probs - row_delta) * (1.0 - tanh_part * tanh_part)).astype(low)
    grad_query_raw = jnp.einsum(
        "kgqs,ksd->kgqd", grad_scores, keys, preferred_element_type=jnp.float32
    )
    grad_query = (
        (grad_query_raw * cosine - rotate_half(grad_query_raw) * sine_wave) * QUERY_SCALE
    ).astype(low)
    grad_keys_raw = jnp.einsum(
        "kgqs,kgqd->ksd", grad_scores, query, preferred_element_type=jnp.float32
    )
    grad_keys = (grad_keys_raw * cosine - rotate_half(grad_keys_raw) * sine_wave).astype(low)
    grad_qkv = jnp.concatenate(
        [
            grad_query.transpose(2, 0, 1, 3).reshape(row_count, -1),
            grad_keys.transpose(1, 0, 2).reshape(row_count, -1),
            grad_values.transpose(1, 0, 2).reshape(row_count, -1),
        ],
        axis=1,
    )
    grad_a_part = right_product(grad_qkv, attn_full[:, :qkv_cols]).astype(low)
    grad_h_attn = scatter_sum(
        grad_a_part.reshape(tensor, split_rows, -1),
        lanes,
        False,
        ("x", "core"),
        ("core", "x"),
        7,
    )
    _, pull_one = jax.vjp(rms_scale, layer_own, norm_attn_in)
    grad_input_part, grad_norm_attn_in = pull_one(grad_h_attn)
    input_own = grad_resid + grad_input_part

    norm_rows = jnp.stack(
        [grad_norm_attn_in, grad_norm_attn_out, grad_norm_ffn_in, grad_norm_ffn_out]
    )
    strips = norm_rows.reshape(4, outer * inner, shard_rows).transpose(1, 0, 2)
    strips = strips.reshape(outer * inner, 1, -1).astype(low)
    attn_cols = attn_shard.shape[1]
    strips = jnp.pad(strips, ((0, 0), (0, 15), (0, attn_cols - strips.shape[2])))
    tail = jnp.concatenate([output_own, input_own.astype(low)], axis=0)
    sum_last, tails = finish(
        lanes, h_attn.T, grad_attn_branch.T, grad_qkv, mixed_flat, strips, tail, 8
    )
    layer_output = tails[:, :split_rows].reshape(row_count, -1)
    input_grad = tails[:, split_rows:].reshape(row_count, -1).astype(jnp.float32)
    sum_attn_in, sum_attn_out, sum_ffn_in, sum_ffn_out = (
        sum_last[shard_rows, i * shard_rows : (i + 1) * shard_rows] for i in range(4)
    )
    sum_last = sum_last[:shard_rows]
    sum_out = sum_last[:, qkv_cols:].T
    sum_query = sum_last[:, :query_cols]
    sum_key = sum_last[:, query_cols : query_cols + key_cols]
    sum_value = sum_last[:, query_cols + key_cols : qkv_cols]
    return (
        layer_output,
        input_grad,
        sum_attn_in,
        sum_query,
        sum_key,
        sum_value,
        sum_out,
        sum_attn_out,
        sum_ffn_in,
        sum_gate,
        sum_up,
        sum_down,
        sum_ffn_out,
    )


def solution(mesh):
    dp_size, tensor = mesh.shape["dp"], mesh.shape["tensor"]
    outer = math.gcd(4, dp_size)
    lanes = (outer, dp_size // outer, tensor)
    split = Mesh(mesh.devices.reshape(lanes), ("outer", "inner", "tensor"))
    dp = ("outer", "inner")

    def run(*args):
        return jax.shard_map(
            lambda *blocks: shards(lanes, *blocks),
            mesh=split,
            in_specs=(
                P(dp, None),
                P(dp, None),
                P(dp, None),
                P(),
                P(dp, "tensor"),
                P(dp, "tensor"),
                P(dp, "tensor"),
                P("tensor", dp),
                P(),
                P(),
                P(dp, "tensor"),
                P(dp, "tensor"),
                P("tensor", dp),
                P(),
            ),
            out_specs=(
                P(dp, None),
                P(dp, None),
                P(dp),
                P(dp, "tensor"),
                P(dp, "tensor"),
                P(dp, "tensor"),
                P("tensor", dp),
                P(dp),
                P(dp),
                P(dp, "tensor"),
                P(dp, "tensor"),
                P("tensor", dp),
                P(dp),
            ),
            check_vma=False,
        )(*args)

    return run
```

```python
import functools
import math

import jax
import jax.numpy as jnp
from jax import lax
from jax.experimental import pallas as pl
from jax.experimental.pallas import tpu as pltpu
from jax.sharding import Mesh, PartitionSpec as P

H = 8
KV = 4
HD = 256


EPSILON = 1e-06
SOFT_CAP = 50.0
QUERY_SCALE = 0.0625
GELU_COEFF = 0.7978845608028654

MESH = pl.DeviceIdType.MESH


def rms_scale(values, scales):
    return values * lax.rsqrt(jnp.mean(values * values, axis=-1, keepdims=True) + EPSILON) * scales


def gelu_tanh(inputs):
    return (
        0.5 * inputs * (1.0 + jnp.tanh(GELU_COEFF * (inputs + 0.044715 * inputs * inputs * inputs)))
    )


def rotate_half(heads):
    middle = heads.shape[-1] // 2
    return jnp.concatenate([-heads[..., middle:], heads[..., :middle]], axis=-1)


def layout(lengths, row_count):
    seq_ends = jnp.cumsum(lengths)
    row_index = jnp.arange(row_count, dtype=jnp.int32)
    passed = (row_index[:, None] >= seq_ends[None, :]).astype(jnp.int32)
    segment = jnp.sum(passed, axis=1)
    is_live = row_index < seq_ends[-1]
    seq_ident = jnp.where(is_live, segment, lengths.shape[0] + row_index)
    offset = row_index - jnp.sum(passed * lengths[None, :], axis=1)
    allowed = (seq_ident[:, None] == seq_ident[None, :]) & (
        row_index[None, :] <= row_index[:, None]
    )
    middle = HD // 2
    inverse = jnp.exp(jnp.arange(middle, dtype=jnp.float32) * (-2.0 * math.log(10000.0) / HD))
    angles = offset.astype(jnp.float32)[:, None] * inverse[None, :]
    cosine = jnp.concatenate([jnp.cos(angles), jnp.cos(angles)], axis=1)
    sine_wave = jnp.concatenate([jnp.sin(angles), jnp.sin(angles)], axis=1)
    return (is_live, allowed, cosine, sine_wave)


def matmul(left, right):
    return jnp.dot(left, right, preferred_element_type=jnp.float32)


def right_product(left, right):
    return jnp.einsum("tc,dc->td", left, right, preferred_element_type=jnp.float32)


def capped_scores(query, keys):
    raw_scores = jnp.einsum("kgqd,ksd->kgqs", query, keys, preferred_element_type=jnp.float32)
    return SOFT_CAP * jnp.tanh(raw_scores / SOFT_CAP)


def shifted(block, axis, size, step):
    return lax.ppermute(block, axis, [(i, (i + step) % size) for i in range(size)])


def pack_kernel(part, g_ref, u_ref, d_ref, *o_refs):
    count = len(o_refs)
    here = lax.axis_index("outer")
    tile = math.gcd(g_ref.shape[0], 16)
    for step, o_ref in enumerate(o_refs):
        for source in range(count):

            @pl.when(lax.rem(here + step, count) == source)
            def _(o_ref=o_ref, source=source):
                def body(r, carry):
                    window = pl.ds(pl.multiple_of(r * tile, tile), tile)
                    for j, ref in enumerate((g_ref, u_ref, d_ref)):
                        o_ref[window, j * part : (j + 1) * part] = ref[
                            window, source * part : (source + 1) * part
                        ]
                    return carry

                lax.fori_loop(0, g_ref.shape[0] // tile, body, 0)


def pack(count, part, gate, up, down_turned):
    vmem = pl.BlockSpec(memory_space=pltpu.VMEM)
    return pl.pallas_call(
        functools.partial(pack_kernel, part),
        out_shape=[jax.ShapeDtypeStruct((gate.shape[0], 3 * part), gate.dtype)] * count,
        in_specs=[vmem] * 3,
        out_specs=[vmem] * count,
        cost_estimate=pl.CostEstimate(
            flops=0, bytes_accessed=12 * gate.size, transcendentals=0
        ),
    )(gate, up, down_turned)


def device_layout(lanes):
    _, inner, tensor = lanes
    cores = 2 if tensor % 2 == 0 else 1
    return {"inner": inner, "x": tensor // cores, "core": cores}


class Spot:
    def __init__(self, lanes, chain, levels):
        self.sizes = device_layout(lanes)
        self.chain, self.levels = chain, levels
        self.length = lanes[0] if chain else 1
        self.at_chain = lax.axis_index("outer")
        tensor = lax.axis_index("tensor")
        cores = self.sizes["core"]
        self.here = {
            "inner": lax.axis_index("inner"),
            "x": lax.div(tensor, cores),
            "core": lax.rem(tensor, cores),
        }
        self.step = self.at_chain if chain else 0
        self.slots = {}
        for level in levels:
            for shift in range(1, self.sizes[level]):
                self.slots[level, shift] = 2 + len(self.slots)

    def moved(self, **shifts):
        at = dict(self.here)
        for level, shift in shifts.items():
            at[level] = lax.rem(at[level] + shift, self.sizes[level])
        return at

    def device(self, at, chain_shift=0):
        return (
            self.at_chain + chain_shift,
            at["inner"],
            at["x"] * self.sizes["core"] + at["core"],
        )

    def flat(self, step, at):
        index = step
        for level in self.levels:
            index = index * self.sizes[level] + at[level]
        return index

    def greet(self):
        barrier = pltpu.get_barrier_semaphore()
        count = 0
        for level in self.levels:
            for shift in range(1, self.sizes[level]):
                pl.semaphore_signal(
                    barrier, device_id=self.device(self.moved(**{level: shift})), device_id_type=MESH
                )
                count += 1
        if self.length > 1:
            for shift, there in ((-1, self.step > 0), (1, self.step < self.length - 1)):
                count = count + there.astype(jnp.int32)

                @pl.when(there)
                def _(shift=shift):
                    pl.semaphore_signal(
                        barrier, device_id=self.device(self.here, shift), device_id_type=MESH
                    )

        pl.semaphore_wait(barrier, count)


def guarded(condition, action):
    if condition is None:
        action()
    else:
        pl.when(condition)(action)


def both(first, second):
    if first is None:
        return second
    return first if second is None else jnp.logical_and(first, second)


def gather_kernel(lanes, chain, levels, places, *refs):
    held_refs, refs = refs[1 : 1 + len(places)], refs[:1] + refs[1 + len(places) :]
    if places:
        x_ref, o_ref, placed_ref, send_sem, recv_sem, local_sem, place_sem = refs
    else:
        x_ref, o_ref, send_sem, recv_sem, local_sem = refs
    spot = Spot(lanes, chain, levels)
    length, step, here = spot.length, spot.step, spot.here
    started = []

    def send(condition, source, index, slot, device):
        def copy():
            return pltpu.make_async_remote_copy(
                src_ref=source,
                dst_ref=o_ref.at[index],
                send_sem=send_sem.at[slot, index],
                recv_sem=recv_sem.at[index],
                device_id=device,
                device_id_type=MESH,
            )

        guarded(condition, lambda: copy().start())
        started.append((condition, copy))

    def arrive(condition, index):
        def wait():
            pltpu.make_async_remote_copy(
                src_ref=o_ref.at[index],
                dst_ref=o_ref.at[index],
                send_sem=send_sem.at[0, index],
                recv_sem=recv_sem.at[index],
                device_id=spot.device(here),
                device_id_type=MESH,
            ).wait_recv()

        guarded(condition, wait)

    def spread(condition, source, index, first):
        for level in levels[first:]:
            for shift in range(1, spot.sizes[level]):
                send(
                    condition,
                    source,
                    index,
                    spot.slots[level, shift],
                    spot.device(spot.moved(**{level: shift})),
                )

    def around(distance):
        if distance == 0:
            return [(None, step)]
        return [(step - distance >= 0, step - distance), (step + distance < length, step + distance)]

    def clipped(position):
        return lax.rem(position + length, length) if length > 1 else position

    spot.greet()
    mine = spot.flat(step, here)
    local = pltpu.make_async_copy(x_ref, o_ref.at[mine], local_sem)
    local.start()
    if length > 1:
        send(step < length - 1, x_ref, mine, 1, spot.device(here, 1))
        send(step > 0, x_ref, mine, 0, spot.device(here, -1))
    spread(None, x_ref, mine, 0)

    outer, inner, _ = lanes
    moves = []
    for number, (back, turn) in enumerate(places):
        index = lax.rem(lax.axis_index("outer") - back + outer, outer) * inner
        index = index + lax.rem(lax.axis_index("inner") - turn + inner, inner)
        moves.append(
            pltpu.make_async_copy(
                held_refs[number], placed_ref.at[index], place_sem.at[number]
            )
        )
        moves[-1].start()

    def relay(distance):
        if len(levels) < 2:
            return
        level = levels[0]
        for there, position in around(distance):
            for shift in range(1, spot.sizes[level]):
                index = spot.flat(clipped(position), spot.moved(**{level: shift}))
                arrive(there, index)
                spread(there, o_ref.at[index], index, 1)

    for distance in range(1, length):
        for way, (there, position) in enumerate(around(distance)):
            index = spot.flat(clipped(position), here)
            arrive(there, index)
            onward = step < length - 1 if way == 0 else step > 0
            send(
                both(there, onward),
                o_ref.at[index],
                index,
                1 - way,
                spot.device(here, 1 if way == 0 else -1),
            )
            spread(there, o_ref.at[index], index, 0)
        relay(distance - 1)
    relay(length - 1)
    last = levels[-1]
    others = [{}]
    for level in levels[:-1]:
        others = [{**rest, level: shift} for rest in others for shift in range(spot.sizes[level])]
    for position in range(length):
        for rest in others:
            for shift in range(1, spot.sizes[last]):
                arrive(None, spot.flat(position, spot.moved(**{**rest, last: shift})))
    for condition, copy in started:
        guarded(condition, lambda copy=copy: copy().wait_send())
    for move in moves:
        move.wait()
    local.wait()


def gather_blocks(block, lanes, chain, levels, collective_id, held=None):
    held = held or {}
    places = tuple(held)
    blocks = [held[key] for key in places]
    sizes = device_layout(lanes)
    count = (lanes[0] if chain else 1) * math.prod(sizes[level] for level in levels)
    slots = 2 + sum(sizes[level] - 1 for level in levels)
    out_shape = [jax.ShapeDtypeStruct((count,) + block.shape, block.dtype)]
    scratch = [
        pltpu.SemaphoreType.DMA((slots, count)),
        pltpu.SemaphoreType.DMA((count,)),
        pltpu.SemaphoreType.DMA,
    ]
    if held:
        out_shape.append(
            jax.ShapeDtypeStruct((lanes[0] * lanes[1],) + blocks[0].shape, blocks[0].dtype)
        )
        scratch.append(pltpu.SemaphoreType.DMA((len(blocks),)))
    results = pl.pallas_call(
        functools.partial(gather_kernel, lanes, chain, levels, places),
        out_shape=out_shape,
        in_specs=[pl.BlockSpec(memory_space=pltpu.VMEM)] * (1 + len(blocks)),
        out_specs=[pl.BlockSpec(memory_space=pl.ANY)] * len(out_shape),
        scratch_shapes=scratch,
        compiler_params=pltpu.CompilerParams(collective_id=collective_id, has_side_effects=True),
        cost_estimate=pl.CostEstimate(
            flops=0, bytes_accessed=20 * count * block.size, transcendentals=0
        ),
    )(block, *blocks)
    return results if held else results[0]


def add_into(target, parts, condition=None):
    rows = target.shape[0]
    tile = math.gcd(rows, 16)

    def action():
        def body(r, carry):
            window = pl.ds(pl.multiple_of(r * tile, tile), tile)
            total = parts[0][window, :].astype(jnp.float32)
            for part in parts[1:]:
                total = total + part[window, :].astype(jnp.float32)
            target[window, :] = total.astype(target.dtype)
            return carry

        lax.fori_loop(0, rows // tile, body, 0)

    guarded(condition, action)


def scatter_kernel(
    lanes, chain, levels, order, x_ref, o_ref, came0, came1, held0, held1, chained, sems, got0, got1, gotc
):
    spot = Spot(lanes, chain, levels)
    length, step, here = spot.length, spot.step, spot.here
    started = []

    def send(condition, source, target, send_at, recv_at, device):
        def copy():
            return pltpu.make_async_remote_copy(
                src_ref=source,
                dst_ref=target,
                send_sem=send_at,
                recv_sem=recv_at,
                device_id=device,
                device_id_type=MESH,
            )

        guarded(condition, lambda: copy().start())
        started.append((condition, copy))

    def arrive(condition, target, recv_at):
        def wait():
            pltpu.make_async_remote_copy(
                src_ref=target,
                dst_ref=target,
                send_sem=recv_at,
                recv_sem=recv_at,
                device_id=spot.device(here),
                device_id_type=MESH,
            ).wait_recv()

        guarded(condition, wait)

    visits = []
    for distance in range(length - 1, -1, -1):
        if distance == 0:
            visits.append((None, step, 0))
        else:
            visits.append(
                (step - distance >= 0, lax.rem(step - distance + length, length), -1)
            )
            visits.append((step + distance < length, lax.rem(step + distance, length), 1))

    spot.greet()
    first = order[0]
    second = order[1] if len(order) > 1 else None
    n_first = spot.sizes[first]
    n_second = spot.sizes[second] if second else 1

    def second_shifts(own):
        return [0] if own else list(range(1, n_second))

    for own in (False, True):
        for there, position, _ in visits:
            for other in second_shifts(own):
                for shift in range(1, n_first):
                    where = {first: shift}
                    if second:
                        where[second] = other
                    at = spot.moved(**where)
                    lane = position * n_second + (at[second] if second else 0)
                    send(
                        there,
                        x_ref.at[spot.flat(position, at)],
                        came0.at[shift - 1, lane],
                        sems.at[shift - 1, lane],
                        got0.at[shift - 1, lane],
                        spot.device(spot.moved(**{first: shift})),
                    )

    def first_sum(there, position, other):
        at = spot.moved(**({second: other} if second else {}))
        lane = position * n_second + (at[second] if second else 0)
        parts = [x_ref.at[spot.flat(position, at)]]
        for shift in range(1, n_first):
            arrive(there, came0.at[shift - 1, lane], got0.at[shift - 1, lane])
            parts.append(came0.at[shift - 1, lane])
        return parts

    for there, position, _ in visits:
        for other in second_shifts(False):
            parts = first_sum(there, position, other)
            add_into(held0.at[other - 1, position], parts, there)
            send(
                there,
                held0.at[other - 1, position],
                came1.at[other - 1, position],
                sems.at[n_first - 1 + other - 1, position],
                got1.at[other - 1, position],
                spot.device(spot.moved(**{second: other})),
            )
    base = n_first - 1 + n_second - 1
    for there, position, way in visits:
        parts = first_sum(there, position, 0)
        for other in second_shifts(False):
            arrive(there, came1.at[other - 1, position], got1.at[other - 1, position])
            parts.append(came1.at[other - 1, position])
        if way == 0:
            if length > 1:
                for side, exists in ((0, step > 0), (1, step < length - 1)):
                    arrive(exists, chained.at[side, position], gotc.at[side, position])

                def extra(sides):
                    return parts + [chained.at[side, position] for side in sides]

                inside = jnp.logical_and(step > 0, step < length - 1)
                add_into(o_ref, extra((0, 1)), inside)
                add_into(o_ref, extra((1,)), step == 0)
                add_into(o_ref, extra((0,)), step == length - 1)
            else:
                add_into(o_ref, parts)
        else:
            side = 1 if way == -1 else 0
            inner_link = step < length - 1 if way == -1 else step > 0
            with_more = both(there, inner_link)
            alone = both(there, jnp.logical_not(inner_link))
            arrive(with_more, chained.at[side, position], gotc.at[side, position])
            add_into(held1.at[position], parts + [chained.at[side, position]], with_more)
            add_into(held1.at[position], parts, alone)
            send(
                there,
                held1.at[position],
                chained.at[side, position],
                sems.at[base, position],
                gotc.at[side, position],
                spot.device(here, way),
            )
    for condition, copy in started:
        guarded(condition, lambda copy=copy: copy().wait_send())


def scatter_sum(blocks, lanes, chain, levels, order, collective_id, kind=jnp.float32):
    sizes = device_layout(lanes)
    length = lanes[0] if chain else 1
    rows, columns = blocks.shape[1:]
    low = blocks.dtype
    n_first = sizes[order[0]]
    n_second = sizes[order[1]] if len(order) > 1 else 1
    extra = max(n_first - 1, 1)
    further = max(n_second - 1, 1)
    return pl.pallas_call(
        functools.partial(scatter_kernel, lanes, chain, levels, order),
        out_shape=jax.ShapeDtypeStruct((rows, columns), kind),
        in_specs=[pl.BlockSpec(memory_space=pltpu.VMEM)],
        out_specs=pl.BlockSpec(memory_space=pltpu.VMEM),
        scratch_shapes=[
            pltpu.VMEM((extra, length * n_second, rows, columns), low),
            pltpu.VMEM((further, length, rows, columns), low),
            pltpu.VMEM((further, length, rows, columns), low),
            pltpu.VMEM((length, rows, columns), low),
            pltpu.VMEM((2, length, rows, columns), low),
            pltpu.SemaphoreType.DMA((n_first + n_second, length * n_second)),
            pltpu.SemaphoreType.DMA((extra, length * n_second)),
            pltpu.SemaphoreType.DMA((further, length)),
            pltpu.SemaphoreType.DMA((2, length)),
        ],
        compiler_params=pltpu.CompilerParams(collective_id=collective_id, has_side_effects=True),
        cost_estimate=pl.CostEstimate(
            flops=0, bytes_accessed=20 * blocks.size, transcendentals=0
        ),
    )(blocks)


def weight_grads_kernel(h_ref, g_ref, both_ref, hidden_ref, o_ref):
    turned = (((0,), (0,)), ((), ()))
    wide = both_ref.shape[1]
    o_ref[:, :wide] = lax.dot_general(
        h_ref[...], both_ref[...], turned, preferred_element_type=jnp.float32
    ).astype(o_ref.dtype)
    o_ref[:, wide:] = lax.dot_general(
        g_ref[...], hidden_ref[...], turned, preferred_element_type=jnp.float32
    ).astype(o_ref.dtype)


def weight_grads(h_all, g_all, both, hidden):
    tokens, width = h_all.shape
    tile = math.gcd(width, 384)
    columns = both.shape[1] + hidden.shape[1]
    return pl.pallas_call(
        weight_grads_kernel,
        grid=(width // tile,),
        out_shape=jax.ShapeDtypeStruct((width, columns), h_all.dtype),
        in_specs=[
            pl.BlockSpec((tokens, tile), lambda i: (0, i)),
            pl.BlockSpec((tokens, tile), lambda i: (0, i)),
            pl.BlockSpec(both.shape, lambda i: (0, 0)),
            pl.BlockSpec(hidden.shape, lambda i: (0, 0)),
        ],
        out_specs=pl.BlockSpec((tile, columns), lambda i: (i, 0)),
        cost_estimate=pl.CostEstimate(
            flops=2 * tokens * width * columns,
            bytes_accessed=4 * tokens * width + 2 * width * columns,
            transcendentals=0,
        ),
    )(h_all, g_all, both, hidden)


def unpack_kernel(part, *refs):
    blocks, targets = refs[:-3], refs[-3:]
    count = len(blocks)
    here = lax.axis_index("outer")
    for step, x_ref in enumerate(blocks):
        for source in range(count):

            @pl.when(lax.rem(here - step + count, count) == source)
            def _(x_ref=x_ref, source=source):
                for j, target in enumerate(targets):
                    target[:, source * part : (source + 1) * part] = x_ref[
                        :, j * part : (j + 1) * part
                    ].astype(jnp.float32)


def unpack(blocks, part):
    count = len(blocks)
    rows, columns = blocks[0].shape
    tile = math.gcd(rows, 48)
    width = count * part
    return pl.pallas_call(
        functools.partial(unpack_kernel, part),
        grid=(rows // tile,),
        out_shape=[jax.ShapeDtypeStruct((rows, width), jnp.float32)] * 3,
        in_specs=[pl.BlockSpec((tile, columns), lambda i: (i, 0))] * count,
        out_specs=[pl.BlockSpec((tile, width), lambda i: (i, 0))] * 3,
    )(*blocks)


def finish_kernel(
    lanes, h_ref, a_ref, qkv_ref, mixed_ref, strip_ref, tail_ref,
    o_ref, tails_ref,
    made, came, held, chained, shared, total,
    send0, got0, sendc, gotc, sendt, gott, sends, gots, local_sem,
):
    outer, inner, tensor = lanes
    step = lax.axis_index("outer")
    row = lax.axis_index("inner")
    lane = lax.axis_index("tensor")
    rows = h_ref.shape[0] // (outer * inner)
    extra = strip_ref.shape[1]
    wide = qkv_ref.shape[1]
    left, right = step > 0, step < outer - 1

    def peer_row(shift):
        return lax.rem(row + shift, inner)

    def peer_lane(shift):
        return lax.rem(lane + shift, tensor)

    barrier = pltpu.get_barrier_semaphore()
    for shift in range(1, inner):
        pl.semaphore_signal(barrier, device_id=(step, peer_row(shift), lane), device_id_type=MESH)
    for shift in range(1, tensor):
        pl.semaphore_signal(barrier, device_id=(step, row, peer_lane(shift)), device_id_type=MESH)
    for there, move in ((left, -1), (right, 1)):

        @pl.when(there)
        def _(move=move):
            pl.semaphore_signal(barrier, device_id=(step + move, row, lane), device_id_type=MESH)

    pl.semaphore_wait(
        barrier, inner + tensor - 2 + left.astype(jnp.int32) + right.astype(jnp.int32)
    )

    def make(index):
        window = pl.ds(pl.multiple_of(index * rows, rows), rows)
        made[index, :rows, :wide] = jnp.dot(
            h_ref[window, :], qkv_ref[...], preferred_element_type=jnp.float32
        ).astype(made.dtype)
        made[index, :rows, wide:] = jnp.dot(
            a_ref[window, :], mixed_ref[...], preferred_element_type=jnp.float32
        ).astype(made.dtype)
        made[index, rows:, :] = strip_ref[index]

    def remote(source, target, send_at, recv_at, device):
        return pltpu.make_async_remote_copy(
            src_ref=source,
            dst_ref=target,
            send_sem=send_at,
            recv_sem=recv_at,
            device_id=device,
            device_id_type=MESH,
        )

    orders = [sorted(range(outer), key=lambda p, at=at: -abs(p - at)) for at in range(outer)]

    def place(j):
        position = 0
        for at in range(outer):
            for number in range(outer):
                chosen = (step == at).astype(jnp.int32) * (j == number).astype(jnp.int32)
                position = position + chosen * orders[at][number]
        return position

    def row_copy(k):
        shift = 1 + lax.div(k, outer)
        position = place(lax.rem(k, outer))
        there = peer_row(shift)
        return position * inner + there, remote(
            made.at[position * inner + there],
            came.at[shift - 1, position],
            send0.at[shift - 1, position],
            got0.at[shift - 1, position],
            (step, there, lane),
        )

    def first(k, carry):
        index, copy = row_copy(k)
        make(index)
        copy.start()
        return carry

    lax.fori_loop(0, outer * (inner - 1), first, 0)

    def tail_copy(shift):
        return remote(
            tail_ref,
            tails_ref.at[lane],
            sendt.at[shift - 1],
            gott.at[shift - 1],
            (step, row, peer_lane(shift)),
        )

    local = pltpu.make_async_copy(tail_ref, tails_ref.at[lane], local_sem)
    local.start()
    for shift in range(1, tensor):
        tail_copy(shift).start()

    def second(j, carry):
        make(place(j) * inner + row)
        return carry

    lax.fori_loop(0, outer, second, 0)

    visits = []
    for distance in range(outer - 1, -1, -1):
        if distance == 0:
            visits.append((None, step, 0))
        else:
            visits.append((step - distance >= 0, lax.rem(step - distance + outer, outer), -1))
            visits.append((step + distance < outer, lax.rem(step + distance, outer), 1))

    started = []
    for there, position, way in visits:
        parts = [made.at[position * inner + row]]
        for shift in range(1, inner):
            target = came.at[shift - 1, position]
            guarded(
                there,
                remote(
                    target,
                    target,
                    send0.at[shift - 1, position],
                    got0.at[shift - 1, position],
                    (step, row, lane),
                ).wait_recv,
            )
            parts.append(target)

        def linked(side, position=position):
            target = chained.at[side, position]
            return remote(
                target, target, sendc.at[position], gotc.at[side, position], (step, row, lane)
            )

        if way == 0:
            for side, exists in ((0, left), (1, right)):
                guarded(exists, linked(side).wait_recv)
            inside = jnp.logical_and(left, right)
            add_into(total, parts + [chained.at[0, position], chained.at[1, position]], inside)
            add_into(total, parts + [chained.at[1, position]], jnp.logical_not(left))
            add_into(total, parts + [chained.at[0, position]], jnp.logical_not(right))
        else:
            side = 1 if way == -1 else 0
            link = right if way == -1 else left
            more, alone = jnp.logical_and(there, link), jnp.logical_and(there, jnp.logical_not(link))
            guarded(more, linked(side).wait_recv)
            add_into(held.at[position], parts + [chained.at[side, position]], more)
            add_into(held.at[position], parts, alone)
            copy = remote(
                held.at[position],
                chained.at[side, position],
                sendc.at[position],
                gotc.at[side, position],
                (step + way, row, lane),
            )
            guarded(there, copy.start)
            started.append((there, copy))

    strip = total.at[pl.ds(rows, extra), :]
    small = [
        remote(
            strip,
            shared.at[shift - 1],
            sends.at[shift - 1],
            gots.at[shift - 1],
            (step, row, peer_lane(shift)),
        )
        for shift in range(1, tensor)
    ]
    for copy in small:
        copy.start()
    o_ref[pl.ds(0, rows), :] = total[pl.ds(0, rows), :]
    summed = total[pl.ds(rows, extra), :]
    for shift in range(1, tensor):
        small[shift - 1].wait_recv()
        summed = summed + shared[shift - 1]
    o_ref[pl.ds(rows, extra), :] = summed

    for shift in range(1, tensor):
        small[shift - 1].wait_send()
        tail_copy(shift).wait()
    for there, copy in started:
        guarded(there, copy.wait_send)

    def drain(k, carry):
        row_copy(k)[1].wait_send()
        return carry

    lax.fori_loop(0, outer * (inner - 1), drain, 0)
    local.wait()


def finish(lanes, h_turned, a_turned, grad_qkv, mixed, strips, tail, collective_id):
    outer, inner, tensor = lanes
    low = h_turned.dtype
    count, extra, columns = strips.shape
    rows = h_turned.shape[0] // count
    block = (rows + extra, columns)
    peers = max(inner - 1, 1)
    vmem = pl.BlockSpec(memory_space=pltpu.VMEM)
    dma = pltpu.SemaphoreType.DMA
    return pl.pallas_call(
        functools.partial(finish_kernel, lanes),
        out_shape=[
            jax.ShapeDtypeStruct(block, jnp.float32),
            jax.ShapeDtypeStruct((tensor,) + tail.shape, low),
        ],
        in_specs=[vmem] * 6,
        out_specs=[vmem, pl.BlockSpec(memory_space=pl.ANY)],
        scratch_shapes=[
            pltpu.VMEM((count,) + block, low),
            pltpu.VMEM((peers, outer) + block, low),
            pltpu.VMEM((outer,) + block, low),
            pltpu.VMEM((2, outer) + block, low),
            pltpu.VMEM((tensor - 1, extra, columns), jnp.float32),
            pltpu.VMEM(block, jnp.float32),
            dma((peers, outer)),
            dma((peers, outer)),
            dma((outer,)),
            dma((2, outer)),
            dma((tensor - 1,)),
            dma((tensor - 1,)),
            dma((tensor - 1,)),
            dma((tensor - 1,)),
            dma,
        ],
        compiler_params=pltpu.CompilerParams(collective_id=collective_id, has_side_effects=True),
        cost_estimate=pl.CostEstimate(
            flops=2 * h_turned.size * columns,
            bytes_accessed=20 * count * rows * columns,
            transcendentals=0,
        ),
    )(h_turned, a_turned, grad_qkv, mixed, strips, tail)


def shards(
    lanes,
    layer_input,
    cotangent,
    seq_lengths,
    norm_attn_in,
    w_query,
    w_key,
    w_value,
    w_out,
    norm_attn_out,
    norm_ffn_in,
    w_gate,
    w_up,
    w_down,
    norm_ffn_out,
):
    outer, inner, tensor = lanes
    low = jnp.bfloat16
    shard_rows, width = w_gate.shape
    part = width // outer
    query_cols, key_cols = w_query.shape[1], w_key.shape[1]
    qkv_cols = query_cols + 2 * key_cols

    attn_shard = jnp.concatenate([w_query, w_key, w_value, w_out.T], axis=1)
    attn_full = gather_blocks(attn_shard, lanes, True, ("inner",), 0)
    attn_full = attn_full.reshape(-1, attn_shard.shape[1])
    ffn_parts = pack(outer, part, w_gate, w_up, w_down.T)
    early = [step for step in range(1, outer) if step % 2 == 1]
    late = [step for step in range(1, outer) if step % 2 == 0]
    across = {0: ffn_parts[0]}
    for step in early:
        across[step] = shifted(ffn_parts[step], "outer", outer, step)
    beside = {(0, turn): shifted(across[0], "inner", inner, turn) for turn in range(1, inner)}
    held = {step: ffn_parts[step] for step in late}
    attn_full, across, held = lax.optimization_barrier((attn_full, across, held))
    for step in late:
        across[step] = shifted(held[step], "outer", outer, step)
    for step in early:
        for turn in range(1, inner):
            beside[step, turn] = shifted(across[step], "inner", inner, turn)
    for step in late:
        for turn in range(1, inner):
            beside[step, turn] = shifted(across[step], "inner", inner, turn)
    for step in range(outer):
        beside[step, 0] = across[step]

    row_count = layer_input.shape[0]
    split_rows = row_count // tensor
    first_row = lax.axis_index("tensor") * split_rows

    def own_rows(array):
        return lax.dynamic_slice_in_dim(array, first_row, split_rows, 0)

    is_live, allowed, cosine, sine_wave = layout(seq_lengths[0], row_count)
    kv_heads = key_cols // HD
    groups = H // KV
    layer_float = layer_input.astype(jnp.float32)
    h_attn = rms_scale(layer_float, norm_attn_in).astype(low)
    projected = matmul(h_attn, attn_full[:, :qkv_cols])
    query_pre = (
        projected[:, :query_cols].reshape(row_count, kv_heads, groups, HD).transpose(1, 2, 0, 3)
    )
    query = ((query_pre * cosine + rotate_half(query_pre) * sine_wave) * QUERY_SCALE).astype(low)
    key_pre = (
        projected[:, query_cols : query_cols + key_cols]
        .reshape(row_count, kv_heads, HD)
        .transpose(1, 0, 2)
    )
    keys = (key_pre * cosine + rotate_half(key_pre) * sine_wave).astype(low)
    values = (
        projected[:, query_cols + key_cols :]
        .astype(low)
        .reshape(row_count, kv_heads, HD)
        .transpose(1, 0, 2)
    )
    capped = capped_scores(query, keys)
    expo = jnp.where(allowed, jnp.exp(capped), 0.0)
    log_total = jnp.log(jnp.sum(expo, axis=-1, keepdims=True))
    weights = jnp.where(allowed, jnp.exp(capped - log_total), 0.0)
    probs = weights.astype(low)
    mixed = jnp.einsum("kgqs,ksd->kgqd", probs, values, preferred_element_type=jnp.float32).astype(
        low
    )
    mixed_flat = mixed.transpose(2, 0, 1, 3).reshape(row_count, -1)
    out_turned = attn_full[:, qkv_cols:]
    attn_branch = scatter_sum(
        right_product(mixed_flat, out_turned).astype(low).reshape(tensor, split_rows, -1),
        lanes,
        False,
        ("x", "core"),
        ("core", "x"),
        1,
    )
    layer_own = own_rows(layer_float)
    resid = layer_own + rms_scale(attn_branch, norm_attn_out)
    h_ffn = rms_scale(resid, norm_ffn_in).astype(low)

    last = [(step, turn) for step in late for turn in range(1, inner)]
    h_all, ffn_full = gather_blocks(
        h_ffn,
        lanes,
        True,
        ("x", "core"),
        2,
        {key: item for key, item in beside.items() if key not in last},
    )
    h_all = h_all.reshape(-1, h_ffn.shape[1])
    for step, turn in last:
        place = lax.rem(lax.axis_index("outer") - step + outer, outer) * inner
        place = place + lax.rem(lax.axis_index("inner") - turn + inner, inner)
        ffn_full = lax.dynamic_update_slice(ffn_full, beside[step, turn][None], (place, 0, 0))
    ffn_full = ffn_full.reshape(-1, 3 * part)
    gate_up = matmul(h_all, ffn_full[:, : 2 * part])
    gate_pre, up_pre = gate_up[:, :part], gate_up[:, part:]
    gelu_gate = gelu_tanh(gate_pre)
    hidden = (gelu_gate * up_pre).astype(low)
    down_full = ffn_full[:, 2 * part :]
    ffn_branch = scatter_sum(
        right_product(hidden, down_full).astype(low).reshape(outer * tensor, split_rows, -1),
        lanes,
        True,
        ("x", "core"),
        ("core", "x"),
        3,
    )
    output_own = (resid + rms_scale(ffn_branch, norm_ffn_out)).astype(low)

    grad_out = own_rows(cotangent).astype(jnp.float32) * own_rows(
        is_live.astype(jnp.float32)[:, None]
    )
    _, pull_four = jax.vjp(rms_scale, ffn_branch, norm_ffn_out)
    grad_ffn_float, grad_norm_ffn_out = pull_four(grad_out)
    grad_ffn_all = gather_blocks(grad_ffn_float.astype(low), lanes, True, ("x", "core"), 4)
    grad_ffn_all = grad_ffn_all.reshape(-1, h_ffn.shape[1])
    grad_hidden = matmul(grad_ffn_all, down_full)
    grad_up = (grad_hidden * gelu_gate).astype(low)
    _, pull_gelu = jax.vjp(gelu_tanh, gate_pre)
    grad_gate = pull_gelu(grad_hidden * up_pre)[0].astype(low)
    grad_both = jnp.concatenate([grad_gate, grad_up], axis=1)
    grad_h_part = right_product(grad_both, ffn_full[:, : 2 * part]).astype(low)
    grad_h_ffn = scatter_sum(
        grad_h_part.reshape(outer * tensor, split_rows, -1),
        lanes,
        True,
        ("x", "core"),
        ("core", "x"),
        5,
    )
    grad_w_ffn = weight_grads(h_all, grad_ffn_all, grad_both, hidden)
    grad_w_ffn = grad_w_ffn.reshape(outer, inner, shard_rows, 3 * part)
    here, row = lax.axis_index("outer"), lax.axis_index("inner")

    def grad_block(step, turn):
        place = (lax.rem(here + step, outer), lax.rem(row + turn, inner), 0, 0)
        return lax.dynamic_slice(grad_w_ffn, place, (1, 1, shard_rows, 3 * part))[0, 0]

    half = max(outer // 2, 1)
    groups_of_steps = (range(1, 1 + half), [*range(1 + half, outer), 0])
    outgoing = [
        {(step, turn): grad_block(step, turn) for step in steps for turn in range(1, inner)}
        for steps in groups_of_steps
    ]
    grad_h_ffn, outgoing[1] = lax.optimization_barrier((grad_h_ffn, outgoing[1]))

    def start_rows(number):
        return {
            key: shifted(item, "inner", inner, key[1]) for key, item in outgoing[number].items()
        }

    def sum_rows(number, came):
        summed = {}
        for step in groups_of_steps[number]:
            total = grad_block(step, 0).astype(jnp.float32)
            for turn in range(1, inner):
                total = total + came[step, turn].astype(jnp.float32)
            summed[step] = total.astype(low)
        return summed

    def send_rows(summed):
        return {
            step: shifted(item, "outer", outer, step) if step else item
            for step, item in summed.items()
        }

    rows_now = sum_rows(0, start_rows(0))
    rows_later = start_rows(1)

    _, pull_three = jax.vjp(rms_scale, resid, norm_ffn_in)
    grad_resid_part, grad_norm_ffn_in = pull_three(grad_h_ffn)
    grad_resid = grad_out + grad_resid_part
    _, pull_two = jax.vjp(rms_scale, attn_branch, norm_attn_out)
    grad_attn_float, grad_norm_attn_out = pull_two(grad_resid)
    grad_attn_own, rows_now = lax.optimization_barrier((grad_attn_float.astype(low), rows_now))
    summed = send_rows(rows_now)
    grad_attn_branch = gather_blocks(
        grad_attn_own, lanes, False, ("x", "core"), 6
    ).reshape(row_count, -1)
    grad_attn_branch, rows_later = lax.optimization_barrier((grad_attn_branch, rows_later))
    summed.update(send_rows(sum_rows(1, rows_later)))
    sum_gate, sum_up, sum_down = unpack([summed[step] for step in range(outer)], part)
    sum_down = sum_down.T
    grad_mixed = matmul(grad_attn_branch, out_turned).astype(low)
    grad_mixed = grad_mixed.reshape(row_count, kv_heads, groups, HD).transpose(1, 2, 0, 3)
    grad_values = jnp.einsum(
        "kgqs,kgqd->ksd", probs, grad_mixed, preferred_element_type=jnp.float32
    ).astype(low)
    grad_probs = jnp.einsum(
        "kgqd,ksd->kgqs", grad_mixed, values, preferred_element_type=jnp.float32
    )
    row_delta = jnp.sum(weights * grad_probs, axis=-1, keepdims=True)
    tanh_part = capped / SOFT_CAP
    grad_scores = (weights * (grad_probs - row_delta) * (1.0 - tanh_part * tanh_part)).astype(low)
    grad_query_raw = jnp.einsum(
        "kgqs,ksd->kgqd", grad_scores, keys, preferred_element_type=jnp.float32
    )
    grad_query = (
        (grad_query_raw * cosine - rotate_half(grad_query_raw) * sine_wave) * QUERY_SCALE
    ).astype(low)
    grad_keys_raw = jnp.einsum(
        "kgqs,kgqd->ksd", grad_scores, query, preferred_element_type=jnp.float32
    )
    grad_keys = (grad_keys_raw * cosine - rotate_half(grad_keys_raw) * sine_wave).astype(low)
    grad_qkv = jnp.concatenate(
        [
            grad_query.transpose(2, 0, 1, 3).reshape(row_count, -1),
            grad_keys.transpose(1, 0, 2).reshape(row_count, -1),
            grad_values.transpose(1, 0, 2).reshape(row_count, -1),
        ],
        axis=1,
    )
    grad_a_part = right_product(grad_qkv, attn_full[:, :qkv_cols]).astype(low)
    grad_h_attn = scatter_sum(
        grad_a_part.reshape(tensor, split_rows, -1),
        lanes,
        False,
        ("x", "core"),
        ("core", "x"),
        7,
    )
    _, pull_one = jax.vjp(rms_scale, layer_own, norm_attn_in)
    grad_input_part, grad_norm_attn_in = pull_one(grad_h_attn)
    input_own = grad_resid + grad_input_part

    norm_rows = jnp.stack(
        [grad_norm_attn_in, grad_norm_attn_out, grad_norm_ffn_in, grad_norm_ffn_out]
    )
    strips = norm_rows.reshape(4, outer * inner, shard_rows).transpose(1, 0, 2)
    strips = strips.reshape(outer * inner, 1, -1).astype(low)
    attn_cols = attn_shard.shape[1]
    strips = jnp.pad(strips, ((0, 0), (0, 15), (0, attn_cols - strips.shape[2])))
    tail = jnp.concatenate([output_own, input_own.astype(low)], axis=0)
    sum_last, tails = finish(
        lanes, h_attn.T, grad_attn_branch.T, grad_qkv, mixed_flat, strips, tail, 8
    )
    layer_output = tails[:, :split_rows].reshape(row_count, -1)
    input_grad = tails[:, split_rows:].reshape(row_count, -1).astype(jnp.float32)
    sum_attn_in, sum_attn_out, sum_ffn_in, sum_ffn_out = (
        sum_last[shard_rows, i * shard_rows : (i + 1) * shard_rows] for i in range(4)
    )
    sum_last = sum_last[:shard_rows]
    sum_out = sum_last[:, qkv_cols:].T
    sum_query = sum_last[:, :query_cols]
    sum_key = sum_last[:, query_cols : query_cols + key_cols]
    sum_value = sum_last[:, query_cols + key_cols : qkv_cols]
    return (
        layer_output,
        input_grad,
        sum_attn_in,
        sum_query,
        sum_key,
        sum_value,
        sum_out,
        sum_attn_out,
        sum_ffn_in,
        sum_gate,
        sum_up,
        sum_down,
        sum_ffn_out,
    )


def solution(mesh):
    dp_size, tensor = mesh.shape["dp"], mesh.shape["tensor"]
    outer = math.gcd(4, dp_size)
    lanes = (outer, dp_size // outer, tensor)
    split = Mesh(mesh.devices.reshape(lanes), ("outer", "inner", "tensor"))
    dp = ("outer", "inner")

    def run(*args):
        return jax.shard_map(
            lambda *blocks: shards(lanes, *blocks),
            mesh=split,
            in_specs=(
                P(dp, None),
                P(dp, None),
                P(dp, None),
                P(),
                P(dp, "tensor"),
                P(dp, "tensor"),
                P(dp, "tensor"),
                P("tensor", dp),
                P(),
                P(),
                P(dp, "tensor"),
                P(dp, "tensor"),
                P("tensor", dp),
                P(),
            ),
            out_specs=(
                P(dp, None),
                P(dp, None),
                P(dp),
                P(dp, "tensor"),
                P(dp, "tensor"),
                P(dp, "tensor"),
                P("tensor", dp),
                P(dp),
                P(dp),
                P(dp, "tensor"),
                P(dp, "tensor"),
                P("tensor", dp),
                P(dp),
            ),
            check_vma=False,
        )(*args)

    return run
```

```python
import functools
import math

import jax
import jax.numpy as jnp
from jax import lax
from jax.experimental import pallas as pl
from jax.experimental.pallas import tpu as pltpu
from jax.sharding import Mesh, PartitionSpec as P

H = 8
KV = 4
HD = 256


EPSILON = 1e-06
SOFT_CAP = 50.0
QUERY_SCALE = 0.0625
GELU_COEFF = 0.7978845608028654

MESH = pl.DeviceIdType.MESH


def rms_scale(values, scales):
    return values * lax.rsqrt(jnp.mean(values * values, axis=-1, keepdims=True) + EPSILON) * scales


def gelu_tanh(inputs):
    return (
        0.5 * inputs * (1.0 + jnp.tanh(GELU_COEFF * (inputs + 0.044715 * inputs * inputs * inputs)))
    )


def rotate_half(heads):
    middle = heads.shape[-1] // 2
    return jnp.concatenate([-heads[..., middle:], heads[..., :middle]], axis=-1)


def layout(lengths, row_count):
    seq_ends = jnp.cumsum(lengths)
    row_index = jnp.arange(row_count, dtype=jnp.int32)
    passed = (row_index[:, None] >= seq_ends[None, :]).astype(jnp.int32)
    segment = jnp.sum(passed, axis=1)
    is_live = row_index < seq_ends[-1]
    seq_ident = jnp.where(is_live, segment, lengths.shape[0] + row_index)
    offset = row_index - jnp.sum(passed * lengths[None, :], axis=1)
    allowed = (seq_ident[:, None] == seq_ident[None, :]) & (
        row_index[None, :] <= row_index[:, None]
    )
    middle = HD // 2
    inverse = jnp.exp(jnp.arange(middle, dtype=jnp.float32) * (-2.0 * math.log(10000.0) / HD))
    angles = offset.astype(jnp.float32)[:, None] * inverse[None, :]
    cosine = jnp.concatenate([jnp.cos(angles), jnp.cos(angles)], axis=1)
    sine_wave = jnp.concatenate([jnp.sin(angles), jnp.sin(angles)], axis=1)
    return (is_live, allowed, cosine, sine_wave)


def matmul(left, right):
    return jnp.dot(left, right, preferred_element_type=jnp.float32)


def right_product(left, right):
    return jnp.einsum("tc,dc->td", left, right, preferred_element_type=jnp.float32)


def capped_scores(query, keys):
    raw_scores = jnp.einsum("kgqd,ksd->kgqs", query, keys, preferred_element_type=jnp.float32)
    return SOFT_CAP * jnp.tanh(raw_scores / SOFT_CAP)


def shifted(block, axis, size, step):
    return lax.ppermute(block, axis, [(i, (i + step) % size) for i in range(size)])


def pack_kernel(part, g_ref, u_ref, d_ref, *o_refs):
    count = len(o_refs)
    here = lax.axis_index("outer")
    tile = math.gcd(g_ref.shape[0], 16)
    for step, o_ref in enumerate(o_refs):
        for source in range(count):

            @pl.when(lax.rem(here + step, count) == source)
            def _(o_ref=o_ref, source=source):
                def body(r, carry):
                    window = pl.ds(pl.multiple_of(r * tile, tile), tile)
                    for j, ref in enumerate((g_ref, u_ref, d_ref)):
                        o_ref[window, j * part : (j + 1) * part] = ref[
                            window, source * part : (source + 1) * part
                        ]
                    return carry

                lax.fori_loop(0, g_ref.shape[0] // tile, body, 0)


def pack(count, part, gate, up, down_turned):
    vmem = pl.BlockSpec(memory_space=pltpu.VMEM)
    return pl.pallas_call(
        functools.partial(pack_kernel, part),
        out_shape=[jax.ShapeDtypeStruct((gate.shape[0], 3 * part), gate.dtype)] * count,
        in_specs=[vmem] * 3,
        out_specs=[vmem] * count,
        cost_estimate=pl.CostEstimate(
            flops=0, bytes_accessed=12 * gate.size, transcendentals=0
        ),
    )(gate, up, down_turned)


def device_layout(lanes):
    _, inner, tensor = lanes
    cores = 2 if tensor % 2 == 0 else 1
    return {"inner": inner, "x": tensor // cores, "core": cores}


class Spot:
    def __init__(self, lanes, chain, levels):
        self.sizes = device_layout(lanes)
        self.chain, self.levels = chain, levels
        self.length = lanes[0] if chain else 1
        self.at_chain = lax.axis_index("outer")
        tensor = lax.axis_index("tensor")
        cores = self.sizes["core"]
        self.here = {
            "inner": lax.axis_index("inner"),
            "x": lax.div(tensor, cores),
            "core": lax.rem(tensor, cores),
        }
        self.step = self.at_chain if chain else 0
        self.slots = {}
        for level in levels:
            for shift in range(1, self.sizes[level]):
                self.slots[level, shift] = 2 + len(self.slots)

    def moved(self, **shifts):
        at = dict(self.here)
        for level, shift in shifts.items():
            at[level] = lax.rem(at[level] + shift, self.sizes[level])
        return at

    def device(self, at, chain_shift=0):
        return (
            self.at_chain + chain_shift,
            at["inner"],
            at["x"] * self.sizes["core"] + at["core"],
        )

    def flat(self, step, at):
        index = step
        for level in self.levels:
            index = index * self.sizes[level] + at[level]
        return index

    def greet(self):
        barrier = pltpu.get_barrier_semaphore()
        count = 0
        for level in self.levels:
            for shift in range(1, self.sizes[level]):
                pl.semaphore_signal(
                    barrier, device_id=self.device(self.moved(**{level: shift})), device_id_type=MESH
                )
                count += 1
        if self.length > 1:
            for shift, there in ((-1, self.step > 0), (1, self.step < self.length - 1)):
                count = count + there.astype(jnp.int32)

                @pl.when(there)
                def _(shift=shift):
                    pl.semaphore_signal(
                        barrier, device_id=self.device(self.here, shift), device_id_type=MESH
                    )

        pl.semaphore_wait(barrier, count)


def guarded(condition, action):
    if condition is None:
        action()
    else:
        pl.when(condition)(action)


def both(first, second):
    if first is None:
        return second
    return first if second is None else jnp.logical_and(first, second)


def gather_kernel(lanes, chain, levels, places, *refs):
    held_refs, refs = refs[1 : 1 + len(places)], refs[:1] + refs[1 + len(places) :]
    if places:
        x_ref, o_ref, placed_ref, send_sem, recv_sem, local_sem, place_sem = refs
    else:
        x_ref, o_ref, send_sem, recv_sem, local_sem = refs
    spot = Spot(lanes, chain, levels)
    length, step, here = spot.length, spot.step, spot.here
    started = []

    def send(condition, source, index, slot, device):
        def copy():
            return pltpu.make_async_remote_copy(
                src_ref=source,
                dst_ref=o_ref.at[index],
                send_sem=send_sem.at[slot, index],
                recv_sem=recv_sem.at[index],
                device_id=device,
                device_id_type=MESH,
            )

        guarded(condition, lambda: copy().start())
        started.append((condition, copy))

    def arrive(condition, index):
        def wait():
            pltpu.make_async_remote_copy(
                src_ref=o_ref.at[index],
                dst_ref=o_ref.at[index],
                send_sem=send_sem.at[0, index],
                recv_sem=recv_sem.at[index],
                device_id=spot.device(here),
                device_id_type=MESH,
            ).wait_recv()

        guarded(condition, wait)

    def spread(condition, source, index, first):
        for level in levels[first:]:
            for shift in range(1, spot.sizes[level]):
                send(
                    condition,
                    source,
                    index,
                    spot.slots[level, shift],
                    spot.device(spot.moved(**{level: shift})),
                )

    def around(distance):
        if distance == 0:
            return [(None, step)]
        return [(step - distance >= 0, step - distance), (step + distance < length, step + distance)]

    def clipped(position):
        return lax.rem(position + length, length) if length > 1 else position

    spot.greet()
    mine = spot.flat(step, here)
    local = pltpu.make_async_copy(x_ref, o_ref.at[mine], local_sem)
    local.start()
    if length > 1:
        send(step < length - 1, x_ref, mine, 1, spot.device(here, 1))
        send(step > 0, x_ref, mine, 0, spot.device(here, -1))
    spread(None, x_ref, mine, 0)

    outer, inner, _ = lanes
    moves = []
    for number, (back, turn) in enumerate(places):
        index = lax.rem(lax.axis_index("outer") - back + outer, outer) * inner
        index = index + lax.rem(lax.axis_index("inner") - turn + inner, inner)
        moves.append(
            pltpu.make_async_copy(
                held_refs[number], placed_ref.at[index], place_sem.at[number]
            )
        )
        moves[-1].start()

    def relay(distance):
        if len(levels) < 2:
            return
        level = levels[0]
        for there, position in around(distance):
            for shift in range(1, spot.sizes[level]):
                index = spot.flat(clipped(position), spot.moved(**{level: shift}))
                arrive(there, index)
                spread(there, o_ref.at[index], index, 1)

    for distance in range(1, length):
        for way, (there, position) in enumerate(around(distance)):
            index = spot.flat(clipped(position), here)
            arrive(there, index)
            onward = step < length - 1 if way == 0 else step > 0
            send(
                both(there, onward),
                o_ref.at[index],
                index,
                1 - way,
                spot.device(here, 1 if way == 0 else -1),
            )
            spread(there, o_ref.at[index], index, 0)
        relay(distance - 1)
    relay(length - 1)
    last = levels[-1]
    others = [{}]
    for level in levels[:-1]:
        others = [{**rest, level: shift} for rest in others for shift in range(spot.sizes[level])]
    for position in range(length):
        for rest in others:
            for shift in range(1, spot.sizes[last]):
                arrive(None, spot.flat(position, spot.moved(**{**rest, last: shift})))
    for condition, copy in started:
        guarded(condition, lambda copy=copy: copy().wait_send())
    for move in moves:
        move.wait()
    local.wait()


def gather_blocks(block, lanes, chain, levels, collective_id, held=None):
    held = held or {}
    places = tuple(held)
    blocks = [held[key] for key in places]
    sizes = device_layout(lanes)
    count = (lanes[0] if chain else 1) * math.prod(sizes[level] for level in levels)
    slots = 2 + sum(sizes[level] - 1 for level in levels)
    out_shape = [jax.ShapeDtypeStruct((count,) + block.shape, block.dtype)]
    scratch = [
        pltpu.SemaphoreType.DMA((slots, count)),
        pltpu.SemaphoreType.DMA((count,)),
        pltpu.SemaphoreType.DMA,
    ]
    if held:
        out_shape.append(
            jax.ShapeDtypeStruct((lanes[0] * lanes[1],) + blocks[0].shape, blocks[0].dtype)
        )
        scratch.append(pltpu.SemaphoreType.DMA((len(blocks),)))
    results = pl.pallas_call(
        functools.partial(gather_kernel, lanes, chain, levels, places),
        out_shape=out_shape,
        in_specs=[pl.BlockSpec(memory_space=pltpu.VMEM)] * (1 + len(blocks)),
        out_specs=[pl.BlockSpec(memory_space=pl.ANY)] * len(out_shape),
        scratch_shapes=scratch,
        compiler_params=pltpu.CompilerParams(collective_id=collective_id, has_side_effects=True),
        cost_estimate=pl.CostEstimate(
            flops=0, bytes_accessed=20 * count * block.size, transcendentals=0
        ),
    )(block, *blocks)
    return results if held else results[0]


def add_into(target, parts, condition=None):
    rows = target.shape[0]
    tile = math.gcd(rows, 16)

    def action():
        def body(r, carry):
            window = pl.ds(pl.multiple_of(r * tile, tile), tile)
            total = parts[0][window, :].astype(jnp.float32)
            for part in parts[1:]:
                total = total + part[window, :].astype(jnp.float32)
            target[window, :] = total.astype(target.dtype)
            return carry

        lax.fori_loop(0, rows // tile, body, 0)

    guarded(condition, action)


def scatter_kernel(
    lanes, chain, levels, order, x_ref, o_ref, came0, came1, held0, held1, chained, sems, got0, got1, gotc
):
    spot = Spot(lanes, chain, levels)
    length, step, here = spot.length, spot.step, spot.here
    started = []

    def send(condition, source, target, send_at, recv_at, device):
        def copy():
            return pltpu.make_async_remote_copy(
                src_ref=source,
                dst_ref=target,
                send_sem=send_at,
                recv_sem=recv_at,
                device_id=device,
                device_id_type=MESH,
            )

        guarded(condition, lambda: copy().start())
        started.append((condition, copy))

    def arrive(condition, target, recv_at):
        def wait():
            pltpu.make_async_remote_copy(
                src_ref=target,
                dst_ref=target,
                send_sem=recv_at,
                recv_sem=recv_at,
                device_id=spot.device(here),
                device_id_type=MESH,
            ).wait_recv()

        guarded(condition, wait)

    visits = []
    for distance in range(length - 1, -1, -1):
        if distance == 0:
            visits.append((None, step, 0))
        else:
            visits.append(
                (step - distance >= 0, lax.rem(step - distance + length, length), -1)
            )
            visits.append((step + distance < length, lax.rem(step + distance, length), 1))

    spot.greet()
    first = order[0]
    second = order[1] if len(order) > 1 else None
    n_first = spot.sizes[first]
    n_second = spot.sizes[second] if second else 1

    def second_shifts(own):
        return [0] if own else list(range(1, n_second))

    for own in (False, True):
        for there, position, _ in visits:
            for other in second_shifts(own):
                for shift in range(1, n_first):
                    where = {first: shift}
                    if second:
                        where[second] = other
                    at = spot.moved(**where)
                    lane = position * n_second + (at[second] if second else 0)
                    send(
                        there,
                        x_ref.at[spot.flat(position, at)],
                        came0.at[shift - 1, lane],
                        sems.at[shift - 1, lane],
                        got0.at[shift - 1, lane],
                        spot.device(spot.moved(**{first: shift})),
                    )

    def first_sum(there, position, other):
        at = spot.moved(**({second: other} if second else {}))
        lane = position * n_second + (at[second] if second else 0)
        parts = [x_ref.at[spot.flat(position, at)]]
        for shift in range(1, n_first):
            arrive(there, came0.at[shift - 1, lane], got0.at[shift - 1, lane])
            parts.append(came0.at[shift - 1, lane])
        return parts

    for there, position, _ in visits:
        for other in second_shifts(False):
            parts = first_sum(there, position, other)
            add_into(held0.at[other - 1, position], parts, there)
            send(
                there,
                held0.at[other - 1, position],
                came1.at[other - 1, position],
                sems.at[n_first - 1 + other - 1, position],
                got1.at[other - 1, position],
                spot.device(spot.moved(**{second: other})),
            )
    base = n_first - 1 + n_second - 1
    for there, position, way in visits:
        parts = first_sum(there, position, 0)
        for other in second_shifts(False):
            arrive(there, came1.at[other - 1, position], got1.at[other - 1, position])
            parts.append(came1.at[other - 1, position])
        if way == 0:
            if length > 1:
                for side, exists in ((0, step > 0), (1, step < length - 1)):
                    arrive(exists, chained.at[side, position], gotc.at[side, position])

                def extra(sides):
                    return parts + [chained.at[side, position] for side in sides]

                inside = jnp.logical_and(step > 0, step < length - 1)
                add_into(o_ref, extra((0, 1)), inside)
                add_into(o_ref, extra((1,)), step == 0)
                add_into(o_ref, extra((0,)), step == length - 1)
            else:
                add_into(o_ref, parts)
        else:
            side = 1 if way == -1 else 0
            inner_link = step < length - 1 if way == -1 else step > 0
            with_more = both(there, inner_link)
            alone = both(there, jnp.logical_not(inner_link))
            arrive(with_more, chained.at[side, position], gotc.at[side, position])
            add_into(held1.at[position], parts + [chained.at[side, position]], with_more)
            add_into(held1.at[position], parts, alone)
            send(
                there,
                held1.at[position],
                chained.at[side, position],
                sems.at[base, position],
                gotc.at[side, position],
                spot.device(here, way),
            )
    for condition, copy in started:
        guarded(condition, lambda copy=copy: copy().wait_send())


def scatter_sum(blocks, lanes, chain, levels, order, collective_id, kind=jnp.float32):
    sizes = device_layout(lanes)
    length = lanes[0] if chain else 1
    rows, columns = blocks.shape[1:]
    low = blocks.dtype
    n_first = sizes[order[0]]
    n_second = sizes[order[1]] if len(order) > 1 else 1
    extra = max(n_first - 1, 1)
    further = max(n_second - 1, 1)
    return pl.pallas_call(
        functools.partial(scatter_kernel, lanes, chain, levels, order),
        out_shape=jax.ShapeDtypeStruct((rows, columns), kind),
        in_specs=[pl.BlockSpec(memory_space=pltpu.VMEM)],
        out_specs=pl.BlockSpec(memory_space=pltpu.VMEM),
        scratch_shapes=[
            pltpu.VMEM((extra, length * n_second, rows, columns), low),
            pltpu.VMEM((further, length, rows, columns), low),
            pltpu.VMEM((further, length, rows, columns), low),
            pltpu.VMEM((length, rows, columns), low),
            pltpu.VMEM((2, length, rows, columns), low),
            pltpu.SemaphoreType.DMA((n_first + n_second, length * n_second)),
            pltpu.SemaphoreType.DMA((extra, length * n_second)),
            pltpu.SemaphoreType.DMA((further, length)),
            pltpu.SemaphoreType.DMA((2, length)),
        ],
        compiler_params=pltpu.CompilerParams(collective_id=collective_id, has_side_effects=True),
        cost_estimate=pl.CostEstimate(
            flops=0, bytes_accessed=20 * blocks.size, transcendentals=0
        ),
    )(blocks)


def product_scatter_kernel(
    lanes, chain, columns, left_ref, right_ref, o_ref,
    made, came0, came1, held0, held1, chained, send0, send1, sendc, got0, got1, gotc,
):
    spot = Spot(lanes, chain, ("x", "core"))
    length, step, here = spot.length, spot.step, spot.here
    n_x, n_core = spot.sizes["x"], spot.sizes["core"]
    rows = o_ref.shape[0]
    begin, end = columns
    started = []

    def remote(source, target, send_at, recv_at, device):
        return pltpu.make_async_remote_copy(
            src_ref=source,
            dst_ref=target,
            send_sem=send_at,
            recv_sem=recv_at,
            device_id=device,
            device_id_type=MESH,
        )

    def arrive(condition, target, recv_at):
        copy = remote(target, target, recv_at, recv_at, spot.device(here))
        guarded(condition, copy.wait_recv)

    span = n_x * n_core

    def make(position):
        window = pl.ds(pl.multiple_of(position * span * rows, span * rows), span * rows)
        product = lax.dot_general(
            left_ref[window, :],
            right_ref[:, begin:end],
            (((1,), (1,)), ((), ())),
            preferred_element_type=jnp.float32,
        ).astype(made.dtype)
        for lane in range(span):
            made[position * span + lane] = product[lane * rows : (lane + 1) * rows]

    orders = [sorted(range(length), key=lambda p, at=at: -abs(p - at)) for at in range(length)]

    def place(j):
        position = 0
        for at in range(length):
            for number in range(length):
                chosen = (step == at).astype(jnp.int32) * (j == number).astype(jnp.int32)
                position = position + chosen * orders[at][number]
        return position

    def core_copy(position, x_shift, shift):
        at_x = spot.moved(x=x_shift)["x"]
        peer = spot.moved(core=shift)
        lane = position * n_x + at_x
        return remote(
            made.at[lane * n_core + peer["core"]],
            came0.at[shift - 1, lane],
            send0.at[shift - 1, lane],
            got0.at[shift - 1, lane],
            spot.device(peer),
        )

    def x_copy(position, shift):
        return remote(
            held0.at[shift - 1, position],
            came1.at[shift - 1, position],
            send1.at[shift - 1, position],
            got1.at[shift - 1, position],
            spot.device(spot.moved(x=shift)),
        )

    def core_parts(there, position, shift_x):
        lane = position * n_x + spot.moved(x=shift_x)["x"]
        parts = [made.at[lane * n_core + here["core"]]]
        for shift in range(1, n_core):
            arrive(there, came0.at[shift - 1, lane], got0.at[shift - 1, lane])
            parts.append(came0.at[shift - 1, lane])
        return parts

    spot.greet()

    def produce(j, carry):
        @pl.when(j < length)
        def _():
            position = place(j)
            make(position)
            for x_shift in (*range(1, n_x), 0):
                for shift in range(1, n_core):
                    core_copy(position, x_shift, shift).start()

        @pl.when(j > 0)
        def _():
            position = place(j - 1)
            for shift in range(1, n_x):
                add_into(held0.at[shift - 1, position], core_parts(None, position, shift))
                x_copy(position, shift).start()

        return carry

    lax.fori_loop(0, length + 1, produce, 0)

    visits = []
    for distance in range(length - 1, -1, -1):
        if distance == 0:
            visits.append((None, step, 0))
        else:
            visits.append(
                (step - distance >= 0, lax.rem(step - distance + length, length), -1)
            )
            visits.append((step + distance < length, lax.rem(step + distance, length), 1))

    for there, position, way in visits:
        parts = core_parts(there, position, 0)
        for shift in range(1, n_x):
            arrive(there, came1.at[shift - 1, position], got1.at[shift - 1, position])
            parts.append(came1.at[shift - 1, position])
        if length == 1:
            add_into(o_ref, parts)
        elif way == 0:
            left, right = step > 0, step < length - 1
            for side, exists in ((0, left), (1, right)):
                arrive(exists, chained.at[side, position], gotc.at[side, position])
            sides = [chained.at[0, position], chained.at[1, position]]
            add_into(o_ref, parts + sides, jnp.logical_and(left, right))
            add_into(o_ref, parts + sides[1:], jnp.logical_not(left))
            add_into(o_ref, parts + sides[:1], jnp.logical_not(right))
        else:
            side = 1 if way == -1 else 0
            link = step < length - 1 if way == -1 else step > 0
            more = jnp.logical_and(there, link)
            alone = jnp.logical_and(there, jnp.logical_not(link))
            arrive(more, chained.at[side, position], gotc.at[side, position])
            add_into(held1.at[position], parts + [chained.at[side, position]], more)
            add_into(held1.at[position], parts, alone)
            copy = remote(
                held1.at[position],
                chained.at[side, position],
                sendc.at[position],
                gotc.at[side, position],
                spot.device(here, way),
            )
            guarded(there, copy.start)
            started.append((there, copy))
    for condition, copy in started:
        guarded(condition, copy.wait_send)

    def drain(position, carry):
        for x_shift in range(n_x):
            for shift in range(1, n_core):
                core_copy(position, x_shift, shift).wait_send()
        for shift in range(1, n_x):
            x_copy(position, shift).wait_send()
        return carry

    lax.fori_loop(0, length, drain, 0)


def product_scatter(left, right, columns, lanes, chain, collective_id):
    sizes = device_layout(lanes)
    length = lanes[0] if chain else 1
    n_x, n_core = sizes["x"], sizes["core"]
    count = length * n_x * n_core
    block = (left.shape[0] // count, right.shape[0])
    low = left.dtype
    more_core, more_x = max(n_core - 1, 1), max(n_x - 1, 1)
    vmem = pl.BlockSpec(memory_space=pltpu.VMEM)
    dma = pltpu.SemaphoreType.DMA
    return pl.pallas_call(
        functools.partial(product_scatter_kernel, lanes, chain, columns),
        out_shape=jax.ShapeDtypeStruct(block, jnp.float32),
        in_specs=[vmem, vmem],
        out_specs=vmem,
        scratch_shapes=[
            pltpu.VMEM((count,) + block, low),
            pltpu.VMEM((more_core, length * n_x) + block, low),
            pltpu.VMEM((more_x, length) + block, low),
            pltpu.VMEM((more_x, length) + block, low),
            pltpu.VMEM((length,) + block, low),
            pltpu.VMEM((2, length) + block, low),
            dma((more_core, length * n_x)),
            dma((more_x, length)),
            dma((length,)),
            dma((more_core, length * n_x)),
            dma((more_x, length)),
            dma((2, length)),
        ],
        compiler_params=pltpu.CompilerParams(collective_id=collective_id, has_side_effects=True),
        cost_estimate=pl.CostEstimate(
            flops=2 * left.size * right.shape[0],
            bytes_accessed=40 * left.shape[0] * right.shape[0],
            transcendentals=0,
        ),
    )(left, right)


def weight_grads_kernel(h_ref, g_ref, both_ref, hidden_ref, o_ref):
    turned = (((0,), (0,)), ((), ()))
    wide = both_ref.shape[1]
    o_ref[:, :wide] = lax.dot_general(
        h_ref[...], both_ref[...], turned, preferred_element_type=jnp.float32
    ).astype(o_ref.dtype)
    o_ref[:, wide:] = lax.dot_general(
        g_ref[...], hidden_ref[...], turned, preferred_element_type=jnp.float32
    ).astype(o_ref.dtype)


def weight_grads(h_all, g_all, both, hidden):
    tokens, width = h_all.shape
    tile = math.gcd(width, 384)
    columns = both.shape[1] + hidden.shape[1]
    return pl.pallas_call(
        weight_grads_kernel,
        grid=(width // tile,),
        out_shape=jax.ShapeDtypeStruct((width, columns), h_all.dtype),
        in_specs=[
            pl.BlockSpec((tokens, tile), lambda i: (0, i)),
            pl.BlockSpec((tokens, tile), lambda i: (0, i)),
            pl.BlockSpec(both.shape, lambda i: (0, 0)),
            pl.BlockSpec(hidden.shape, lambda i: (0, 0)),
        ],
        out_specs=pl.BlockSpec((tile, columns), lambda i: (i, 0)),
        cost_estimate=pl.CostEstimate(
            flops=2 * tokens * width * columns,
            bytes_accessed=4 * tokens * width + 2 * width * columns,
            transcendentals=0,
        ),
    )(h_all, g_all, both, hidden)


def unpack_kernel(part, *refs):
    blocks, targets = refs[:-3], refs[-3:]
    count = len(blocks)
    here = lax.axis_index("outer")
    for step, x_ref in enumerate(blocks):
        for source in range(count):

            @pl.when(lax.rem(here - step + count, count) == source)
            def _(x_ref=x_ref, source=source):
                for j, target in enumerate(targets):
                    target[:, source * part : (source + 1) * part] = x_ref[
                        :, j * part : (j + 1) * part
                    ].astype(jnp.float32)


def unpack(blocks, part):
    count = len(blocks)
    rows, columns = blocks[0].shape
    tile = math.gcd(rows, 48)
    width = count * part
    return pl.pallas_call(
        functools.partial(unpack_kernel, part),
        grid=(rows // tile,),
        out_shape=[jax.ShapeDtypeStruct((rows, width), jnp.float32)] * 3,
        in_specs=[pl.BlockSpec((tile, columns), lambda i: (i, 0))] * count,
        out_specs=[pl.BlockSpec((tile, width), lambda i: (i, 0))] * 3,
    )(*blocks)


def finish_kernel(
    lanes, h_ref, a_ref, qkv_ref, mixed_ref, strip_ref, tail_ref,
    o_ref, tails_ref,
    made, came, held, chained, shared, total,
    send0, got0, sendc, gotc, sendt, gott, sends, gots, local_sem,
):
    outer, inner, tensor = lanes
    step = lax.axis_index("outer")
    row = lax.axis_index("inner")
    lane = lax.axis_index("tensor")
    rows = h_ref.shape[0] // (outer * inner)
    extra = strip_ref.shape[1]
    wide = qkv_ref.shape[1]
    left, right = step > 0, step < outer - 1

    def peer_row(shift):
        return lax.rem(row + shift, inner)

    def peer_lane(shift):
        return lax.rem(lane + shift, tensor)

    barrier = pltpu.get_barrier_semaphore()
    for shift in range(1, inner):
        pl.semaphore_signal(barrier, device_id=(step, peer_row(shift), lane), device_id_type=MESH)
    for shift in range(1, tensor):
        pl.semaphore_signal(barrier, device_id=(step, row, peer_lane(shift)), device_id_type=MESH)
    for there, move in ((left, -1), (right, 1)):

        @pl.when(there)
        def _(move=move):
            pl.semaphore_signal(barrier, device_id=(step + move, row, lane), device_id_type=MESH)

    pl.semaphore_wait(
        barrier, inner + tensor - 2 + left.astype(jnp.int32) + right.astype(jnp.int32)
    )

    def make(index):
        window = pl.ds(pl.multiple_of(index * rows, rows), rows)
        made[index, :rows, :wide] = jnp.dot(
            h_ref[window, :], qkv_ref[...], preferred_element_type=jnp.float32
        ).astype(made.dtype)
        made[index, :rows, wide:] = jnp.dot(
            a_ref[window, :], mixed_ref[...], preferred_element_type=jnp.float32
        ).astype(made.dtype)
        made[index, rows:, :] = strip_ref[index]

    def remote(source, target, send_at, recv_at, device):
        return pltpu.make_async_remote_copy(
            src_ref=source,
            dst_ref=target,
            send_sem=send_at,
            recv_sem=recv_at,
            device_id=device,
            device_id_type=MESH,
        )

    orders = [sorted(range(outer), key=lambda p, at=at: -abs(p - at)) for at in range(outer)]

    def place(j):
        position = 0
        for at in range(outer):
            for number in range(outer):
                chosen = (step == at).astype(jnp.int32) * (j == number).astype(jnp.int32)
                position = position + chosen * orders[at][number]
        return position

    def row_copy(k):
        shift = 1 + lax.div(k, outer)
        position = place(lax.rem(k, outer))
        there = peer_row(shift)
        return position * inner + there, remote(
            made.at[position * inner + there],
            came.at[shift - 1, position],
            send0.at[shift - 1, position],
            got0.at[shift - 1, position],
            (step, there, lane),
        )

    def first(k, carry):
        index, copy = row_copy(k)
        make(index)
        copy.start()
        return carry

    lax.fori_loop(0, outer * (inner - 1), first, 0)

    def tail_copy(shift):
        return remote(
            tail_ref,
            tails_ref.at[lane],
            sendt.at[shift - 1],
            gott.at[shift - 1],
            (step, row, peer_lane(shift)),
        )

    local = pltpu.make_async_copy(tail_ref, tails_ref.at[lane], local_sem)
    local.start()
    for shift in range(1, tensor):
        tail_copy(shift).start()

    def second(j, carry):
        make(place(j) * inner + row)
        return carry

    lax.fori_loop(0, outer, second, 0)

    visits = []
    for distance in range(outer - 1, -1, -1):
        if distance == 0:
            visits.append((None, step, 0))
        else:
            visits.append((step - distance >= 0, lax.rem(step - distance + outer, outer), -1))
            visits.append((step + distance < outer, lax.rem(step + distance, outer), 1))

    started = []
    for there, position, way in visits:
        parts = [made.at[position * inner + row]]
        for shift in range(1, inner):
            target = came.at[shift - 1, position]
            guarded(
                there,
                remote(
                    target,
                    target,
                    send0.at[shift - 1, position],
                    got0.at[shift - 1, position],
                    (step, row, lane),
                ).wait_recv,
            )
            parts.append(target)

        def linked(side, position=position):
            target = chained.at[side, position]
            return remote(
                target, target, sendc.at[position], gotc.at[side, position], (step, row, lane)
            )

        if way == 0:
            for side, exists in ((0, left), (1, right)):
                guarded(exists, linked(side).wait_recv)
            inside = jnp.logical_and(left, right)
            add_into(total, parts + [chained.at[0, position], chained.at[1, position]], inside)
            add_into(total, parts + [chained.at[1, position]], jnp.logical_not(left))
            add_into(total, parts + [chained.at[0, position]], jnp.logical_not(right))
        else:
            side = 1 if way == -1 else 0
            link = right if way == -1 else left
            more, alone = jnp.logical_and(there, link), jnp.logical_and(there, jnp.logical_not(link))
            guarded(more, linked(side).wait_recv)
            add_into(held.at[position], parts + [chained.at[side, position]], more)
            add_into(held.at[position], parts, alone)
            copy = remote(
                held.at[position],
                chained.at[side, position],
                sendc.at[position],
                gotc.at[side, position],
                (step + way, row, lane),
            )
            guarded(there, copy.start)
            started.append((there, copy))

    strip = total.at[pl.ds(rows, extra), :]
    small = [
        remote(
            strip,
            shared.at[shift - 1],
            sends.at[shift - 1],
            gots.at[shift - 1],
            (step, row, peer_lane(shift)),
        )
        for shift in range(1, tensor)
    ]
    for copy in small:
        copy.start()
    o_ref[pl.ds(0, rows), :] = total[pl.ds(0, rows), :]
    summed = total[pl.ds(rows, extra), :]
    for shift in range(1, tensor):
        small[shift - 1].wait_recv()
        summed = summed + shared[shift - 1]
    o_ref[pl.ds(rows, extra), :] = summed

    for shift in range(1, tensor):
        small[shift - 1].wait_send()
        tail_copy(shift).wait()
    for there, copy in started:
        guarded(there, copy.wait_send)

    def drain(k, carry):
        row_copy(k)[1].wait_send()
        return carry

    lax.fori_loop(0, outer * (inner - 1), drain, 0)
    local.wait()


def finish(lanes, h_turned, a_turned, grad_qkv, mixed, strips, tail, collective_id):
    outer, inner, tensor = lanes
    low = h_turned.dtype
    count, extra, columns = strips.shape
    rows = h_turned.shape[0] // count
    block = (rows + extra, columns)
    peers = max(inner - 1, 1)
    vmem = pl.BlockSpec(memory_space=pltpu.VMEM)
    dma = pltpu.SemaphoreType.DMA
    return pl.pallas_call(
        functools.partial(finish_kernel, lanes),
        out_shape=[
            jax.ShapeDtypeStruct(block, jnp.float32),
            jax.ShapeDtypeStruct((tensor,) + tail.shape, low),
        ],
        in_specs=[vmem] * 6,
        out_specs=[vmem, pl.BlockSpec(memory_space=pl.ANY)],
        scratch_shapes=[
            pltpu.VMEM((count,) + block, low),
            pltpu.VMEM((peers, outer) + block, low),
            pltpu.VMEM((outer,) + block, low),
            pltpu.VMEM((2, outer) + block, low),
            pltpu.VMEM((tensor - 1, extra, columns), jnp.float32),
            pltpu.VMEM(block, jnp.float32),
            dma((peers, outer)),
            dma((peers, outer)),
            dma((outer,)),
            dma((2, outer)),
            dma((tensor - 1,)),
            dma((tensor - 1,)),
            dma((tensor - 1,)),
            dma((tensor - 1,)),
            dma,
        ],
        compiler_params=pltpu.CompilerParams(collective_id=collective_id, has_side_effects=True),
        cost_estimate=pl.CostEstimate(
            flops=2 * h_turned.size * columns,
            bytes_accessed=20 * count * rows * columns,
            transcendentals=0,
        ),
    )(h_turned, a_turned, grad_qkv, mixed, strips, tail)


def shards(
    lanes,
    layer_input,
    cotangent,
    seq_lengths,
    norm_attn_in,
    w_query,
    w_key,
    w_value,
    w_out,
    norm_attn_out,
    norm_ffn_in,
    w_gate,
    w_up,
    w_down,
    norm_ffn_out,
):
    outer, inner, tensor = lanes
    low = jnp.bfloat16
    shard_rows, width = w_gate.shape
    part = width // outer
    query_cols, key_cols = w_query.shape[1], w_key.shape[1]
    qkv_cols = query_cols + 2 * key_cols

    attn_shard = jnp.concatenate([w_query, w_key, w_value, w_out.T], axis=1)
    attn_full = gather_blocks(attn_shard, lanes, True, ("inner",), 0)
    attn_full = attn_full.reshape(-1, attn_shard.shape[1])
    ffn_parts = pack(outer, part, w_gate, w_up, w_down.T)
    early = [step for step in range(1, outer) if step % 2 == 1]
    late = [step for step in range(1, outer) if step % 2 == 0]
    across = {0: ffn_parts[0]}
    for step in early:
        across[step] = shifted(ffn_parts[step], "outer", outer, step)
    beside = {(0, turn): shifted(across[0], "inner", inner, turn) for turn in range(1, inner)}
    held = {step: ffn_parts[step] for step in late}
    attn_full, across, held = lax.optimization_barrier((attn_full, across, held))
    for step in late:
        across[step] = shifted(held[step], "outer", outer, step)
    for step in early:
        for turn in range(1, inner):
            beside[step, turn] = shifted(across[step], "inner", inner, turn)
    for step in late:
        for turn in range(1, inner):
            beside[step, turn] = shifted(across[step], "inner", inner, turn)
    for step in range(outer):
        beside[step, 0] = across[step]

    row_count = layer_input.shape[0]
    split_rows = row_count // tensor
    first_row = lax.axis_index("tensor") * split_rows

    def own_rows(array):
        return lax.dynamic_slice_in_dim(array, first_row, split_rows, 0)

    is_live, allowed, cosine, sine_wave = layout(seq_lengths[0], row_count)
    kv_heads = key_cols // HD
    groups = H // KV
    layer_float = layer_input.astype(jnp.float32)
    h_attn = rms_scale(layer_float, norm_attn_in).astype(low)
    projected = matmul(h_attn, attn_full[:, :qkv_cols])
    query_pre = (
        projected[:, :query_cols].reshape(row_count, kv_heads, groups, HD).transpose(1, 2, 0, 3)
    )
    query = ((query_pre * cosine + rotate_half(query_pre) * sine_wave) * QUERY_SCALE).astype(low)
    key_pre = (
        projected[:, query_cols : query_cols + key_cols]
        .reshape(row_count, kv_heads, HD)
        .transpose(1, 0, 2)
    )
    keys = (key_pre * cosine + rotate_half(key_pre) * sine_wave).astype(low)
    values = (
        projected[:, query_cols + key_cols :]
        .astype(low)
        .reshape(row_count, kv_heads, HD)
        .transpose(1, 0, 2)
    )
    capped = capped_scores(query, keys)
    expo = jnp.where(allowed, jnp.exp(capped), 0.0)
    log_total = jnp.log(jnp.sum(expo, axis=-1, keepdims=True))
    weights = jnp.where(allowed, jnp.exp(capped - log_total), 0.0)
    probs = weights.astype(low)
    mixed = jnp.einsum("kgqs,ksd->kgqd", probs, values, preferred_element_type=jnp.float32).astype(
        low
    )
    mixed_flat = mixed.transpose(2, 0, 1, 3).reshape(row_count, -1)
    out_turned = attn_full[:, qkv_cols:]
    attn_branch = scatter_sum(
        right_product(mixed_flat, out_turned).astype(low).reshape(tensor, split_rows, -1),
        lanes,
        False,
        ("x", "core"),
        ("core", "x"),
        1,
    )
    layer_own = own_rows(layer_float)
    resid = layer_own + rms_scale(attn_branch, norm_attn_out)
    h_ffn = rms_scale(resid, norm_ffn_in).astype(low)

    last = [(step, turn) for step in late for turn in range(1, inner)]
    h_all, ffn_full = gather_blocks(
        h_ffn,
        lanes,
        True,
        ("x", "core"),
        2,
        {key: item for key, item in beside.items() if key not in last},
    )
    h_all = h_all.reshape(-1, h_ffn.shape[1])
    for step, turn in last:
        place = lax.rem(lax.axis_index("outer") - step + outer, outer) * inner
        place = place + lax.rem(lax.axis_index("inner") - turn + inner, inner)
        ffn_full = lax.dynamic_update_slice(ffn_full, beside[step, turn][None], (place, 0, 0))
    ffn_full = ffn_full.reshape(-1, 3 * part)
    gate_up = matmul(h_all, ffn_full[:, : 2 * part])
    gate_pre, up_pre = gate_up[:, :part], gate_up[:, part:]
    gelu_gate = gelu_tanh(gate_pre)
    hidden = (gelu_gate * up_pre).astype(low)
    down_full = ffn_full[:, 2 * part :]
    ffn_branch = product_scatter(hidden, ffn_full, (2 * part, 3 * part), lanes, True, 3)
    output_own = (resid + rms_scale(ffn_branch, norm_ffn_out)).astype(low)

    grad_out = own_rows(cotangent).astype(jnp.float32) * own_rows(
        is_live.astype(jnp.float32)[:, None]
    )
    _, pull_four = jax.vjp(rms_scale, ffn_branch, norm_ffn_out)
    grad_ffn_float, grad_norm_ffn_out = pull_four(grad_out)
    grad_ffn_all = gather_blocks(grad_ffn_float.astype(low), lanes, True, ("x", "core"), 4)
    grad_ffn_all = grad_ffn_all.reshape(-1, h_ffn.shape[1])
    grad_hidden = matmul(grad_ffn_all, down_full)
    grad_up = (grad_hidden * gelu_gate).astype(low)
    _, pull_gelu = jax.vjp(gelu_tanh, gate_pre)
    grad_gate = pull_gelu(grad_hidden * up_pre)[0].astype(low)
    grad_both = jnp.concatenate([grad_gate, grad_up], axis=1)
    grad_h_ffn = product_scatter(grad_both, ffn_full, (0, 2 * part), lanes, True, 5)
    grad_w_ffn = weight_grads(h_all, grad_ffn_all, grad_both, hidden)
    grad_w_ffn = grad_w_ffn.reshape(outer, inner, shard_rows, 3 * part)
    here, row = lax.axis_index("outer"), lax.axis_index("inner")

    def grad_block(step, turn):
        place = (lax.rem(here + step, outer), lax.rem(row + turn, inner), 0, 0)
        return lax.dynamic_slice(grad_w_ffn, place, (1, 1, shard_rows, 3 * part))[0, 0]

    half = max(outer // 2, 1)
    groups_of_steps = (range(1, 1 + half), [*range(1 + half, outer), 0])
    outgoing = [
        {(step, turn): grad_block(step, turn) for step in steps for turn in range(1, inner)}
        for steps in groups_of_steps
    ]
    grad_h_ffn, outgoing[1] = lax.optimization_barrier((grad_h_ffn, outgoing[1]))

    def start_rows(number):
        return {
            key: shifted(item, "inner", inner, key[1]) for key, item in outgoing[number].items()
        }

    def sum_rows(number, came):
        summed = {}
        for step in groups_of_steps[number]:
            total = grad_block(step, 0).astype(jnp.float32)
            for turn in range(1, inner):
                total = total + came[step, turn].astype(jnp.float32)
            summed[step] = total.astype(low)
        return summed

    def send_rows(summed):
        return {
            step: shifted(item, "outer", outer, step) if step else item
            for step, item in summed.items()
        }

    rows_now = sum_rows(0, start_rows(0))
    rows_later = start_rows(1)

    _, pull_three = jax.vjp(rms_scale, resid, norm_ffn_in)
    grad_resid_part, grad_norm_ffn_in = pull_three(grad_h_ffn)
    grad_resid = grad_out + grad_resid_part
    _, pull_two = jax.vjp(rms_scale, attn_branch, norm_attn_out)
    grad_attn_float, grad_norm_attn_out = pull_two(grad_resid)
    grad_attn_own, rows_now = lax.optimization_barrier((grad_attn_float.astype(low), rows_now))
    summed = send_rows(rows_now)
    grad_attn_branch = gather_blocks(
        grad_attn_own, lanes, False, ("x", "core"), 6
    ).reshape(row_count, -1)
    grad_mixed = matmul(grad_attn_branch, out_turned).astype(low)
    grad_mixed = grad_mixed.reshape(row_count, kv_heads, groups, HD).transpose(1, 2, 0, 3)
    grad_values = jnp.einsum(
        "kgqs,kgqd->ksd", probs, grad_mixed, preferred_element_type=jnp.float32
    ).astype(low)
    grad_probs = jnp.einsum(
        "kgqd,ksd->kgqs", grad_mixed, values, preferred_element_type=jnp.float32
    )
    row_delta = jnp.sum(weights * grad_probs, axis=-1, keepdims=True)
    tanh_part = capped / SOFT_CAP
    grad_scores = (weights * (grad_probs - row_delta) * (1.0 - tanh_part * tanh_part)).astype(low)
    grad_scores, rows_later = lax.optimization_barrier((grad_scores, rows_later))
    summed.update(send_rows(sum_rows(1, rows_later)))
    sum_gate, sum_up, sum_down = unpack([summed[step] for step in range(outer)], part)
    sum_down = sum_down.T
    grad_query_raw = jnp.einsum(
        "kgqs,ksd->kgqd", grad_scores, keys, preferred_element_type=jnp.float32
    )
    grad_query = (
        (grad_query_raw * cosine - rotate_half(grad_query_raw) * sine_wave) * QUERY_SCALE
    ).astype(low)
    grad_keys_raw = jnp.einsum(
        "kgqs,kgqd->ksd", grad_scores, query, preferred_element_type=jnp.float32
    )
    grad_keys = (grad_keys_raw * cosine - rotate_half(grad_keys_raw) * sine_wave).astype(low)
    grad_qkv = jnp.concatenate(
        [
            grad_query.transpose(2, 0, 1, 3).reshape(row_count, -1),
            grad_keys.transpose(1, 0, 2).reshape(row_count, -1),
            grad_values.transpose(1, 0, 2).reshape(row_count, -1),
        ],
        axis=1,
    )
    grad_a_part = right_product(grad_qkv, attn_full[:, :qkv_cols]).astype(low)
    grad_h_attn = scatter_sum(
        grad_a_part.reshape(tensor, split_rows, -1),
        lanes,
        False,
        ("x", "core"),
        ("core", "x"),
        7,
    )
    _, pull_one = jax.vjp(rms_scale, layer_own, norm_attn_in)
    grad_input_part, grad_norm_attn_in = pull_one(grad_h_attn)
    input_own = grad_resid + grad_input_part

    norm_rows = jnp.stack(
        [grad_norm_attn_in, grad_norm_attn_out, grad_norm_ffn_in, grad_norm_ffn_out]
    )
    strips = norm_rows.reshape(4, outer * inner, shard_rows).transpose(1, 0, 2)
    strips = strips.reshape(outer * inner, 1, -1).astype(low)
    attn_cols = attn_shard.shape[1]
    strips = jnp.pad(strips, ((0, 0), (0, 15), (0, attn_cols - strips.shape[2])))
    tail = jnp.concatenate([output_own, input_own.astype(low)], axis=0)
    sum_last, tails = finish(
        lanes, h_attn.T, grad_attn_branch.T, grad_qkv, mixed_flat, strips, tail, 8
    )
    layer_output = tails[:, :split_rows].reshape(row_count, -1)
    input_grad = tails[:, split_rows:].reshape(row_count, -1).astype(jnp.float32)
    sum_attn_in, sum_attn_out, sum_ffn_in, sum_ffn_out = (
        sum_last[shard_rows, i * shard_rows : (i + 1) * shard_rows] for i in range(4)
    )
    sum_last = sum_last[:shard_rows]
    sum_out = sum_last[:, qkv_cols:].T
    sum_query = sum_last[:, :query_cols]
    sum_key = sum_last[:, query_cols : query_cols + key_cols]
    sum_value = sum_last[:, query_cols + key_cols : qkv_cols]
    return (
        layer_output,
        input_grad,
        sum_attn_in,
        sum_query,
        sum_key,
        sum_value,
        sum_out,
        sum_attn_out,
        sum_ffn_in,
        sum_gate,
        sum_up,
        sum_down,
        sum_ffn_out,
    )


def solution(mesh):
    dp_size, tensor = mesh.shape["dp"], mesh.shape["tensor"]
    outer = math.gcd(4, dp_size)
    lanes = (outer, dp_size // outer, tensor)
    split = Mesh(mesh.devices.reshape(lanes), ("outer", "inner", "tensor"))
    dp = ("outer", "inner")

    def run(*args):
        return jax.shard_map(
            lambda *blocks: shards(lanes, *blocks),
            mesh=split,
            in_specs=(
                P(dp, None),
                P(dp, None),
                P(dp, None),
                P(),
                P(dp, "tensor"),
                P(dp, "tensor"),
                P(dp, "tensor"),
                P("tensor", dp),
                P(),
                P(),
                P(dp, "tensor"),
                P(dp, "tensor"),
                P("tensor", dp),
                P(),
            ),
            out_specs=(
                P(dp, None),
                P(dp, None),
                P(dp),
                P(dp, "tensor"),
                P(dp, "tensor"),
                P(dp, "tensor"),
                P("tensor", dp),
                P(dp),
                P(dp),
                P(dp, "tensor"),
                P(dp, "tensor"),
                P("tensor", dp),
                P(dp),
            ),
            check_vma=False,
        )(*args)

    return run
```

```python
import functools
import math

import jax
import jax.numpy as jnp
from jax import lax
from jax.experimental import pallas as pl
from jax.experimental.pallas import tpu as pltpu
from jax.sharding import Mesh, PartitionSpec as P

H = 8
KV = 4
HD = 256


EPSILON = 1e-06
SOFT_CAP = 50.0
QUERY_SCALE = 0.0625
GELU_COEFF = 0.7978845608028654

MESH = pl.DeviceIdType.MESH


def rms_scale(values, scales):
    return values * lax.rsqrt(jnp.mean(values * values, axis=-1, keepdims=True) + EPSILON) * scales


def gelu_tanh(inputs):
    return (
        0.5 * inputs * (1.0 + jnp.tanh(GELU_COEFF * (inputs + 0.044715 * inputs * inputs * inputs)))
    )


def rotate_half(heads):
    middle = heads.shape[-1] // 2
    return jnp.concatenate([-heads[..., middle:], heads[..., :middle]], axis=-1)


def layout(lengths, row_count):
    seq_ends = jnp.cumsum(lengths)
    row_index = jnp.arange(row_count, dtype=jnp.int32)
    passed = (row_index[:, None] >= seq_ends[None, :]).astype(jnp.int32)
    segment = jnp.sum(passed, axis=1)
    is_live = row_index < seq_ends[-1]
    seq_ident = jnp.where(is_live, segment, lengths.shape[0] + row_index)
    offset = row_index - jnp.sum(passed * lengths[None, :], axis=1)
    allowed = (seq_ident[:, None] == seq_ident[None, :]) & (
        row_index[None, :] <= row_index[:, None]
    )
    middle = HD // 2
    inverse = jnp.exp(jnp.arange(middle, dtype=jnp.float32) * (-2.0 * math.log(10000.0) / HD))
    angles = offset.astype(jnp.float32)[:, None] * inverse[None, :]
    cosine = jnp.concatenate([jnp.cos(angles), jnp.cos(angles)], axis=1)
    sine_wave = jnp.concatenate([jnp.sin(angles), jnp.sin(angles)], axis=1)
    return (is_live, allowed, cosine, sine_wave)


def matmul(left, right):
    return jnp.dot(left, right, preferred_element_type=jnp.float32)


def right_product(left, right):
    return jnp.einsum("tc,dc->td", left, right, preferred_element_type=jnp.float32)


def capped_scores(query, keys):
    raw_scores = jnp.einsum("kgqd,ksd->kgqs", query, keys, preferred_element_type=jnp.float32)
    return SOFT_CAP * jnp.tanh(raw_scores / SOFT_CAP)


def shifted(block, axis, size, step):
    return lax.ppermute(block, axis, [(i, (i + step) % size) for i in range(size)])


def pack_kernel(part, g_ref, u_ref, d_ref, *o_refs):
    count = len(o_refs)
    here = lax.axis_index("outer")
    tile = math.gcd(g_ref.shape[0], 16)
    for step, o_ref in enumerate(o_refs):
        for source in range(count):

            @pl.when(lax.rem(here + step, count) == source)
            def _(o_ref=o_ref, source=source):
                def body(r, carry):
                    window = pl.ds(pl.multiple_of(r * tile, tile), tile)
                    for j, ref in enumerate((g_ref, u_ref, d_ref)):
                        o_ref[window, j * part : (j + 1) * part] = ref[
                            window, source * part : (source + 1) * part
                        ]
                    return carry

                lax.fori_loop(0, g_ref.shape[0] // tile, body, 0)


def pack(count, part, gate, up, down_turned):
    rows, width = gate.shape
    tile = math.gcd(rows, 48)
    return pl.pallas_call(
        functools.partial(pack_kernel, part),
        grid=(rows // tile,),
        out_shape=[jax.ShapeDtypeStruct((rows, 3 * part), gate.dtype)] * count,
        in_specs=[pl.BlockSpec((tile, width), lambda i: (i, 0))] * 3,
        out_specs=[pl.BlockSpec((tile, 3 * part), lambda i: (i, 0))] * count,
        cost_estimate=pl.CostEstimate(
            flops=0, bytes_accessed=12 * gate.size, transcendentals=0
        ),
    )(gate, up, down_turned)


def device_layout(lanes):
    _, inner, tensor = lanes
    cores = 2 if tensor % 2 == 0 else 1
    return {"inner": inner, "x": tensor // cores, "core": cores}


class Spot:
    def __init__(self, lanes, chain, levels):
        self.sizes = device_layout(lanes)
        self.chain, self.levels = chain, levels
        self.length = lanes[0] if chain else 1
        self.at_chain = lax.axis_index("outer")
        tensor = lax.axis_index("tensor")
        cores = self.sizes["core"]
        self.here = {
            "inner": lax.axis_index("inner"),
            "x": lax.div(tensor, cores),
            "core": lax.rem(tensor, cores),
        }
        self.step = self.at_chain if chain else 0
        self.slots = {}
        for level in levels:
            for shift in range(1, self.sizes[level]):
                self.slots[level, shift] = 2 + len(self.slots)

    def moved(self, **shifts):
        at = dict(self.here)
        for level, shift in shifts.items():
            at[level] = lax.rem(at[level] + shift, self.sizes[level])
        return at

    def device(self, at, chain_shift=0):
        return (
            self.at_chain + chain_shift,
            at["inner"],
            at["x"] * self.sizes["core"] + at["core"],
        )

    def flat(self, step, at):
        index = step
        for level in self.levels:
            index = index * self.sizes[level] + at[level]
        return index

    def greet(self):
        barrier = pltpu.get_barrier_semaphore()
        count = 0
        for level in self.levels:
            for shift in range(1, self.sizes[level]):
                pl.semaphore_signal(
                    barrier, device_id=self.device(self.moved(**{level: shift})), device_id_type=MESH
                )
                count += 1
        if self.length > 1:
            for shift, there in ((-1, self.step > 0), (1, self.step < self.length - 1)):
                count = count + there.astype(jnp.int32)

                @pl.when(there)
                def _(shift=shift):
                    pl.semaphore_signal(
                        barrier, device_id=self.device(self.here, shift), device_id_type=MESH
                    )

        pl.semaphore_wait(barrier, count)


def guarded(condition, action):
    if condition is None:
        action()
    else:
        pl.when(condition)(action)


def both(first, second):
    if first is None:
        return second
    return first if second is None else jnp.logical_and(first, second)


def gather_kernel(lanes, chain, levels, places, *refs):
    held_refs, refs = refs[1 : 1 + len(places)], refs[:1] + refs[1 + len(places) :]
    if places:
        x_ref, o_ref, placed_ref, send_sem, recv_sem, local_sem, place_sem = refs
    else:
        x_ref, o_ref, send_sem, recv_sem, local_sem = refs
    spot = Spot(lanes, chain, levels)
    length, step, here = spot.length, spot.step, spot.here
    started = []

    def send(condition, source, index, slot, device):
        def copy():
            return pltpu.make_async_remote_copy(
                src_ref=source,
                dst_ref=o_ref.at[index],
                send_sem=send_sem.at[slot, index],
                recv_sem=recv_sem.at[index],
                device_id=device,
                device_id_type=MESH,
            )

        guarded(condition, lambda: copy().start())
        started.append((condition, copy))

    def arrive(condition, index):
        def wait():
            pltpu.make_async_remote_copy(
                src_ref=o_ref.at[index],
                dst_ref=o_ref.at[index],
                send_sem=send_sem.at[0, index],
                recv_sem=recv_sem.at[index],
                device_id=spot.device(here),
                device_id_type=MESH,
            ).wait_recv()

        guarded(condition, wait)

    def spread(condition, source, index, first):
        for level in levels[first:]:
            for shift in range(1, spot.sizes[level]):
                send(
                    condition,
                    source,
                    index,
                    spot.slots[level, shift],
                    spot.device(spot.moved(**{level: shift})),
                )

    def around(distance):
        if distance == 0:
            return [(None, step)]
        return [(step - distance >= 0, step - distance), (step + distance < length, step + distance)]

    def clipped(position):
        return lax.rem(position + length, length) if length > 1 else position

    spot.greet()
    mine = spot.flat(step, here)
    local = pltpu.make_async_copy(x_ref, o_ref.at[mine], local_sem)
    local.start()
    if length > 1:
        send(step < length - 1, x_ref, mine, 1, spot.device(here, 1))
        send(step > 0, x_ref, mine, 0, spot.device(here, -1))
    spread(None, x_ref, mine, 0)

    outer, inner, _ = lanes
    moves = []
    for number, (back, turn) in enumerate(places):
        index = lax.rem(lax.axis_index("outer") - back + outer, outer) * inner
        index = index + lax.rem(lax.axis_index("inner") - turn + inner, inner)
        moves.append(
            pltpu.make_async_copy(
                held_refs[number], placed_ref.at[index], place_sem.at[number]
            )
        )
        moves[-1].start()

    def relay(distance):
        if len(levels) < 2:
            return
        level = levels[0]
        for there, position in around(distance):
            for shift in range(1, spot.sizes[level]):
                index = spot.flat(clipped(position), spot.moved(**{level: shift}))
                arrive(there, index)
                spread(there, o_ref.at[index], index, 1)

    for distance in range(1, length):
        for way, (there, position) in enumerate(around(distance)):
            index = spot.flat(clipped(position), here)
            arrive(there, index)
            onward = step < length - 1 if way == 0 else step > 0
            send(
                both(there, onward),
                o_ref.at[index],
                index,
                1 - way,
                spot.device(here, 1 if way == 0 else -1),
            )
            spread(there, o_ref.at[index], index, 0)
        relay(distance - 1)
    relay(length - 1)
    last = levels[-1]
    others = [{}]
    for level in levels[:-1]:
        others = [{**rest, level: shift} for rest in others for shift in range(spot.sizes[level])]
    for position in range(length):
        for rest in others:
            for shift in range(1, spot.sizes[last]):
                arrive(None, spot.flat(position, spot.moved(**{**rest, last: shift})))
    for condition, copy in started:
        guarded(condition, lambda copy=copy: copy().wait_send())
    for move in moves:
        move.wait()
    local.wait()


def gather_blocks(block, lanes, chain, levels, collective_id, held=None):
    held = held or {}
    places = tuple(held)
    blocks = [held[key] for key in places]
    sizes = device_layout(lanes)
    count = (lanes[0] if chain else 1) * math.prod(sizes[level] for level in levels)
    slots = 2 + sum(sizes[level] - 1 for level in levels)
    out_shape = [jax.ShapeDtypeStruct((count,) + block.shape, block.dtype)]
    scratch = [
        pltpu.SemaphoreType.DMA((slots, count)),
        pltpu.SemaphoreType.DMA((count,)),
        pltpu.SemaphoreType.DMA,
    ]
    if held:
        out_shape.append(
            jax.ShapeDtypeStruct((lanes[0] * lanes[1],) + blocks[0].shape, blocks[0].dtype)
        )
        scratch.append(pltpu.SemaphoreType.DMA((len(blocks),)))
    results = pl.pallas_call(
        functools.partial(gather_kernel, lanes, chain, levels, places),
        out_shape=out_shape,
        in_specs=[pl.BlockSpec(memory_space=pltpu.VMEM)] * (1 + len(blocks)),
        out_specs=[pl.BlockSpec(memory_space=pl.ANY)] * len(out_shape),
        scratch_shapes=scratch,
        compiler_params=pltpu.CompilerParams(collective_id=collective_id, has_side_effects=True),
        cost_estimate=pl.CostEstimate(
            flops=0, bytes_accessed=20 * count * block.size, transcendentals=0
        ),
    )(block, *blocks)
    return results if held else results[0]


def add_into(target, parts, condition=None):
    rows = target.shape[0]
    tile = math.gcd(rows, 16)

    def action():
        def body(r, carry):
            window = pl.ds(pl.multiple_of(r * tile, tile), tile)
            total = parts[0][window, :].astype(jnp.float32)
            for part in parts[1:]:
                total = total + part[window, :].astype(jnp.float32)
            target[window, :] = total.astype(target.dtype)
            return carry

        lax.fori_loop(0, rows // tile, body, 0)

    guarded(condition, action)


def scatter_kernel(
    lanes, chain, levels, order, x_ref, o_ref, came0, came1, held0, held1, chained, sems, got0, got1, gotc
):
    spot = Spot(lanes, chain, levels)
    length, step, here = spot.length, spot.step, spot.here
    started = []

    def send(condition, source, target, send_at, recv_at, device):
        def copy():
            return pltpu.make_async_remote_copy(
                src_ref=source,
                dst_ref=target,
                send_sem=send_at,
                recv_sem=recv_at,
                device_id=device,
                device_id_type=MESH,
            )

        guarded(condition, lambda: copy().start())
        started.append((condition, copy))

    def arrive(condition, target, recv_at):
        def wait():
            pltpu.make_async_remote_copy(
                src_ref=target,
                dst_ref=target,
                send_sem=recv_at,
                recv_sem=recv_at,
                device_id=spot.device(here),
                device_id_type=MESH,
            ).wait_recv()

        guarded(condition, wait)

    visits = []
    for distance in range(length - 1, -1, -1):
        if distance == 0:
            visits.append((None, step, 0))
        else:
            visits.append(
                (step - distance >= 0, lax.rem(step - distance + length, length), -1)
            )
            visits.append((step + distance < length, lax.rem(step + distance, length), 1))

    spot.greet()
    first = order[0]
    second = order[1] if len(order) > 1 else None
    n_first = spot.sizes[first]
    n_second = spot.sizes[second] if second else 1

    def second_shifts(own):
        return [0] if own else list(range(1, n_second))

    for own in (False, True):
        for there, position, _ in visits:
            for other in second_shifts(own):
                for shift in range(1, n_first):
                    where = {first: shift}
                    if second:
                        where[second] = other
                    at = spot.moved(**where)
                    lane = position * n_second + (at[second] if second else 0)
                    send(
                        there,
                        x_ref.at[spot.flat(position, at)],
                        came0.at[shift - 1, lane],
                        sems.at[shift - 1, lane],
                        got0.at[shift - 1, lane],
                        spot.device(spot.moved(**{first: shift})),
                    )

    def first_sum(there, position, other):
        at = spot.moved(**({second: other} if second else {}))
        lane = position * n_second + (at[second] if second else 0)
        parts = [x_ref.at[spot.flat(position, at)]]
        for shift in range(1, n_first):
            arrive(there, came0.at[shift - 1, lane], got0.at[shift - 1, lane])
            parts.append(came0.at[shift - 1, lane])
        return parts

    for there, position, _ in visits:
        for other in second_shifts(False):
            parts = first_sum(there, position, other)
            add_into(held0.at[other - 1, position], parts, there)
            send(
                there,
                held0.at[other - 1, position],
                came1.at[other - 1, position],
                sems.at[n_first - 1 + other - 1, position],
                got1.at[other - 1, position],
                spot.device(spot.moved(**{second: other})),
            )
    base = n_first - 1 + n_second - 1
    for there, position, way in visits:
        parts = first_sum(there, position, 0)
        for other in second_shifts(False):
            arrive(there, came1.at[other - 1, position], got1.at[other - 1, position])
            parts.append(came1.at[other - 1, position])
        if way == 0:
            if length > 1:
                for side, exists in ((0, step > 0), (1, step < length - 1)):
                    arrive(exists, chained.at[side, position], gotc.at[side, position])

                def extra(sides):
                    return parts + [chained.at[side, position] for side in sides]

                inside = jnp.logical_and(step > 0, step < length - 1)
                add_into(o_ref, extra((0, 1)), inside)
                add_into(o_ref, extra((1,)), step == 0)
                add_into(o_ref, extra((0,)), step == length - 1)
            else:
                add_into(o_ref, parts)
        else:
            side = 1 if way == -1 else 0
            inner_link = step < length - 1 if way == -1 else step > 0
            with_more = both(there, inner_link)
            alone = both(there, jnp.logical_not(inner_link))
            arrive(with_more, chained.at[side, position], gotc.at[side, position])
            add_into(held1.at[position], parts + [chained.at[side, position]], with_more)
            add_into(held1.at[position], parts, alone)
            send(
                there,
                held1.at[position],
                chained.at[side, position],
                sems.at[base, position],
                gotc.at[side, position],
                spot.device(here, way),
            )
    for condition, copy in started:
        guarded(condition, lambda copy=copy: copy().wait_send())


def scatter_sum(blocks, lanes, chain, levels, order, collective_id, kind=jnp.float32):
    sizes = device_layout(lanes)
    length = lanes[0] if chain else 1
    rows, columns = blocks.shape[1:]
    low = blocks.dtype
    n_first = sizes[order[0]]
    n_second = sizes[order[1]] if len(order) > 1 else 1
    extra = max(n_first - 1, 1)
    further = max(n_second - 1, 1)
    return pl.pallas_call(
        functools.partial(scatter_kernel, lanes, chain, levels, order),
        out_shape=jax.ShapeDtypeStruct((rows, columns), kind),
        in_specs=[pl.BlockSpec(memory_space=pltpu.VMEM)],
        out_specs=pl.BlockSpec(memory_space=pltpu.VMEM),
        scratch_shapes=[
            pltpu.VMEM((extra, length * n_second, rows, columns), low),
            pltpu.VMEM((further, length, rows, columns), low),
            pltpu.VMEM((further, length, rows, columns), low),
            pltpu.VMEM((length, rows, columns), low),
            pltpu.VMEM((2, length, rows, columns), low),
            pltpu.SemaphoreType.DMA((n_first + n_second, length * n_second)),
            pltpu.SemaphoreType.DMA((extra, length * n_second)),
            pltpu.SemaphoreType.DMA((further, length)),
            pltpu.SemaphoreType.DMA((2, length)),
        ],
        compiler_params=pltpu.CompilerParams(collective_id=collective_id, has_side_effects=True),
        cost_estimate=pl.CostEstimate(
            flops=0, bytes_accessed=20 * blocks.size, transcendentals=0
        ),
    )(blocks)


def product_scatter_kernel(
    lanes, chain, columns, left_ref, right_ref, o_ref,
    made, came0, came1, held0, held1, chained, send0, send1, sendc, got0, got1, gotc,
):
    spot = Spot(lanes, chain, ("x", "core"))
    length, step, here = spot.length, spot.step, spot.here
    n_x, n_core = spot.sizes["x"], spot.sizes["core"]
    rows = o_ref.shape[0]
    begin, end = columns
    started = []

    def remote(source, target, send_at, recv_at, device):
        return pltpu.make_async_remote_copy(
            src_ref=source,
            dst_ref=target,
            send_sem=send_at,
            recv_sem=recv_at,
            device_id=device,
            device_id_type=MESH,
        )

    def arrive(condition, target, recv_at):
        copy = remote(target, target, recv_at, recv_at, spot.device(here))
        guarded(condition, copy.wait_recv)

    span = n_x * n_core

    def make(position):
        window = pl.ds(pl.multiple_of(position * span * rows, span * rows), span * rows)
        product = lax.dot_general(
            left_ref[window, :],
            right_ref[:, begin:end],
            (((1,), (1,)), ((), ())),
            preferred_element_type=jnp.float32,
        ).astype(made.dtype)
        for lane in range(span):
            made[position * span + lane] = product[lane * rows : (lane + 1) * rows]

    orders = [sorted(range(length), key=lambda p, at=at: -abs(p - at)) for at in range(length)]

    def place(j):
        position = 0
        for at in range(length):
            for number in range(length):
                chosen = (step == at).astype(jnp.int32) * (j == number).astype(jnp.int32)
                position = position + chosen * orders[at][number]
        return position

    def core_copy(position, x_shift, shift):
        at_x = spot.moved(x=x_shift)["x"]
        peer = spot.moved(core=shift)
        lane = position * n_x + at_x
        return remote(
            made.at[lane * n_core + peer["core"]],
            came0.at[shift - 1, lane],
            send0.at[shift - 1, lane],
            got0.at[shift - 1, lane],
            spot.device(peer),
        )

    def x_copy(position, shift):
        return remote(
            held0.at[shift - 1, position],
            came1.at[shift - 1, position],
            send1.at[shift - 1, position],
            got1.at[shift - 1, position],
            spot.device(spot.moved(x=shift)),
        )

    def core_parts(there, position, shift_x):
        lane = position * n_x + spot.moved(x=shift_x)["x"]
        parts = [made.at[lane * n_core + here["core"]]]
        for shift in range(1, n_core):
            arrive(there, came0.at[shift - 1, lane], got0.at[shift - 1, lane])
            parts.append(came0.at[shift - 1, lane])
        return parts

    spot.greet()

    def produce(j, carry):
        @pl.when(j < length)
        def _():
            position = place(j)
            make(position)
            for x_shift in (*range(1, n_x), 0):
                for shift in range(1, n_core):
                    core_copy(position, x_shift, shift).start()

        @pl.when(j > 0)
        def _():
            position = place(j - 1)
            for shift in range(1, n_x):
                add_into(held0.at[shift - 1, position], core_parts(None, position, shift))
                x_copy(position, shift).start()

        return carry

    lax.fori_loop(0, length + 1, produce, 0)

    visits = []
    for distance in range(length - 1, -1, -1):
        if distance == 0:
            visits.append((None, step, 0))
        else:
            visits.append(
                (step - distance >= 0, lax.rem(step - distance + length, length), -1)
            )
            visits.append((step + distance < length, lax.rem(step + distance, length), 1))

    for there, position, way in visits:
        parts = core_parts(there, position, 0)
        for shift in range(1, n_x):
            arrive(there, came1.at[shift - 1, position], got1.at[shift - 1, position])
            parts.append(came1.at[shift - 1, position])
        if length == 1:
            add_into(o_ref, parts)
        elif way == 0:
            left, right = step > 0, step < length - 1
            for side, exists in ((0, left), (1, right)):
                arrive(exists, chained.at[side, position], gotc.at[side, position])
            sides = [chained.at[0, position], chained.at[1, position]]
            add_into(o_ref, parts + sides, jnp.logical_and(left, right))
            add_into(o_ref, parts + sides[1:], jnp.logical_not(left))
            add_into(o_ref, parts + sides[:1], jnp.logical_not(right))
        else:
            side = 1 if way == -1 else 0
            link = step < length - 1 if way == -1 else step > 0
            more = jnp.logical_and(there, link)
            alone = jnp.logical_and(there, jnp.logical_not(link))
            arrive(more, chained.at[side, position], gotc.at[side, position])
            add_into(held1.at[position], parts + [chained.at[side, position]], more)
            add_into(held1.at[position], parts, alone)
            copy = remote(
                held1.at[position],
                chained.at[side, position],
                sendc.at[position],
                gotc.at[side, position],
                spot.device(here, way),
            )
            guarded(there, copy.start)
            started.append((there, copy))
    for condition, copy in started:
        guarded(condition, copy.wait_send)

    def drain(position, carry):
        for x_shift in range(n_x):
            for shift in range(1, n_core):
                core_copy(position, x_shift, shift).wait_send()
        for shift in range(1, n_x):
            x_copy(position, shift).wait_send()
        return carry

    lax.fori_loop(0, length, drain, 0)


def product_scatter(left, right, columns, lanes, chain, collective_id):
    sizes = device_layout(lanes)
    length = lanes[0] if chain else 1
    n_x, n_core = sizes["x"], sizes["core"]
    count = length * n_x * n_core
    block = (left.shape[0] // count, right.shape[0])
    low = left.dtype
    more_core, more_x = max(n_core - 1, 1), max(n_x - 1, 1)
    vmem = pl.BlockSpec(memory_space=pltpu.VMEM)
    dma = pltpu.SemaphoreType.DMA
    return pl.pallas_call(
        functools.partial(product_scatter_kernel, lanes, chain, columns),
        out_shape=jax.ShapeDtypeStruct(block, jnp.float32),
        in_specs=[vmem, vmem],
        out_specs=vmem,
        scratch_shapes=[
            pltpu.VMEM((count,) + block, low),
            pltpu.VMEM((more_core, length * n_x) + block, low),
            pltpu.VMEM((more_x, length) + block, low),
            pltpu.VMEM((more_x, length) + block, low),
            pltpu.VMEM((length,) + block, low),
            pltpu.VMEM((2, length) + block, low),
            dma((more_core, length * n_x)),
            dma((more_x, length)),
            dma((length,)),
            dma((more_core, length * n_x)),
            dma((more_x, length)),
            dma((2, length)),
        ],
        compiler_params=pltpu.CompilerParams(collective_id=collective_id, has_side_effects=True),
        cost_estimate=pl.CostEstimate(
            flops=2 * left.size * right.shape[0],
            bytes_accessed=40 * left.shape[0] * right.shape[0],
            transcendentals=0,
        ),
    )(left, right)


def weight_grads_kernel(h_ref, g_ref, both_ref, hidden_ref, o_ref):
    turned = (((0,), (0,)), ((), ()))
    wide = both_ref.shape[1]
    o_ref[:, :wide] = lax.dot_general(
        h_ref[...], both_ref[...], turned, preferred_element_type=jnp.float32
    ).astype(o_ref.dtype)
    o_ref[:, wide:] = lax.dot_general(
        g_ref[...], hidden_ref[...], turned, preferred_element_type=jnp.float32
    ).astype(o_ref.dtype)


def weight_grads(h_all, g_all, both, hidden):
    tokens, width = h_all.shape
    tile = math.gcd(width, 384)
    columns = both.shape[1] + hidden.shape[1]
    return pl.pallas_call(
        weight_grads_kernel,
        grid=(width // tile,),
        out_shape=jax.ShapeDtypeStruct((width, columns), h_all.dtype),
        in_specs=[
            pl.BlockSpec((tokens, tile), lambda i: (0, i)),
            pl.BlockSpec((tokens, tile), lambda i: (0, i)),
            pl.BlockSpec(both.shape, lambda i: (0, 0)),
            pl.BlockSpec(hidden.shape, lambda i: (0, 0)),
        ],
        out_specs=pl.BlockSpec((tile, columns), lambda i: (i, 0)),
        cost_estimate=pl.CostEstimate(
            flops=2 * tokens * width * columns,
            bytes_accessed=4 * tokens * width + 2 * width * columns,
            transcendentals=0,
        ),
    )(h_all, g_all, both, hidden)


def unpack_kernel(part, *refs):
    blocks, targets = refs[:-3], refs[-3:]
    count = len(blocks)
    here = lax.axis_index("outer")
    for step, x_ref in enumerate(blocks):
        for source in range(count):

            @pl.when(lax.rem(here - step + count, count) == source)
            def _(x_ref=x_ref, source=source):
                for j, target in enumerate(targets):
                    target[:, source * part : (source + 1) * part] = x_ref[
                        :, j * part : (j + 1) * part
                    ].astype(jnp.float32)


def unpack(blocks, part):
    count = len(blocks)
    rows, columns = blocks[0].shape
    tile = math.gcd(rows, 48)
    width = count * part
    return pl.pallas_call(
        functools.partial(unpack_kernel, part),
        grid=(rows // tile,),
        out_shape=[jax.ShapeDtypeStruct((rows, width), jnp.float32)] * 3,
        in_specs=[pl.BlockSpec((tile, columns), lambda i: (i, 0))] * count,
        out_specs=[pl.BlockSpec((tile, width), lambda i: (i, 0))] * 3,
    )(*blocks)


def finish_kernel(
    lanes, h_ref, a_ref, qkv_ref, mixed_ref, strip_ref, tail_ref,
    o_ref, tails_ref,
    made, came, held, chained, shared, total,
    send0, got0, sendc, gotc, sendt, gott, sends, gots, local_sem,
):
    outer, inner, tensor = lanes
    step = lax.axis_index("outer")
    row = lax.axis_index("inner")
    lane = lax.axis_index("tensor")
    rows = h_ref.shape[0] // (outer * inner)
    extra = strip_ref.shape[1]
    wide = qkv_ref.shape[1]
    left, right = step > 0, step < outer - 1

    def peer_row(shift):
        return lax.rem(row + shift, inner)

    def peer_lane(shift):
        return lax.rem(lane + shift, tensor)

    barrier = pltpu.get_barrier_semaphore()
    for shift in range(1, inner):
        pl.semaphore_signal(barrier, device_id=(step, peer_row(shift), lane), device_id_type=MESH)
    for shift in range(1, tensor):
        pl.semaphore_signal(barrier, device_id=(step, row, peer_lane(shift)), device_id_type=MESH)
    for there, move in ((left, -1), (right, 1)):

        @pl.when(there)
        def _(move=move):
            pl.semaphore_signal(barrier, device_id=(step + move, row, lane), device_id_type=MESH)

    pl.semaphore_wait(
        barrier, inner + tensor - 2 + left.astype(jnp.int32) + right.astype(jnp.int32)
    )

    def make(index):
        window = pl.ds(pl.multiple_of(index * rows, rows), rows)
        made[index, :rows, :wide] = jnp.dot(
            h_ref[window, :], qkv_ref[...], preferred_element_type=jnp.float32
        ).astype(made.dtype)
        made[index, :rows, wide:] = jnp.dot(
            a_ref[window, :], mixed_ref[...], preferred_element_type=jnp.float32
        ).astype(made.dtype)
        made[index, rows:, :] = strip_ref[index]

    def remote(source, target, send_at, recv_at, device):
        return pltpu.make_async_remote_copy(
            src_ref=source,
            dst_ref=target,
            send_sem=send_at,
            recv_sem=recv_at,
            device_id=device,
            device_id_type=MESH,
        )

    orders = [sorted(range(outer), key=lambda p, at=at: -abs(p - at)) for at in range(outer)]

    def place(j):
        position = 0
        for at in range(outer):
            for number in range(outer):
                chosen = (step == at).astype(jnp.int32) * (j == number).astype(jnp.int32)
                position = position + chosen * orders[at][number]
        return position

    def row_copy(k):
        shift = 1 + lax.div(k, outer)
        position = place(lax.rem(k, outer))
        there = peer_row(shift)
        return position * inner + there, remote(
            made.at[position * inner + there],
            came.at[shift - 1, position],
            send0.at[shift - 1, position],
            got0.at[shift - 1, position],
            (step, there, lane),
        )

    def first(k, carry):
        index, copy = row_copy(k)
        make(index)
        copy.start()
        return carry

    lax.fori_loop(0, outer * (inner - 1), first, 0)

    def tail_copy(shift):
        return remote(
            tail_ref,
            tails_ref.at[lane],
            sendt.at[shift - 1],
            gott.at[shift - 1],
            (step, row, peer_lane(shift)),
        )

    local = pltpu.make_async_copy(tail_ref, tails_ref.at[lane], local_sem)
    local.start()
    for shift in range(1, tensor):
        tail_copy(shift).start()

    def second(j, carry):
        make(place(j) * inner + row)
        return carry

    lax.fori_loop(0, outer, second, 0)

    visits = []
    for distance in range(outer - 1, -1, -1):
        if distance == 0:
            visits.append((None, step, 0))
        else:
            visits.append((step - distance >= 0, lax.rem(step - distance + outer, outer), -1))
            visits.append((step + distance < outer, lax.rem(step + distance, outer), 1))

    started = []
    for there, position, way in visits:
        parts = [made.at[position * inner + row]]
        for shift in range(1, inner):
            target = came.at[shift - 1, position]
            guarded(
                there,
                remote(
                    target,
                    target,
                    send0.at[shift - 1, position],
                    got0.at[shift - 1, position],
                    (step, row, lane),
                ).wait_recv,
            )
            parts.append(target)

        def linked(side, position=position):
            target = chained.at[side, position]
            return remote(
                target, target, sendc.at[position], gotc.at[side, position], (step, row, lane)
            )

        if way == 0:
            for side, exists in ((0, left), (1, right)):
                guarded(exists, linked(side).wait_recv)
            inside = jnp.logical_and(left, right)
            add_into(total, parts + [chained.at[0, position], chained.at[1, position]], inside)
            add_into(total, parts + [chained.at[1, position]], jnp.logical_not(left))
            add_into(total, parts + [chained.at[0, position]], jnp.logical_not(right))
        else:
            side = 1 if way == -1 else 0
            link = right if way == -1 else left
            more, alone = jnp.logical_and(there, link), jnp.logical_and(there, jnp.logical_not(link))
            guarded(more, linked(side).wait_recv)
            add_into(held.at[position], parts + [chained.at[side, position]], more)
            add_into(held.at[position], parts, alone)
            copy = remote(
                held.at[position],
                chained.at[side, position],
                sendc.at[position],
                gotc.at[side, position],
                (step + way, row, lane),
            )
            guarded(there, copy.start)
            started.append((there, copy))

    strip = total.at[pl.ds(rows, extra), :]
    small = [
        remote(
            strip,
            shared.at[shift - 1],
            sends.at[shift - 1],
            gots.at[shift - 1],
            (step, row, peer_lane(shift)),
        )
        for shift in range(1, tensor)
    ]
    for copy in small:
        copy.start()
    o_ref[pl.ds(0, rows), :] = total[pl.ds(0, rows), :]
    summed = total[pl.ds(rows, extra), :]
    for shift in range(1, tensor):
        small[shift - 1].wait_recv()
        summed = summed + shared[shift - 1]
    o_ref[pl.ds(rows, extra), :] = summed

    for shift in range(1, tensor):
        small[shift - 1].wait_send()
        tail_copy(shift).wait()
    for there, copy in started:
        guarded(there, copy.wait_send)

    def drain(k, carry):
        row_copy(k)[1].wait_send()
        return carry

    lax.fori_loop(0, outer * (inner - 1), drain, 0)
    local.wait()


def finish(lanes, h_turned, a_turned, grad_qkv, mixed, strips, tail, collective_id):
    outer, inner, tensor = lanes
    low = h_turned.dtype
    count, extra, columns = strips.shape
    rows = h_turned.shape[0] // count
    block = (rows + extra, columns)
    peers = max(inner - 1, 1)
    vmem = pl.BlockSpec(memory_space=pltpu.VMEM)
    dma = pltpu.SemaphoreType.DMA
    return pl.pallas_call(
        functools.partial(finish_kernel, lanes),
        out_shape=[
            jax.ShapeDtypeStruct(block, jnp.float32),
            jax.ShapeDtypeStruct((tensor,) + tail.shape, low),
        ],
        in_specs=[vmem] * 6,
        out_specs=[vmem, pl.BlockSpec(memory_space=pl.ANY)],
        scratch_shapes=[
            pltpu.VMEM((count,) + block, low),
            pltpu.VMEM((peers, outer) + block, low),
            pltpu.VMEM((outer,) + block, low),
            pltpu.VMEM((2, outer) + block, low),
            pltpu.VMEM((tensor - 1, extra, columns), jnp.float32),
            pltpu.VMEM(block, jnp.float32),
            dma((peers, outer)),
            dma((peers, outer)),
            dma((outer,)),
            dma((2, outer)),
            dma((tensor - 1,)),
            dma((tensor - 1,)),
            dma((tensor - 1,)),
            dma((tensor - 1,)),
            dma,
        ],
        compiler_params=pltpu.CompilerParams(collective_id=collective_id, has_side_effects=True),
        cost_estimate=pl.CostEstimate(
            flops=2 * h_turned.size * columns,
            bytes_accessed=20 * count * rows * columns,
            transcendentals=0,
        ),
    )(h_turned, a_turned, grad_qkv, mixed, strips, tail)


def shards(
    lanes,
    layer_input,
    cotangent,
    seq_lengths,
    norm_attn_in,
    w_query,
    w_key,
    w_value,
    w_out,
    norm_attn_out,
    norm_ffn_in,
    w_gate,
    w_up,
    w_down,
    norm_ffn_out,
):
    outer, inner, tensor = lanes
    low = jnp.bfloat16
    shard_rows, width = w_gate.shape
    part = width // outer
    query_cols, key_cols = w_query.shape[1], w_key.shape[1]
    qkv_cols = query_cols + 2 * key_cols

    attn_shard = jnp.concatenate([w_query, w_key, w_value, w_out.T], axis=1)
    attn_full = gather_blocks(attn_shard, lanes, True, ("inner",), 0)
    attn_full = attn_full.reshape(-1, attn_shard.shape[1])
    ffn_parts = pack(outer, part, w_gate, w_up, w_down.T)
    early = [step for step in range(1, outer) if step % 2 == 1]
    late = [step for step in range(1, outer) if step % 2 == 0]
    across = {0: ffn_parts[0]}
    for step in early:
        across[step] = shifted(ffn_parts[step], "outer", outer, step)
    beside = {(0, turn): shifted(across[0], "inner", inner, turn) for turn in range(1, inner)}
    held = {step: ffn_parts[step] for step in late}
    attn_full, across, held = lax.optimization_barrier((attn_full, across, held))
    for step in late:
        across[step] = shifted(held[step], "outer", outer, step)
    for step in early:
        for turn in range(1, inner):
            beside[step, turn] = shifted(across[step], "inner", inner, turn)
    for step in late:
        for turn in range(1, inner):
            beside[step, turn] = shifted(across[step], "inner", inner, turn)
    for step in range(outer):
        beside[step, 0] = across[step]

    row_count = layer_input.shape[0]
    split_rows = row_count // tensor
    first_row = lax.axis_index("tensor") * split_rows

    def own_rows(array):
        return lax.dynamic_slice_in_dim(array, first_row, split_rows, 0)

    is_live, allowed, cosine, sine_wave = layout(seq_lengths[0], row_count)
    kv_heads = key_cols // HD
    groups = H // KV
    layer_float = layer_input.astype(jnp.float32)
    h_attn = rms_scale(layer_float, norm_attn_in).astype(low)
    projected = matmul(h_attn, attn_full[:, :qkv_cols])
    query_pre = (
        projected[:, :query_cols].reshape(row_count, kv_heads, groups, HD).transpose(1, 2, 0, 3)
    )
    query = ((query_pre * cosine + rotate_half(query_pre) * sine_wave) * QUERY_SCALE).astype(low)
    key_pre = (
        projected[:, query_cols : query_cols + key_cols]
        .reshape(row_count, kv_heads, HD)
        .transpose(1, 0, 2)
    )
    keys = (key_pre * cosine + rotate_half(key_pre) * sine_wave).astype(low)
    values = (
        projected[:, query_cols + key_cols :]
        .astype(low)
        .reshape(row_count, kv_heads, HD)
        .transpose(1, 0, 2)
    )
    capped = capped_scores(query, keys)
    expo = jnp.where(allowed, jnp.exp(capped), 0.0)
    log_total = jnp.log(jnp.sum(expo, axis=-1, keepdims=True))
    weights = jnp.where(allowed, jnp.exp(capped - log_total), 0.0)
    probs = weights.astype(low)
    mixed = jnp.einsum("kgqs,ksd->kgqd", probs, values, preferred_element_type=jnp.float32).astype(
        low
    )
    mixed_flat = mixed.transpose(2, 0, 1, 3).reshape(row_count, -1)
    out_turned = attn_full[:, qkv_cols:]
    attn_branch = scatter_sum(
        right_product(mixed_flat, out_turned).astype(low).reshape(tensor, split_rows, -1),
        lanes,
        False,
        ("x", "core"),
        ("core", "x"),
        1,
    )
    layer_own = own_rows(layer_float)
    resid = layer_own + rms_scale(attn_branch, norm_attn_out)
    h_ffn = rms_scale(resid, norm_ffn_in).astype(low)

    last = [(step, turn) for step in late for turn in range(1, inner)]
    h_all, ffn_full = gather_blocks(
        h_ffn,
        lanes,
        True,
        ("x", "core"),
        2,
        {key: item for key, item in beside.items() if key not in last},
    )
    h_all = h_all.reshape(-1, h_ffn.shape[1])
    for step, turn in last:
        place = lax.rem(lax.axis_index("outer") - step + outer, outer) * inner
        place = place + lax.rem(lax.axis_index("inner") - turn + inner, inner)
        ffn_full = lax.dynamic_update_slice(ffn_full, beside[step, turn][None], (place, 0, 0))
    ffn_full = ffn_full.reshape(-1, 3 * part)
    gate_up = matmul(h_all, ffn_full[:, : 2 * part])
    gate_pre, up_pre = gate_up[:, :part], gate_up[:, part:]
    gelu_gate = gelu_tanh(gate_pre)
    hidden = (gelu_gate * up_pre).astype(low)
    down_full = ffn_full[:, 2 * part :]
    ffn_branch = product_scatter(hidden, ffn_full, (2 * part, 3 * part), lanes, True, 3)
    output_own = (resid + rms_scale(ffn_branch, norm_ffn_out)).astype(low)

    grad_out = own_rows(cotangent).astype(jnp.float32) * own_rows(
        is_live.astype(jnp.float32)[:, None]
    )
    _, pull_four = jax.vjp(rms_scale, ffn_branch, norm_ffn_out)
    grad_ffn_float, grad_norm_ffn_out = pull_four(grad_out)
    grad_ffn_all = gather_blocks(grad_ffn_float.astype(low), lanes, True, ("x", "core"), 4)
    grad_ffn_all = grad_ffn_all.reshape(-1, h_ffn.shape[1])
    grad_hidden = matmul(grad_ffn_all, down_full)
    grad_up = (grad_hidden * gelu_gate).astype(low)
    _, pull_gelu = jax.vjp(gelu_tanh, gate_pre)
    grad_gate = pull_gelu(grad_hidden * up_pre)[0].astype(low)
    grad_both = jnp.concatenate([grad_gate, grad_up], axis=1)
    grad_h_ffn = product_scatter(grad_both, ffn_full, (0, 2 * part), lanes, True, 5)
    grad_w_ffn = weight_grads(h_all, grad_ffn_all, grad_both, hidden)
    grad_w_ffn = grad_w_ffn.reshape(outer, inner, shard_rows, 3 * part)
    here, row = lax.axis_index("outer"), lax.axis_index("inner")

    def grad_block(step, turn):
        place = (lax.rem(here + step, outer), lax.rem(row + turn, inner), 0, 0)
        return lax.dynamic_slice(grad_w_ffn, place, (1, 1, shard_rows, 3 * part))[0, 0]

    groups_of_steps = (range(1, outer), [0])
    outgoing = [
        {(step, turn): grad_block(step, turn) for step in steps for turn in range(1, inner)}
        for steps in groups_of_steps
    ]
    grad_h_ffn, outgoing[1] = lax.optimization_barrier((grad_h_ffn, outgoing[1]))

    def start_rows(number):
        return {
            key: shifted(item, "inner", inner, key[1]) for key, item in outgoing[number].items()
        }

    def sum_rows(number, came):
        summed = {}
        for step in groups_of_steps[number]:
            total = grad_block(step, 0).astype(jnp.float32)
            for turn in range(1, inner):
                total = total + came[step, turn].astype(jnp.float32)
            summed[step] = total.astype(low)
        return summed

    def send_rows(summed):
        return {
            step: shifted(item, "outer", outer, step) if step else item
            for step, item in summed.items()
        }

    rows_now = sum_rows(0, start_rows(0))
    rows_later = start_rows(1)

    _, pull_three = jax.vjp(rms_scale, resid, norm_ffn_in)
    grad_resid_part, grad_norm_ffn_in = pull_three(grad_h_ffn)
    grad_resid = grad_out + grad_resid_part
    _, pull_two = jax.vjp(rms_scale, attn_branch, norm_attn_out)
    grad_attn_float, grad_norm_attn_out = pull_two(grad_resid)
    grad_attn_own, rows_now = lax.optimization_barrier((grad_attn_float.astype(low), rows_now))
    summed = send_rows(rows_now)
    grad_attn_branch = gather_blocks(
        grad_attn_own, lanes, False, ("x", "core"), 6
    ).reshape(row_count, -1)
    grad_mixed = matmul(grad_attn_branch, out_turned).astype(low)
    grad_mixed = grad_mixed.reshape(row_count, kv_heads, groups, HD).transpose(1, 2, 0, 3)
    grad_values = jnp.einsum(
        "kgqs,kgqd->ksd", probs, grad_mixed, preferred_element_type=jnp.float32
    ).astype(low)
    grad_probs = jnp.einsum(
        "kgqd,ksd->kgqs", grad_mixed, values, preferred_element_type=jnp.float32
    )
    row_delta = jnp.sum(weights * grad_probs, axis=-1, keepdims=True)
    tanh_part = capped / SOFT_CAP
    grad_scores = (weights * (grad_probs - row_delta) * (1.0 - tanh_part * tanh_part)).astype(low)
    grad_scores, rows_later = lax.optimization_barrier((grad_scores, rows_later))
    summed.update(send_rows(sum_rows(1, rows_later)))
    sum_gate, sum_up, sum_down = unpack([summed[step] for step in range(outer)], part)
    sum_down = sum_down.T
    grad_query_raw = jnp.einsum(
        "kgqs,ksd->kgqd", grad_scores, keys, preferred_element_type=jnp.float32
    )
    grad_query = (
        (grad_query_raw * cosine - rotate_half(grad_query_raw) * sine_wave) * QUERY_SCALE
    ).astype(low)
    grad_keys_raw = jnp.einsum(
        "kgqs,kgqd->ksd", grad_scores, query, preferred_element_type=jnp.float32
    )
    grad_keys = (grad_keys_raw * cosine - rotate_half(grad_keys_raw) * sine_wave).astype(low)
    grad_qkv = jnp.concatenate(
        [
            grad_query.transpose(2, 0, 1, 3).reshape(row_count, -1),
            grad_keys.transpose(1, 0, 2).reshape(row_count, -1),
            grad_values.transpose(1, 0, 2).reshape(row_count, -1),
        ],
        axis=1,
    )
    grad_a_part = right_product(grad_qkv, attn_full[:, :qkv_cols]).astype(low)
    grad_h_attn = scatter_sum(
        grad_a_part.reshape(tensor, split_rows, -1),
        lanes,
        False,
        ("x", "core"),
        ("core", "x"),
        7,
    )
    _, pull_one = jax.vjp(rms_scale, layer_own, norm_attn_in)
    grad_input_part, grad_norm_attn_in = pull_one(grad_h_attn)
    input_own = grad_resid + grad_input_part

    norm_rows = jnp.stack(
        [grad_norm_attn_in, grad_norm_attn_out, grad_norm_ffn_in, grad_norm_ffn_out]
    )
    strips = norm_rows.reshape(4, outer * inner, shard_rows).transpose(1, 0, 2)
    strips = strips.reshape(outer * inner, 1, -1).astype(low)
    attn_cols = attn_shard.shape[1]
    strips = jnp.pad(strips, ((0, 0), (0, 15), (0, attn_cols - strips.shape[2])))
    tail = jnp.concatenate([output_own, input_own.astype(low)], axis=0)
    sum_last, tails = finish(
        lanes, h_attn.T, grad_attn_branch.T, grad_qkv, mixed_flat, strips, tail, 8
    )
    layer_output = tails[:, :split_rows].reshape(row_count, -1)
    input_grad = tails[:, split_rows:].reshape(row_count, -1).astype(jnp.float32)
    sum_attn_in, sum_attn_out, sum_ffn_in, sum_ffn_out = (
        sum_last[shard_rows, i * shard_rows : (i + 1) * shard_rows] for i in range(4)
    )
    sum_last = sum_last[:shard_rows]
    sum_out = sum_last[:, qkv_cols:].T
    sum_query = sum_last[:, :query_cols]
    sum_key = sum_last[:, query_cols : query_cols + key_cols]
    sum_value = sum_last[:, query_cols + key_cols : qkv_cols]
    return (
        layer_output,
        input_grad,
        sum_attn_in,
        sum_query,
        sum_key,
        sum_value,
        sum_out,
        sum_attn_out,
        sum_ffn_in,
        sum_gate,
        sum_up,
        sum_down,
        sum_ffn_out,
    )


def solution(mesh):
    dp_size, tensor = mesh.shape["dp"], mesh.shape["tensor"]
    outer = math.gcd(4, dp_size)
    lanes = (outer, dp_size // outer, tensor)
    split = Mesh(mesh.devices.reshape(lanes), ("outer", "inner", "tensor"))
    dp = ("outer", "inner")

    def run(*args):
        return jax.shard_map(
            lambda *blocks: shards(lanes, *blocks),
            mesh=split,
            in_specs=(
                P(dp, None),
                P(dp, None),
                P(dp, None),
                P(),
                P(dp, "tensor"),
                P(dp, "tensor"),
                P(dp, "tensor"),
                P("tensor", dp),
                P(),
                P(),
                P(dp, "tensor"),
                P(dp, "tensor"),
                P("tensor", dp),
                P(),
            ),
            out_specs=(
                P(dp, None),
                P(dp, None),
                P(dp),
                P(dp, "tensor"),
                P(dp, "tensor"),
                P(dp, "tensor"),
                P("tensor", dp),
                P(dp),
                P(dp),
                P(dp, "tensor"),
                P(dp, "tensor"),
                P("tensor", dp),
                P(dp),
            ),
            check_vma=False,
        )(*args)

    return run
```
